8 devices in a mesh: data: 1 (over z), ctxo: 2 (over y), ctx: 4 (over x, core).
Axes of the slice: x: 2, y: 2, z: 1, core: 2. Of those that a mesh axis runs over, the one named last changes fastest.
Arguments:
- q_seq: bfloat16 [16, 3072, 6, 128], P('data', ('ctxo', 'ctx'))
- k_seq: bfloat16 [16, 3072, 2, 128], P('data', ('ctxo', 'ctx'))
- v_seq: bfloat16 [16, 3072, 2, 128], P('data', ('ctxo', 'ctx'))
- do_seq: bfloat16 [16, 3072, 6, 128], P('data', ('ctxo', 'ctx'))
Outputs:
- output 1: bfloat16 [16, 3072, 6, 128], P('data', ('ctxo', 'ctx'))
- output 2: bfloat16 [16, 3072, 6, 128], P('data', ('ctxo', 'ctx'))
- output 3: bfloat16 [16, 3072, 2, 128], P('data', ('ctxo', 'ctx'))
- output 4: bfloat16 [16, 3072, 2, 128], P('data', ('ctxo', 'ctx'))
All inputs are finite; a program needn't handle non-finite values.
Results may differ from the reference program's by a relative error of at most 0.0125474.
Values are sent between devices in bfloat16 or wider.
A program may use at most 1 GiB of HBM per device.

```python
import math
import jax
import jax.numpy as jnp
from jax import lax

BATCH_SEQS = 16
SEQ_LEN = 3072
Q_LOCAL = 6
KV_LOCAL = 2
HEAD_DIM = 128
ROW_BLOCK = 64


def setup_inputs(seed: int = 0, part: int = 0) -> dict:
    base_key = jax.random.fold_in(jax.random.key(seed), part)
    key_q, key_k, key_v, key_d = jax.random.split(base_key, 4)
    q_shape = (BATCH_SEQS, SEQ_LEN, Q_LOCAL, HEAD_DIM)
    kv_shape = (BATCH_SEQS, SEQ_LEN, KV_LOCAL, HEAD_DIM)
    spread = math.sqrt(1.0 + math.log(max(SEQ_LEN / 256.0, 1.0)))
    q_seq = spread * jax.random.normal(key_q, q_shape, jnp.float32)
    k_seq = jax.random.normal(key_k, kv_shape, jnp.float32)
    v_seq = jax.random.normal(key_v, kv_shape, jnp.float32)
    do_seq = jax.random.normal(key_d, q_shape, jnp.float32)
    return {'q_seq': q_seq.astype(jnp.bfloat16), 'k_seq': k_seq.astype(jnp.bfloat16), 'v_seq': v_seq.astype(jnp.bfloat16), 'do_seq': do_seq.astype(jnp.bfloat16)}


def reference(q_seq, k_seq, v_seq, do_seq):
    group_size = Q_LOCAL // KV_LOCAL
    n_blocks = SEQ_LEN // ROW_BLOCK
    q_scale = 1.0 / math.sqrt(HEAD_DIM)
    blocked = (BATCH_SEQS, n_blocks, ROW_BLOCK, KV_LOCAL, group_size, HEAD_DIM)
    q_rows = jnp.moveaxis(q_seq.astype(jnp.float32).reshape(blocked), 1, 0)
    do_rows = jnp.moveaxis(do_seq.astype(jnp.float32).reshape(blocked), 1, 0)
    key_pos = lax.broadcasted_iota(jnp.int32, (1, 1, SEQ_LEN), 2)
    row_pos = lax.broadcasted_iota(jnp.int32, (ROW_BLOCK, 1, 1), 0)

    def attention(q_blocks, keys_all, vals_all):
        def one_block(block_in):
            q_blk, blk_idx = block_in
            scores = jnp.einsum('bqhgd,bkhd->bhqgk', q_blk, keys_all) * q_scale
            visible = row_pos + blk_idx * ROW_BLOCK >= key_pos
            probs_blk = jax.nn.softmax(jnp.where(visible, scores, -jnp.inf), axis=-1)
            return jnp.einsum('bhqgk,bkhd->bqhgd', probs_blk, vals_all)
        return lax.map(jax.checkpoint(one_block), (q_blocks, jnp.arange(n_blocks)))

    out_rows, pull_back = jax.vjp(attention, q_rows, k_seq.astype(jnp.float32), v_seq.astype(jnp.float32))
    dq_rows, dk_all, dv_all = pull_back(do_rows)
    q_full = (BATCH_SEQS, SEQ_LEN, Q_LOCAL, HEAD_DIM)
    out_seq = jnp.moveaxis(out_rows, 0, 1).reshape(q_full)
    dq_seq = jnp.moveaxis(dq_rows, 0, 1).reshape(q_full)
    return (out_seq.astype(jnp.bfloat16), dq_seq.astype(jnp.bfloat16), dk_all.astype(jnp.bfloat16), dv_all.astype(jnp.bfloat16))
```

```python
import functools
import math
import jax
import jax.numpy as jnp
from jax import lax
from jax.experimental import pallas as pl
from jax.experimental.pallas import tpu as pltpu
from jax.sharding import PartitionSpec as P

CTX_AXES = ('ctxo', 'ctx')
MESH = pl.DeviceIdType.MESH
f32 = jnp.float32
bf16 = jnp.bfloat16
CHUNK = 768
SUB = 256


def dot(a, b):
    return jnp.dot(a, b, preferred_element_type=f32)


def fold(x, op):
    return op(x.reshape(x.shape[0] // 8, 8, x.shape[1]), axis=0)


def tile(i):
    return slice(i * SUB, (i + 1) * SUB)


def attend_chunk(c, q, do, k, v, o, dq, dk, dv, s, scale):
    kT, vT, qT, doT, sc_ref, dp_ref, oT, dqT, pb, sb = s
    score_scale = scale * math.log2(math.e)
    n_sub = CHUNK // SUB
    n_heads = q.shape[0]

    def rows(j, ki):
        return pl.ds(pl.multiple_of(j * CHUNK, CHUNK) + ki * SUB, SUB)

    def cols(ki, diag):
        return range(ki, n_sub) if diag else range(n_sub)

    lowest = tuple(jnp.full((8, SUB), -jnp.inf, f32) for _ in range(n_sub))

    def load_heads(h, b):
        for i in range(n_sub):
            qT[b, :, tile(i)] = q[h, tile(i), :].T
            doT[b, :, tile(i)] = do[h, tile(i), :].T

    def scores(j, b, m, ki, diag):
        for qi in cols(ki, diag):
            x = dot(k[rows(j, ki), :], qT[b, :, tile(qi)]) * score_scale
            if diag and ki == qi:
                key = lax.broadcasted_iota(jnp.int32, (SUB, SUB), 0)
                query = lax.broadcasted_iota(jnp.int32, (SUB, SUB), 1)
                x = jnp.where(key <= query, x, -jnp.inf)
            sc_ref[b, j, tile(ki), tile(qi)] = x
            m[qi] = jnp.maximum(m[qi], fold(x, jnp.max))

    def score_pass(b):
        def body(j, m, diag=False):
            m = list(m)
            for ki in range(n_sub):
                scores(j, b, m, ki, diag)
            return tuple(m)
        return body(c, lax.fori_loop(0, c, body, lowest), True)

    def forward_pass(b, m):
        top = [jnp.max(x, axis=0, keepdims=True) for x in m]
        oT[...] = jnp.zeros_like(oT)

        def body(j, l, diag=False):
            l, acc = list(l), [None] * n_sub

            def probs(ki):
                for qi in cols(ki, diag):
                    e = jnp.exp2(sc_ref[b, j, tile(ki), tile(qi)] - top[qi])
                    sc_ref[b, j, tile(ki), tile(qi)] = e
                    l[qi] = l[qi] + fold(e, jnp.sum)
                    pb[ki % 2, :, tile(qi)] = e.astype(bf16)

            def prob_grads(ki):
                for qi in cols(ki, diag):
                    dp_ref[j, tile(ki), tile(qi)] = dot(v[rows(j, ki), :], doT[b, :, tile(qi)])

            def outputs(ki):
                for qi in cols(ki, diag):
                    d = dot(vT[j, :, tile(ki)], pb[ki % 2, :, tile(qi)])
                    acc[qi] = d if acc[qi] is None else acc[qi] + d

            for ki in range(n_sub + 1):
                if ki < n_sub:
                    prob_grads(ki)
                    probs(ki)
                if ki:
                    outputs(ki - 1)
            for qi in range(n_sub):
                oT[:, tile(qi)] += acc[qi]
            return tuple(l)

        l = tuple(jnp.zeros((8, SUB), f32) for _ in range(n_sub))
        l = body(c, lax.fori_loop(0, c, body, l), True)
        return [1.0 / jnp.sum(x, axis=0, keepdims=True) for x in l]

    def finish_outputs(h, b, inv):
        drow = []
        for qi in range(n_sub):
            out = oT[:, tile(qi)] * inv[qi]
            drow.append(jnp.sum(out * doT[b, :, tile(qi)].astype(f32), axis=0, keepdims=True))
            o[h, tile(qi), :] = out.astype(bf16).T
        return drow

    def backward_pass(h, b, inv, drow, more):
        dqT[...] = jnp.zeros_like(dqT)

        def body(j, m, diag=False):
            m, acc = list(m), [None] * n_sub

            def score_grads(ki):
                for qi in cols(ki, diag):
                    p = sc_ref[b, j, tile(ki), tile(qi)] * inv[qi]
                    g = p * (dp_ref[j, tile(ki), tile(qi)] - drow[qi])
                    pb[ki % 2, :, tile(qi)] = p.astype(bf16)
                    sb[ki % 2, :, tile(qi)] = g.astype(bf16)

            def grads(ki):
                first = ki * SUB if diag else 0
                for qi in cols(ki, diag):
                    d = dot(kT[j, :, tile(ki)], sb[ki % 2, :, tile(qi)])
                    acc[qi] = d if acc[qi] is None else acc[qi] + d
                dv[rows(j, ki), :] += dot(pb[ki % 2, :, first:], do[h, first:, :])
                dk[rows(j, ki), :] += dot(sb[ki % 2, :, first:], q[h, first:, :])

            if more:
                scores(j, 1 - b, m, 0, diag)
            score_grads(0)
            for ki in range(1, n_sub):
                score_grads(ki)
                grads(ki - 1)
                if more:
                    scores(j, 1 - b, m, ki, diag)
            grads(n_sub - 1)
            for qi in range(n_sub):
                dqT[:, tile(qi)] += acc[qi]
            return tuple(m)

        m = body(c, lax.fori_loop(0, c, body, lowest), True)
        for qi in range(n_sub):
            dq[h, tile(qi), :] = (dqT[:, tile(qi)] * scale).astype(bf16).T
        return m

    load_heads(0, 0)
    m = score_pass(0)
    for h in range(n_heads):
        b = h % 2
        inv = forward_pass(b, m)
        drow = finish_outputs(h, b, inv)
        if h + 1 < n_heads:
            load_heads(h + 1, 1 - b)
        m = backward_pass(h, b, inv, drow, h + 1 < n_heads)


def kernel(n_dev, q, k, v, do, o, dq, dk, dv, qg, kg, vg, dog,
           q_v, do_v, k_v, v_v, o_v, dq_v, dk_v, dv_v, dka, dva,
           kT, vT, qT, doT, sc_ref, dp_ref, oT, dqT, pb, sb,
           in_send, in_recv, out_send, out_recv, load_sem, g_send):
    me = lax.axis_index('ctxo') * lax.axis_size('ctx') + lax.axis_index('ctx')
    n_in = lax.axis_size('ctx')
    n_rows, n_heads, blk, dim = q.shape
    n_kv = k.shape[1]
    grp = n_heads // n_kv
    own = n_rows // n_dev
    scale = 1.0 / math.sqrt(dim)
    n_chunks = n_dev * blk // CHUNK
    per_chunk = CHUNK // blk

    def where(dev):
        return (0, dev // n_in, dev % n_in)

    barrier = pltpu.get_barrier_semaphore()
    for d in range(1, n_dev):
        pl.semaphore_signal(barrier, inc=1, device_id=where((me + d) % n_dev), device_id_type=MESH)
    pl.semaphore_wait(barrier, n_dev - 1)

    arrays = ((q, qg, grp), (do, dog, grp), (k, kg, 1), (v, vg, 1))

    def send_unit(u, _):
        r, g = u // n_kv, u % n_kv
        for d in range(1, n_dev):
            peer = (me + d) % n_dev
            for a, (src, dst, w) in enumerate(arrays):
                pltpu.make_async_remote_copy(
                    src.at[own * peer + r, pl.ds(g * w, w)],
                    dst.at[u, :, pl.ds(pl.multiple_of(me * blk, blk), blk), :],
                    in_send.at[a], in_recv.at[u, a],
                    device_id=where(peer), device_id_type=MESH).start()
        return 0
    n_units = own * n_kv
    lax.fori_loop(0, n_units, send_unit, 0)

    vm = (q_v, do_v, k_v, v_v)

    def load_unit(u):
        r, g = u // n_kv, u % n_kv
        for a, (src, dst, w) in enumerate(arrays):
            got = dst.at[u, :, pl.ds(0, (n_dev - 1) * blk), :]
            pltpu.make_async_copy(got, got, in_recv.at[u, a]).wait()

        def one(s, start):
            for a, (src, dst, w) in enumerate(arrays):
                at = pl.ds(pl.multiple_of(s * blk, blk), blk)
                here = vm[a].at[:, at, :]

                @pl.when(s == me)
                def _():
                    cp = pltpu.make_async_copy(src.at[own * me + r, pl.ds(g * w, w)], here, load_sem.at[a, s])
                    cp.start() if start else cp.wait()

                @pl.when(s != me)
                def _():
                    cp = pltpu.make_async_copy(dst.at[u, :, at, :], here, load_sem.at[a, s])
                    cp.start() if start else cp.wait()
            return 0
        lax.fori_loop(0, n_dev, lambda s, _: one(s, True), 0)
        lax.fori_loop(0, n_dev, lambda s, _: one(s, False), 0)

    def place(src, dst_of, dev, send_sem, recv_sem):
        @pl.when(dev == me)
        def _():
            pltpu.make_async_copy(src, dst_of, send_sem).start()

        @pl.when(dev != me)
        def _():
            pltpu.make_async_remote_copy(src, dst_of, send_sem, recv_sem,
                                         device_id=where(dev), device_id_type=MESH).start()

    def unit(u, _):
        r, g = u // n_kv, u % n_kv
        row = own * me + r
        load_unit(u)
        for j in range(n_chunks):
            kT[j] = k_v[0, j * CHUNK:(j + 1) * CHUNK, :].T
            vT[j] = v_v[0, j * CHUNK:(j + 1) * CHUNK, :].T
        dka[...] = jnp.zeros_like(dka)
        dva[...] = jnp.zeros_like(dva)

        def chunk(c, _):
            step = u * n_chunks + c
            slot = step % 2
            at = pl.ds(pl.multiple_of(c * CHUNK, CHUNK), CHUNK)

            @pl.when(step >= 2)
            def _():
                for a, st in enumerate((o_v, dq_v)):
                    pltpu.make_async_copy(st.at[slot], st.at[slot], out_send.at[a, slot]).wait()
            attend_chunk(c, q_v.at[:, at, :], do_v.at[:, at, :], k_v.at[0], v_v.at[0],
                         o_v.at[slot], dq_v.at[slot], dka, dva,
                         (kT, vT, qT, doT, sc_ref, dp_ref, oT, dqT, pb, sb), scale)
            for e in range(per_chunk):
                for a, (st, dst) in enumerate(((o_v, o), (dq_v, dq))):
                    place(st.at[slot, :, e * blk:(e + 1) * blk, :], dst.at[row, pl.ds(g * grp, grp)],
                          c * per_chunk + e, out_send.at[a, slot], out_recv.at[a])
            return 0
        lax.fori_loop(0, n_chunks, chunk, 0)

        @pl.when(u >= 1)
        def _():
            for a, st in enumerate((dk_v, dv_v)):
                pltpu.make_async_copy(st, st, g_send.at[a]).wait()
        dk_v[...] = (dka[...] * scale).astype(bf16)
        dv_v[...] = dva[...].astype(bf16)

        def spread(s, _):
            at = pl.ds(pl.multiple_of(s * blk, blk), blk)
            for a, (st, dst) in enumerate(((dk_v, dk), (dv_v, dv))):
                place(st.at[at, :], dst.at[row, g], s, g_send.at[a], out_recv.at[2 + a])
            return 0
        lax.fori_loop(0, n_dev, spread, 0)
        return 0
    lax.fori_loop(0, n_units, unit, 0)

    for a, st in enumerate((o_v, dq_v)):
        for slot in range(2):
            pltpu.make_async_copy(st.at[slot], st.at[slot], out_send.at[a, slot]).wait()
    for a, st in enumerate((dk_v, dv_v)):
        pltpu.make_async_copy(st, st, g_send.at[a]).wait()
    for a, (src, _, _) in enumerate(arrays):
        part = src.at[pl.ds(0, n_rows - own)]
        pltpu.make_async_copy(part, part, in_send.at[a]).wait()
    for a, dst in enumerate((o, dq, dk, dv)):
        part = dst.at[pl.ds(0, n_rows - own)]
        pltpu.make_async_copy(part, part, out_recv.at[a]).wait()


def solution(mesh):
    n_dev = mesh.shape['ctxo'] * mesh.shape['ctx']
    spec = P('data', CTX_AXES, None, None)

    def local_attn(q_in, k_in, v_in, do_in):
        n_rows, blk, n_heads, dim = q_in.shape
        n_kv = k_in.shape[2]
        grp = n_heads // n_kv
        seq = blk * n_dev
        n_units = n_rows // n_dev * n_kv
        n_chunks = seq // CHUNK
        to_heads = lambda x: jnp.swapaxes(x, 1, 2)
        any_spec = pl.BlockSpec(memory_space=pl.ANY)
        shape = jax.ShapeDtypeStruct
        q_shape = shape((n_rows, n_heads, blk, dim), bf16)
        k_shape = shape((n_rows, n_kv, blk, dim), bf16)
        got_q = shape((n_units, grp, seq, dim), bf16)
        got_k = shape((n_units, 1, seq, dim), bf16)
        vmem, dma = pltpu.VMEM, pltpu.SemaphoreType.DMA
        res = pl.pallas_call(
            functools.partial(kernel, n_dev),
            out_shape=(q_shape, q_shape, k_shape, k_shape, got_q, got_k, got_k, got_q),
            in_specs=[any_spec] * 4,
            out_specs=(any_spec,) * 8,
            scratch_shapes=[
                vmem((grp, seq, dim), bf16), vmem((grp, seq, dim), bf16),
                vmem((1, seq, dim), bf16), vmem((1, seq, dim), bf16),
                vmem((2, grp, CHUNK, dim), bf16), vmem((2, grp, CHUNK, dim), bf16),
                vmem((seq, dim), bf16), vmem((seq, dim), bf16),
                vmem((seq, dim), f32), vmem((seq, dim), f32),
                vmem((n_chunks, dim, CHUNK), bf16), vmem((n_chunks, dim, CHUNK), bf16),
                vmem((2, dim, CHUNK), bf16), vmem((2, dim, CHUNK), bf16),
                vmem((2, n_chunks, CHUNK, CHUNK), f32), vmem((n_chunks, CHUNK, CHUNK), f32),
                vmem((dim, CHUNK), f32), vmem((dim, CHUNK), f32),
                vmem((2, SUB, CHUNK), bf16), vmem((2, SUB, CHUNK), bf16),
                dma((4,)), dma((n_units, 4)), dma((2, 2)), dma((4,)), dma((4, n_dev)), dma((2,)),
            ],
            compiler_params=pltpu.CompilerParams(
                collective_id=0, has_side_effects=True, vmem_limit_bytes=63 * 2**20),
            name='rows_attention',
        )(*(to_heads(x) for x in (q_in, k_in, v_in, do_in)))
        return tuple(to_heads(x) for x in res[:4])

    return jax.shard_map(local_attn, mesh=mesh, in_specs=(spec,) * 4, out_specs=(spec,) * 4, check_vma=False)
```

```python
import functools
import math
import jax
import jax.numpy as jnp
from jax import lax
from jax.experimental import pallas as pl
from jax.experimental.pallas import tpu as pltpu
from jax.sharding import PartitionSpec as P

CTX_AXES = ('ctxo', 'ctx')
MESH = pl.DeviceIdType.MESH
f32 = jnp.float32
bf16 = jnp.bfloat16
CHUNK = 768
SUB = 256
AHEAD = 3
LAG = 2


def dot(a, b):
    return jnp.dot(a, b, preferred_element_type=f32)


def fold(x, op):
    return op(x.reshape(x.shape[0] // 8, 8, x.shape[1]), axis=0)


def tile(i):
    return slice(i * SUB, (i + 1) * SUB)


def attend_chunk(c, q, do, kv, o, dq, g, s, scale, hooks):
    kT, vT, qT, doT, sc_ref, dp_ref, oT, dqT, pb, sb = s
    score_scale = scale * math.log2(math.e)
    n_sub = CHUNK // SUB
    n_heads = q.shape[0]

    def cols(ki, diag):
        return range(ki, n_sub) if diag else range(n_sub)

    lowest = tuple(jnp.full((8, SUB), -jnp.inf, f32) for _ in range(n_sub))

    def load_heads(h, b):
        for i in range(n_sub):
            qT[b, :, tile(i)] = q[h, tile(i), :].T
            doT[b, :, tile(i)] = do[h, tile(i), :].T

    def scores(j, b, m, ki, diag):
        for qi in cols(ki, diag):
            x = dot(kv[j, 0, tile(ki), :], qT[b, :, tile(qi)]) * score_scale
            if diag and ki == qi:
                key = lax.broadcasted_iota(jnp.int32, (SUB, SUB), 0)
                query = lax.broadcasted_iota(jnp.int32, (SUB, SUB), 1)
                x = jnp.where(key <= query, x, -jnp.inf)
            sc_ref[b, j, tile(ki), tile(qi)] = x
            m[qi] = jnp.maximum(m[qi], fold(x, jnp.max))

    def score_pass(b):
        def body(j, m, diag=False):
            m = list(m)
            for ki in range(n_sub):
                scores(j, b, m, ki, diag)
            return tuple(m)
        return body(c, lax.fori_loop(0, c, body, lowest), True)

    def forward_pass(b, m):
        top = [jnp.max(x, axis=0, keepdims=True) for x in m]
        oT[...] = jnp.zeros_like(oT)

        def body(j, l, diag=False):
            l, acc = list(l), [None] * n_sub

            def probs(ki):
                for qi in cols(ki, diag):
                    e = jnp.exp2(sc_ref[b, j, tile(ki), tile(qi)] - top[qi])
                    sc_ref[b, j, tile(ki), tile(qi)] = e
                    l[qi] = l[qi] + fold(e, jnp.sum)
                    pb[ki % 2, :, tile(qi)] = e.astype(bf16)

            def prob_grads(ki):
                for qi in cols(ki, diag):
                    dp_ref[j, tile(ki), tile(qi)] = dot(kv[j, 1, tile(ki), :], doT[b, :, tile(qi)])

            def outputs(ki):
                for qi in cols(ki, diag):
                    d = dot(vT[j, :, tile(ki)], pb[ki % 2, :, tile(qi)])
                    acc[qi] = d if acc[qi] is None else acc[qi] + d

            for ki in range(n_sub + 1):
                if ki < n_sub:
                    prob_grads(ki)
                    probs(ki)
                if ki:
                    outputs(ki - 1)
            for qi in range(n_sub):
                oT[:, tile(qi)] += acc[qi]
            return tuple(l)

        l = tuple(jnp.zeros((8, SUB), f32) for _ in range(n_sub))
        l = body(c, lax.fori_loop(0, c, body, l), True)
        return [1.0 / jnp.sum(x, axis=0, keepdims=True) for x in l]

    def finish_outputs(h, b, inv):
        drow = []
        for qi in range(n_sub):
            out = oT[:, tile(qi)] * inv[qi]
            drow.append(jnp.sum(out * doT[b, :, tile(qi)].astype(f32), axis=0, keepdims=True))
            o[h, tile(qi), :] = out.astype(bf16).T
        return drow

    def backward_pass(h, b, inv, drow, more):
        dqT[...] = jnp.zeros_like(dqT)

        def body(j, m, diag=False):
            m, acc = list(m), [None] * n_sub

            def score_grads(ki):
                for qi in cols(ki, diag):
                    p = sc_ref[b, j, tile(ki), tile(qi)] * inv[qi]
                    ds = p * (dp_ref[j, tile(ki), tile(qi)] - drow[qi])
                    pb[ki % 2, :, tile(qi)] = p.astype(bf16)
                    sb[ki % 2, :, tile(qi)] = ds.astype(bf16)

            def grads(ki):
                first = ki * SUB if diag else 0
                for qi in cols(ki, diag):
                    d = dot(kT[j, :, tile(ki)], sb[ki % 2, :, tile(qi)])
                    acc[qi] = d if acc[qi] is None else acc[qi] + d
                g[j, 1, tile(ki), :] += dot(pb[ki % 2, :, first:], do[h, first:, :])
                g[j, 0, tile(ki), :] += dot(sb[ki % 2, :, first:], q[h, first:, :])

            if more:
                scores(j, 1 - b, m, 0, diag)
            score_grads(0)
            for ki in range(1, n_sub):
                score_grads(ki)
                grads(ki - 1)
                if more:
                    scores(j, 1 - b, m, ki, diag)
            grads(n_sub - 1)
            for qi in range(n_sub):
                dqT[:, tile(qi)] += acc[qi]
            return tuple(m)

        m = body(c, lax.fori_loop(0, c, body, lowest), True)
        for qi in range(n_sub):
            dq[h, tile(qi), :] = (dqT[:, tile(qi)] * scale).astype(bf16).T
        return m

    load_heads(0, 0)
    m = score_pass(0)
    for h in range(n_heads):
        b = h % 2
        inv = forward_pass(b, m)
        drow = finish_outputs(h, b, inv)
        if h + 1 < n_heads:
            load_heads(h + 1, 1 - b)
        m = backward_pass(h, b, inv, drow, h + 1 < n_heads)
        if h < len(hooks):
            hooks[h]()


def kernel(q, k, v, do, o, dq, dk, dv, qd_l, kv_l, g_l,
           qd_v, kv_v, od_v, acc, g_in, g_out, kT, vT, *rest):
    scratch, sems = rest[:8], rest[8:]
    own_send, fed_send, kv_send, relay_send, qd_recv, kv_recv, g_send, g_recv, out_send, out_recv, grad_send, qd_load, kv_load, g_load = sems
    y, b = lax.axis_index('ctxo'), lax.axis_index('ctx')
    x, e = b // 2, b % 2
    n_rows, n_heads, blk, dim = q.shape
    n_kv = k.shape[1]
    grp = n_heads // n_kv
    lane_rows = n_rows // 2
    n_units = lane_rows
    c_own = 2 * y + x
    scale = 1.0 / math.sqrt(dim)

    def core(cy, cx, ce):
        return (0, cy, 2 * cx + ce)

    def both(kind, even, odd):
        return jnp.where(kind == 0, even, odd)

    def feeder(kind):
        return both(kind, 1 - y, y), both(kind, x, 1 - x)

    def partner(kind):
        return both(kind, y, 1 - y), both(kind, 1 - x, x)

    def chunk_of(kind, t):
        return both(kind, x + 2 * t, 2 * y + t)

    def row_of(w, lane):
        return lane * lane_rows + w

    def head_of(kind):
        return both(kind, y, x)

    def half(h):
        return pl.ds(pl.multiple_of(h * blk, blk), blk)

    def remote(src, dst, send, recv, dev):
        pltpu.make_async_remote_copy(src, dst, send, recv, device_id=dev, device_id_type=MESH).start()

    def drain(ref, sem):
        pltpu.make_async_copy(ref, ref, sem).wait()

    barrier = pltpu.get_barrier_semaphore()
    peers = [core(y, x, 1 - e)] + [core(1 - y, x, c) for c in range(2)] + [core(y, 1 - x, c) for c in range(2)]
    for dev in peers:
        pl.semaphore_signal(barrier, inc=1, device_id=dev, device_id_type=MESH)
    pl.semaphore_wait(barrier, len(peers))

    def first_has_kv(kind):
        return both(kind, x + y < 2, y == 0)

    def fed_goes_on(kind):
        return both(kind, (x == 0) | (y == 1), y == 0)

    def block(src, row, head, n):
        return src.at[row, pl.ds(head * n, n)]

    def send_ahead(w):
        kind = w % 2
        mine = head_of(kind)
        row = row_of(w, 1 - e)
        dev = core(y, x, 1 - e)
        for a, src in enumerate((q, do)):
            remote(block(src, row, mine, grp), qd_l.at[w, 0, a, :, half(e), :], own_send.at[a], qd_recv.at[w, 0], dev)
        for a, src in enumerate((k, v)):
            remote(src.at[row, mine], kv_l.at[w, c_own, a, half(e), :], own_send.at[2 + a], kv_recv.at[w, c_own], dev)
        fy, fx = feeder(kind)
        theirs = 1 - mine
        for lane in range(2):
            row = row_of(w, lane)
            dev = core(fy, fx, lane)
            for a, src in enumerate((k, v)):
                remote(src.at[row, theirs], kv_l.at[w, c_own, a, half(e), :], fed_send.at[2 + a], kv_recv.at[w, c_own], dev)
            for a, src in enumerate((q, do)):
                remote(block(src, row, theirs, grp), qd_l.at[w, 1, a, :, half(e), :], fed_send.at[a], qd_recv.at[w, 1], dev)
        py, px = partner(kind)

        @pl.when(first_has_kv(kind))
        def _():
            for lane in range(2):
                row = row_of(w, lane)
                for a, src in enumerate((k, v)):
                    remote(src.at[row, mine], kv_l.at[w, c_own, a, half(e), :], kv_send.at[a], kv_recv.at[w, c_own], core(py, px, lane))

    def fed_chunk(kind):
        fy, fx = feeder(kind)
        return 2 * fy + fx

    def pass_on(w):
        kind = w % 2
        c = fed_chunk(kind)
        drain(kv_l.at[w, c], kv_recv.at[w, c])
        py, px = partner(kind)

        @pl.when(fed_goes_on(kind))
        def _():
            remote(kv_l.at[w, c], kv_l.at[w, c], relay_send, kv_recv.at[w, c], core(py, px, e))

    def new_chunks(kind, t):
        return both(t, 0, chunk_of(kind, 0) + 1), chunk_of(kind, t) + 1

    def fetch(s):
        w, t = s // 2, s % 2
        kind, slot = w % 2, s % 2
        c = chunk_of(kind, t)
        own = c == c_own
        row, mine = row_of(w, e), head_of(kind)
        lo, hi = new_chunks(kind, t)

        def keys(j, _):
            dst = kv_v.at[w % 2, j]

            @pl.when(j == c_own)
            def _():
                other = kv_l.at[w, j, :, half(1 - e), :]
                drain(other, kv_recv.at[w, j])
                pltpu.make_async_copy(other, dst.at[:, half(1 - e), :], kv_load.at[w % 2, j]).start()
                for a, src in enumerate((k, v)):
                    pltpu.make_async_copy(src.at[row, mine], dst.at[a, half(e), :], kv_load.at[w % 2, j]).start()

            @pl.when(j != c_own)
            def _():
                @pl.when(j != fed_chunk(kind))
                def _():
                    drain(kv_l.at[w, j], kv_recv.at[w, j])
                pltpu.make_async_copy(kv_l.at[w, j], dst, kv_load.at[w % 2, j]).start()
            return 0
        lax.fori_loop(lo, hi, keys, 0)

        @pl.when(own)
        def _():
            other = qd_l.at[w, 0, :, :, half(1 - e), :]
            drain(other, qd_recv.at[w, 0])
            pltpu.make_async_copy(other, qd_v.at[slot, :, :, half(1 - e), :], qd_load.at[slot]).start()
            for a, src in enumerate((q, do)):
                pltpu.make_async_copy(block(src, row, mine, grp), qd_v.at[slot, a, :, half(e), :], qd_load.at[slot]).start()

        @pl.when(jnp.logical_not(own))
        def _():
            drain(qd_l.at[w, 1], qd_recv.at[w, 1])
            pltpu.make_async_copy(qd_l.at[w, 1], qd_v.at[slot], qd_load.at[slot]).start()

    def place(kind, c, send, pieces):
        fy, fx = feeder(kind)
        own = c == c_own
        oy, ox = jnp.where(own, y, fy), jnp.where(own, x, fx)
        for h in range(2):
            here = own & (e == h)
            for src, dst, recv in pieces(h):
                @pl.when(here)
                def _():
                    pltpu.make_async_copy(src, dst, send).start()

                @pl.when(jnp.logical_not(here))
                def _():
                    remote(src, dst, send, recv, core(oy, ox, h))

    def incoming(kind, a):
        return both(kind, (x == 0) | (a == 0), y == 0)

    def fetch_sums(w):
        kind = w % 2
        for a in range(2):
            @pl.when(incoming(kind, a))
            def _():
                drain(g_l.at[w, a], g_recv.at[w, a])
                pltpu.make_async_copy(g_l.at[w, a], g_in.at[a], g_load.at[a]).start()

    def merge(w):
        kind, slot = w % 2, w % (LAG + 1)
        row, mine = row_of(w, e), head_of(kind)
        for a in range(2):
            c = chunk_of(kind, a)

            @pl.when(w >= 1)
            def _():
                drain(g_out.at[a], grad_send.at[a])

            @pl.when(incoming(kind, a))
            def _():
                drain(g_in.at[a], g_load.at[a])
                g_out[a, 0] = ((acc[slot, c, 0] + g_in[a, 0]) * scale).astype(bf16)
                g_out[a, 1] = (acc[slot, c, 1] + g_in[a, 1]).astype(bf16)

            @pl.when(jnp.logical_not(incoming(kind, a)))
            def _():
                g_out[a, 0] = (acc[slot, c, 0] * scale).astype(bf16)
                g_out[a, 1] = acc[slot, c, 1].astype(bf16)
            place(kind, c, grad_send.at[a], lambda h: [
                (g_out.at[a, i, h * blk:(h + 1) * blk, :], dst.at[row, mine], out_recv.at[2 + i]) for i, dst in enumerate((dk, dv))])

    def n_sums_out(kind):
        return both(kind, 1 + x, 2 * y)

    def send_sums(w):
        kind, slot = w % 2, w % (LAG + 1)
        dev = core(*partner(kind), e)

        def one(c, a):
            remote(acc.at[slot, c], g_l.at[w, a], g_send.at[slot], g_recv.at[w, a], dev)

        @pl.when((kind == 0) & (x == 0))
        def _():
            one(1, 0)

        @pl.when((kind == 0) & (x == 1))
        def _():
            one(2, 1)
            one(0, 0)

        @pl.when((kind == 1) & (y == 1))
        def _():
            one(0, 0)
            one(1, 1)

    def sums_left(w):
        kind, slot = w % 2, w % (LAG + 1)
        n = n_sums_out(kind)
        for m in (1, 2):
            @pl.when(n == m)
            def _():
                drain(acc.at[slot, 0:m], g_send.at[slot])

    for w in range(AHEAD):
        send_ahead(w)
    pass_on(0)
    fetch(0)
    n_tasks = 2 * n_units

    def task(s, _):
        w, t = s // 2, s % 2
        kind, slot, a_slot = w % 2, s % 2, w % (LAG + 1)
        c = chunk_of(kind, t)

        @pl.when(t == 0)
        def _():
            @pl.when(w >= LAG + 1)
            def _():
                sums_left(w - LAG - 1)
            acc[a_slot] = jnp.zeros(acc.shape[1:], f32)
        lo, hi = new_chunks(kind, t)

        def turn(j, _):
            drain(kv_v.at[w % 2, j], kv_load.at[w % 2, j])
            kT[j] = kv_v[w % 2, j, 0].T
            vT[j] = kv_v[w % 2, j, 1].T
            return 0
        lax.fori_loop(lo, hi, turn, 0)
        drain(qd_v.at[slot], qd_load.at[slot])

        @pl.when(s >= 2)
        def _():
            drain(od_v.at[slot], out_send.at[slot])

        def early():
            @pl.when((t == 0) & (w + AHEAD < n_units))
            def _():
                send_ahead(w + AHEAD)

            @pl.when((t == 0) & (w + 1 < n_units))
            def _():
                pass_on(w + 1)

        def late():
            @pl.when(s + 1 < n_tasks)
            def _():
                fetch(s + 1)

            @pl.when((t == 1) & (w >= LAG))
            def _():
                fetch_sums(w - LAG)
        attend_chunk(c, qd_v.at[slot, 0], qd_v.at[slot, 1], kv_v.at[w % 2], od_v.at[slot, 0], od_v.at[slot, 1],
                     acc.at[a_slot], (kT, vT, *scratch), scale, (early, late))
        row, mine = row_of(w, e), head_of(kind)
        place(kind, c, out_send.at[slot], lambda h: [
            (od_v.at[slot, i, :, h * blk:(h + 1) * blk, :], block(dst, row, mine, grp), out_recv.at[i]) for i, dst in enumerate((o, dq))])

        @pl.when(t == 1)
        def _():
            send_sums(w)

            @pl.when(w >= LAG)
            def _():
                merge(w - LAG)
        return 0
    lax.fori_loop(0, n_tasks, task, 0)
    for w in range(n_units - LAG, n_units):
        fetch_sums(w)
        merge(w)

    for slot in range(2):
        drain(od_v.at[slot], out_send.at[slot])
        drain(g_out.at[slot], grad_send.at[slot])
    for w in range(n_units - LAG - 1, n_units):
        sums_left(w)
    part = n_units // 2
    for a, src in enumerate((q, do, k, v)):
        drain(src.at[0:part], own_send.at[a])
        drain(src.at[0:2 * part], fed_send.at[a])
    for kind in range(2):
        @pl.when(first_has_kv(kind))
        def _():
            for a, src in enumerate((k, v)):
                drain(src.at[0:part], kv_send.at[a])

        @pl.when(fed_goes_on(kind))
        def _():
            drain(kv_l.at[0:part, 0], relay_send)
    for a, dst in enumerate((o, dq, dk, dv)):
        drain(dst.at[0:3 * part], out_recv.at[a])


def solution(mesh):
    spec = P('data', CTX_AXES, None, None)

    def local_attn(q_in, k_in, v_in, do_in):
        n_rows, blk, n_heads, dim = q_in.shape
        n_kv = k_in.shape[2]
        grp = n_heads // n_kv
        n_units = n_rows // 2
        n_chunks = 4
        to_heads = lambda x: jnp.swapaxes(x, 1, 2)
        any_spec = pl.BlockSpec(memory_space=pl.ANY)
        shape = jax.ShapeDtypeStruct
        q_shape = shape((n_rows, n_heads, blk, dim), bf16)
        k_shape = shape((n_rows, n_kv, blk, dim), bf16)
        landing = (shape((n_units, 2, 2, grp, CHUNK, dim), bf16), shape((n_units, n_chunks, 2, CHUNK, dim), bf16),
                   shape((n_units, 2, 2, CHUNK, dim), f32))
        vmem, dma = pltpu.VMEM, pltpu.SemaphoreType.DMA
        res = pl.pallas_call(
            kernel,
            out_shape=(q_shape, q_shape, k_shape, k_shape, *landing),
            in_specs=[any_spec] * 4,
            out_specs=(any_spec,) * 7,
            scratch_shapes=[
                vmem((2, 2, grp, CHUNK, dim), bf16), vmem((2, n_chunks, 2, CHUNK, dim), bf16),
                vmem((2, 2, grp, CHUNK, dim), bf16),
                vmem((LAG + 1, n_chunks, 2, CHUNK, dim), f32),
                vmem((2, 2, CHUNK, dim), f32), vmem((2, 2, CHUNK, dim), bf16),
                vmem((n_chunks, dim, CHUNK), bf16), vmem((n_chunks, dim, CHUNK), bf16),
                vmem((2, dim, CHUNK), bf16), vmem((2, dim, CHUNK), bf16),
                vmem((2, n_chunks, CHUNK, CHUNK), f32), vmem((n_chunks, CHUNK, CHUNK), f32),
                vmem((dim, CHUNK), f32), vmem((dim, CHUNK), f32),
                vmem((2, SUB, CHUNK), bf16), vmem((2, SUB, CHUNK), bf16),
                dma((4,)), dma((4,)), dma((2,)), dma,
                dma((n_units, 2)), dma((n_units, n_chunks)),
                dma((LAG + 1,)), dma((n_units, 2)),
                dma((2,)), dma((4,)), dma((2,)), dma((2,)), dma((2, n_chunks)), dma((2,)),
            ],
            compiler_params=pltpu.CompilerParams(
                collective_id=0, has_side_effects=True, vmem_limit_bytes=63 * 2**20),
            name='pair_attention',
        )(*(to_heads(x) for x in (q_in, k_in, v_in, do_in)))
        return tuple(to_heads(x) for x in res[:4])

    return jax.shard_map(local_attn, mesh=mesh, in_specs=(spec,) * 4, out_specs=(spec,) * 4, check_vma=False)
```

```python
import functools
import math
import jax
import jax.numpy as jnp
from jax import lax
from jax.experimental import pallas as pl
from jax.experimental.pallas import tpu as pltpu
from jax.sharding import PartitionSpec as P

CTX_AXES = ('ctxo', 'ctx')
MESH = pl.DeviceIdType.MESH
f32 = jnp.float32
bf16 = jnp.bfloat16
CHUNK = 768
SUB = 256
LEADS = ((20, 20), (5, 4), (8, 12), (4, 4), (4, 6))
LAG = 2
OUT_SLOTS = 4


def dot(a, b):
    return jnp.dot(a, b, preferred_element_type=f32)


def fold(x, op):
    return op(x.reshape(x.shape[0] // 8, 8, x.shape[1]), axis=0)


def tile(i):
    return slice(i * SUB, (i + 1) * SUB)


def attend_chunk(c, q, do, kv, o, dq, g, s, scale, hooks):
    kT, vT, qT, doT, sc_ref, dp_ref, oT, dqT, pb, sb = s
    score_scale = scale * math.log2(math.e)
    n_sub = CHUNK // SUB
    n_heads = q.shape[0]

    def cols(ki, diag):
        return range(ki, n_sub) if diag else range(n_sub)

    lowest = tuple(jnp.full((8, SUB), -jnp.inf, f32) for _ in range(n_sub))

    def load_heads(h, b):
        for i in range(n_sub):
            qT[b, :, tile(i)] = q[h, tile(i), :].T
            doT[b, :, tile(i)] = do[h, tile(i), :].T

    def scores(j, b, m, ki, diag):
        for qi in cols(ki, diag):
            x = dot(kv[j, 0, tile(ki), :], qT[b, :, tile(qi)]) * score_scale
            if diag and ki == qi:
                key = lax.broadcasted_iota(jnp.int32, (SUB, SUB), 0)
                query = lax.broadcasted_iota(jnp.int32, (SUB, SUB), 1)
                x = jnp.where(key <= query, x, -jnp.inf)
            sc_ref[b, j, tile(ki), tile(qi)] = x
            m[qi] = jnp.maximum(m[qi], fold(x, jnp.max))

    def score_pass(b):
        def body(j, m, diag=False):
            m = list(m)
            for ki in range(n_sub):
                scores(j, b, m, ki, diag)
            return tuple(m)
        return body(c, lax.fori_loop(0, c, body, lowest), True)

    def forward_pass(b, m):
        top = [jnp.max(x, axis=0, keepdims=True) for x in m]
        oT[...] = jnp.zeros_like(oT)

        def body(j, l, diag=False):
            l, acc = list(l), [None] * n_sub

            def probs(ki):
                for qi in cols(ki, diag):
                    e = jnp.exp2(sc_ref[b, j, tile(ki), tile(qi)] - top[qi])
                    sc_ref[b, j, tile(ki), tile(qi)] = e
                    l[qi] = l[qi] + fold(e, jnp.sum)
                    pb[ki % 2, :, tile(qi)] = e.astype(bf16)

            def prob_grads(ki):
                for qi in cols(ki, diag):
                    dp_ref[j, tile(ki), tile(qi)] = dot(kv[j, 1, tile(ki), :], doT[b, :, tile(qi)])

            def outputs(ki):
                for qi in cols(ki, diag):
                    d = dot(vT[j, :, tile(ki)], pb[ki % 2, :, tile(qi)])
                    acc[qi] = d if acc[qi] is None else acc[qi] + d

            for ki in range(n_sub + 1):
                if ki < n_sub:
                    prob_grads(ki)
                    probs(ki)
                if ki:
                    outputs(ki - 1)
            for qi in range(n_sub):
                oT[:, tile(qi)] += acc[qi]
            return tuple(l)

        l = tuple(jnp.zeros((8, SUB), f32) for _ in range(n_sub))
        l = body(c, lax.fori_loop(0, c, body, l), True)
        return [1.0 / jnp.sum(x, axis=0, keepdims=True) for x in l]

    def finish_outputs(h, b, inv):
        drow = []
        for qi in range(n_sub):
            out = oT[:, tile(qi)] * inv[qi]
            drow.append(jnp.sum(out * doT[b, :, tile(qi)].astype(f32), axis=0, keepdims=True))
            o[h, tile(qi), :] = out.astype(bf16).T
        return drow

    def backward_pass(h, b, inv, drow, more):
        dqT[...] = jnp.zeros_like(dqT)

        def body(j, m, diag=False):
            m, acc = list(m), [None] * n_sub

            def score_grads(ki):
                for qi in cols(ki, diag):
                    p = sc_ref[b, j, tile(ki), tile(qi)] * inv[qi]
                    ds = p * (dp_ref[j, tile(ki), tile(qi)] - drow[qi])
                    pb[ki % 2, :, tile(qi)] = p.astype(bf16)
                    sb[ki % 2, :, tile(qi)] = ds.astype(bf16)

            def grads(ki):
                first = ki * SUB if diag else 0
                for qi in cols(ki, diag):
                    d = dot(kT[j, :, tile(ki)], sb[ki % 2, :, tile(qi)])
                    acc[qi] = d if acc[qi] is None else acc[qi] + d
                g[j, 1, tile(ki), :] += dot(pb[ki % 2, :, first:], do[h, first:, :])
                g[j, 0, tile(ki), :] += dot(sb[ki % 2, :, first:], q[h, first:, :])

            if more:
                scores(j, 1 - b, m, 0, diag)
            score_grads(0)
            for ki in range(1, n_sub):
                score_grads(ki)
                grads(ki - 1)
                if more:
                    scores(j, 1 - b, m, ki, diag)
            grads(n_sub - 1)
            for qi in range(n_sub):
                dqT[:, tile(qi)] += acc[qi]
            return tuple(m)

        m = body(c, lax.fori_loop(0, c, body, lowest), True)
        for qi in range(n_sub):
            dq[h, tile(qi), :] = (dqT[:, tile(qi)] * scale).astype(bf16).T
        return m

    load_heads(0, 0)
    m = score_pass(0)
    for h in range(n_heads):
        b = h % 2
        inv = forward_pass(b, m)
        drow = finish_outputs(h, b, inv)
        if h + 1 < n_heads:
            load_heads(h + 1, 1 - b)
        m = backward_pass(h, b, inv, drow, h + 1 < n_heads)
        if h < len(hooks):
            hooks[h]()


def kernel(q, k, v, do, o, dq, dk, dv, qd_l, kv_l, g_l,
           qd_v, kv_v, od_v, acc, g_in, g_out, kT, vT, *rest):
    scratch, sems = rest[:8], rest[8:]
    own_send, fed_send, kv_send, relay_send, qd_recv, kv_recv, g_send, g_recv, out_send, out_recv, grad_send, qd_load, kv_load, g_load = sems
    y, b = lax.axis_index('ctxo'), lax.axis_index('ctx')
    x, e = b // 2, b % 2
    n_rows, n_heads, blk, dim = q.shape
    n_kv = k.shape[1]
    grp = n_heads // n_kv
    lane_rows = n_rows // 2
    n_units = lane_rows
    c_own = 2 * y + x
    scale = 1.0 / math.sqrt(dim)

    def core(cy, cx, ce):
        return (0, cy, 2 * cx + ce)

    def both(kind, even, odd):
        return jnp.where(kind == 0, even, odd)

    def kind_of(w):
        return 1 - w % 2

    def feeder(kind):
        return both(kind, 1 - y, y), both(kind, x, 1 - x)

    def partner(kind):
        return both(kind, y, 1 - y), both(kind, 1 - x, x)

    def chunk_of(kind, t):
        return both(kind, x + 2 * t, 2 * y + t)

    def row_of(w, lane):
        return lane * lane_rows + w

    def head_of(kind):
        return both(kind, y, x)

    def half(h):
        return pl.ds(pl.multiple_of(h * blk, blk), blk)

    def remote(src, dst, send, recv, dev):
        pltpu.make_async_remote_copy(src, dst, send, recv, device_id=dev, device_id_type=MESH).start()

    def drain(ref, sem):
        pltpu.make_async_copy(ref, ref, sem).wait()

    barrier = pltpu.get_barrier_semaphore()
    peers = [core(y, x, 1 - e)] + [core(1 - y, x, c) for c in range(2)] + [core(y, 1 - x, c) for c in range(2)]
    for dev in peers:
        pl.semaphore_signal(barrier, inc=1, device_id=dev, device_id_type=MESH)
    pl.semaphore_wait(barrier, len(peers))

    def first_has_kv(kind):
        return both(kind, x + y < 2, y == 0)

    def fed_goes_on(kind):
        return both(kind, (x == 0) | (y == 1), y == 0)

    def block(src, row, head, n):
        return src.at[row, pl.ds(head * n, n)]

    def send_own(w, kind):
        mine, row, dev = head_of(kind), row_of(w, 1 - e), core(y, x, 1 - e)
        for a, src in enumerate((q, do)):
            remote(block(src, row, mine, grp), qd_l.at[w, 0, a, :, half(e), :], own_send.at[a], qd_recv.at[w, 0], dev)
        for a, src in enumerate((k, v)):
            remote(src.at[row, mine], kv_l.at[w, c_own, a, half(e), :], own_send.at[2 + a], kv_recv.at[w, c_own], dev)

    def feed_keys(w, kind):
        fy, fx = feeder(kind)
        for lane in range(2):
            for a, src in enumerate((k, v)):
                remote(src.at[row_of(w, lane), 1 - head_of(kind)], kv_l.at[w, c_own, a, half(e), :],
                       fed_send.at[2 + a], kv_recv.at[w, c_own], core(fy, fx, lane))

    def feed_queries(w, kind):
        fy, fx = feeder(kind)
        for lane in range(2):
            for a, src in enumerate((q, do)):
                remote(block(src, row_of(w, lane), 1 - head_of(kind), grp), qd_l.at[w, 1, a, :, half(e), :],
                       fed_send.at[a], qd_recv.at[w, 1], core(fy, fx, lane))

    def share_keys(w, kind):
        py, px = partner(kind)

        @pl.when(first_has_kv(kind))
        def _():
            for lane in range(2):
                for a, src in enumerate((k, v)):
                    remote(src.at[row_of(w, lane), head_of(kind)], kv_l.at[w, c_own, a, half(e), :],
                           kv_send.at[a], kv_recv.at[w, c_own], core(py, px, lane))

    def fed_chunk(kind):
        fy, fx = feeder(kind)
        return 2 * fy + fx

    def pass_on(w, kind):
        c = fed_chunk(kind)
        py, px = partner(kind)

        @pl.when(fed_goes_on(kind))
        def _():
            drain(kv_l.at[w, c], kv_recv.at[w, c])
            remote(kv_l.at[w, c], kv_l.at[w, c], relay_send, kv_recv.at[w, c], core(py, px, e))

    def new_chunks(kind, t):
        return both(t, 0, chunk_of(kind, 0) + 1), chunk_of(kind, t) + 1

    def fetch(s):
        w, t = s // 2, s % 2
        kind, slot = kind_of(w), s % 2
        c = chunk_of(kind, t)
        own = c == c_own
        row, mine = row_of(w, e), head_of(kind)
        lo, hi = new_chunks(kind, t)

        def keys(j, _):
            dst = kv_v.at[w % 2, j]

            @pl.when(j == c_own)
            def _():
                other = kv_l.at[w, j, :, half(1 - e), :]
                drain(other, kv_recv.at[w, j])
                pltpu.make_async_copy(other, dst.at[:, half(1 - e), :], kv_load.at[w % 2, j]).start()
                for a, src in enumerate((k, v)):
                    pltpu.make_async_copy(src.at[row, mine], dst.at[a, half(e), :], kv_load.at[w % 2, j]).start()

            @pl.when(j != c_own)
            def _():
                @pl.when((j != fed_chunk(kind)) | jnp.logical_not(fed_goes_on(kind)))
                def _():
                    drain(kv_l.at[w, j], kv_recv.at[w, j])
                pltpu.make_async_copy(kv_l.at[w, j], dst, kv_load.at[w % 2, j]).start()
            return 0
        lax.fori_loop(lo, hi, keys, 0)

        @pl.when(own)
        def _():
            other = qd_l.at[w, 0, :, :, half(1 - e), :]
            drain(other, qd_recv.at[w, 0])
            pltpu.make_async_copy(other, qd_v.at[slot, :, :, half(1 - e), :], qd_load.at[slot]).start()
            for a, src in enumerate((q, do)):
                pltpu.make_async_copy(block(src, row, mine, grp), qd_v.at[slot, a, :, half(e), :], qd_load.at[slot]).start()

        @pl.when(jnp.logical_not(own))
        def _():
            drain(qd_l.at[w, 1], qd_recv.at[w, 1])
            pltpu.make_async_copy(qd_l.at[w, 1], qd_v.at[slot], qd_load.at[slot]).start()

    def place(kind, c, send, pieces):
        fy, fx = feeder(kind)
        own = c == c_own
        oy, ox = jnp.where(own, y, fy), jnp.where(own, x, fx)
        for h in range(2):
            here = own & (e == h)
            for src, dst, recv in pieces(h):
                @pl.when(here)
                def _():
                    pltpu.make_async_copy(src, dst, send).start()

                @pl.when(jnp.logical_not(here))
                def _():
                    remote(src, dst, send, recv, core(oy, ox, h))

    def incoming(kind, a):
        return both(kind, (x == 0) | (a == 0), y == 0)

    def fetch_sums(w):
        kind = kind_of(w)
        for a in range(2):
            @pl.when(incoming(kind, a))
            def _():
                drain(g_l.at[w, a], g_recv.at[w, a])
                pltpu.make_async_copy(g_l.at[w, a], g_in.at[a], g_load.at[a]).start()

    def merge(w):
        kind, slot = kind_of(w), w % (LAG + 1)
        row, mine = row_of(w, e), head_of(kind)
        for a in range(2):
            c = chunk_of(kind, a)

            @pl.when(w >= 2)
            def _():
                drain(g_out.at[w % 2, a], grad_send.at[w % 2, a])

            @pl.when(incoming(kind, a))
            def _():
                drain(g_in.at[a], g_load.at[a])
                g_out[w % 2, a, 0] = ((acc[slot, c, 0] + g_in[a, 0]) * scale).astype(bf16)
                g_out[w % 2, a, 1] = (acc[slot, c, 1] + g_in[a, 1]).astype(bf16)

            @pl.when(jnp.logical_not(incoming(kind, a)))
            def _():
                g_out[w % 2, a, 0] = (acc[slot, c, 0] * scale).astype(bf16)
                g_out[w % 2, a, 1] = acc[slot, c, 1].astype(bf16)
            place(kind, c, grad_send.at[w % 2, a], lambda h: [
                (g_out.at[w % 2, a, i, h * blk:(h + 1) * blk, :], dst.at[row, mine], out_recv.at[2 + i]) for i, dst in enumerate((dk, dv))])

    def n_sums_out(kind):
        return both(kind, 1 + x, 2 * y)

    def send_sums(w):
        kind, slot = kind_of(w), w % (LAG + 1)
        dev = core(*partner(kind), e)

        def one(c, a):
            remote(acc.at[slot, c], g_l.at[w, a], g_send.at[slot], g_recv.at[w, a], dev)

        @pl.when((kind == 0) & (x == 0))
        def _():
            one(1, 0)

        @pl.when((kind == 0) & (x == 1))
        def _():
            one(2, 1)
            one(0, 0)

        @pl.when((kind == 1) & (y == 1))
        def _():
            one(0, 0)
            one(1, 1)

    def sums_left(w):
        kind, slot = kind_of(w), w % (LAG + 1)
        n = n_sums_out(kind)
        for m in (1, 2):
            @pl.when(n == m)
            def _():
                drain(acc.at[slot, 0:m], g_send.at[slot])

    jobs = (send_own, share_keys, feed_keys, pass_on, feed_queries)

    def run_due(h):
        for job, leads in zip(jobs, LEADS):
            for kind in range(2):
                later = h + leads[kind]
                w = later // 4

                @pl.when((later % 4 == 0) & (w < n_units) & (kind_of(w) == kind))
                def _():
                    job(w, kind)

    first = [(4 * w - LEADS[j][kind_of(w)], w, j) for w in range(n_units) for j in range(len(jobs))]
    for h, w, j in sorted(first):
        if h < 0:
            jobs[j](w, kind_of(w))
    fetch(0)
    n_tasks = 2 * n_units

    def task(s, _):
        w, t = s // 2, s % 2
        kind, slot, a_slot = kind_of(w), s % 2, w % (LAG + 1)
        c = chunk_of(kind, t)

        @pl.when(t == 0)
        def _():
            @pl.when(w >= LAG + 1)
            def _():
                sums_left(w - LAG - 1)
            acc[a_slot] = jnp.zeros(acc.shape[1:], f32)
        lo, hi = new_chunks(kind, t)

        def turn(j, _):
            drain(kv_v.at[w % 2, j], kv_load.at[w % 2, j])
            kT[j] = kv_v[w % 2, j, 0].T
            vT[j] = kv_v[w % 2, j, 1].T
            return 0
        lax.fori_loop(lo, hi, turn, 0)
        drain(qd_v.at[slot], qd_load.at[slot])

        o_slot = s % OUT_SLOTS

        @pl.when(s >= OUT_SLOTS)
        def _():
            drain(od_v.at[o_slot], out_send.at[o_slot])

        def early():
            run_due(2 * s)

        def late():
            run_due(2 * s + 1)

            @pl.when(s + 1 < n_tasks)
            def _():
                fetch(s + 1)

            @pl.when((t == 1) & (w >= LAG))
            def _():
                fetch_sums(w - LAG)
        attend_chunk(c, qd_v.at[slot, 0], qd_v.at[slot, 1], kv_v.at[w % 2], od_v.at[o_slot, 0], od_v.at[o_slot, 1],
                     acc.at[a_slot], (kT, vT, *scratch), scale, (early, late))
        row, mine = row_of(w, e), head_of(kind)
        place(kind, c, out_send.at[o_slot], lambda h: [
            (od_v.at[o_slot, i, :, h * blk:(h + 1) * blk, :], block(dst, row, mine, grp), out_recv.at[i]) for i, dst in enumerate((o, dq))])

        @pl.when(t == 1)
        def _():
            send_sums(w)

            @pl.when(w >= LAG)
            def _():
                merge(w - LAG)
        return 0
    lax.fori_loop(0, n_tasks, task, 0)
    for w in range(n_units - LAG, n_units):
        fetch_sums(w)
        merge(w)

    for slot in range(OUT_SLOTS):
        drain(od_v.at[slot], out_send.at[slot])
    for slot in range(2):
        for a in range(2):
            drain(g_out.at[slot, a], grad_send.at[slot, a])
    for w in range(n_units - LAG - 1, n_units):
        sums_left(w)
    part = n_units // 2
    for a, src in enumerate((q, do, k, v)):
        drain(src.at[0:part], own_send.at[a])
        drain(src.at[0:2 * part], fed_send.at[a])
    for kind in range(2):
        @pl.when(first_has_kv(kind))
        def _():
            for a, src in enumerate((k, v)):
                drain(src.at[0:part], kv_send.at[a])

        @pl.when(fed_goes_on(kind))
        def _():
            drain(kv_l.at[0:part, 0], relay_send)
    for a, dst in enumerate((o, dq, dk, dv)):
        drain(dst.at[0:3 * part], out_recv.at[a])


def solution(mesh):
    spec = P('data', CTX_AXES, None, None)

    def local_attn(q_in, k_in, v_in, do_in):
        n_rows, blk, n_heads, dim = q_in.shape
        n_kv = k_in.shape[2]
        grp = n_heads // n_kv
        n_units = n_rows // 2
        n_chunks = 4
        to_heads = lambda x: jnp.swapaxes(x, 1, 2)
        any_spec = pl.BlockSpec(memory_space=pl.ANY)
        shape = jax.ShapeDtypeStruct
        q_shape = shape((n_rows, n_heads, blk, dim), bf16)
        k_shape = shape((n_rows, n_kv, blk, dim), bf16)
        landing = (shape((n_units, 2, 2, grp, CHUNK, dim), bf16), shape((n_units, n_chunks, 2, CHUNK, dim), bf16),
                   shape((n_units, 2, 2, CHUNK, dim), f32))
        vmem, dma = pltpu.VMEM, pltpu.SemaphoreType.DMA
        res = pl.pallas_call(
            kernel,
            out_shape=(q_shape, q_shape, k_shape, k_shape, *landing),
            in_specs=[any_spec] * 4,
            out_specs=(any_spec,) * 7,
            scratch_shapes=[
                vmem((2, 2, grp, CHUNK, dim), bf16), vmem((2, n_chunks, 2, CHUNK, dim), bf16),
                vmem((OUT_SLOTS, 2, grp, CHUNK, dim), bf16),
                vmem((LAG + 1, n_chunks, 2, CHUNK, dim), f32),
                vmem((2, 2, CHUNK, dim), f32), vmem((2, 2, 2, CHUNK, dim), bf16),
                vmem((n_chunks, dim, CHUNK), bf16), vmem((n_chunks, dim, CHUNK), bf16),
                vmem((2, dim, CHUNK), bf16), vmem((2, dim, CHUNK), bf16),
                vmem((2, n_chunks, CHUNK, CHUNK), f32), vmem((n_chunks, CHUNK, CHUNK), f32),
                vmem((dim, CHUNK), f32), vmem((dim, CHUNK), f32),
                vmem((2, SUB, CHUNK), bf16), vmem((2, SUB, CHUNK), bf16),
                dma((4,)), dma((4,)), dma((2,)), dma,
                dma((n_units, 2)), dma((n_units, n_chunks)),
                dma((LAG + 1,)), dma((n_units, 2)),
                dma((OUT_SLOTS,)), dma((4,)), dma((2, 2)), dma((2,)), dma((2, n_chunks)), dma((2,)),
            ],
            compiler_params=pltpu.CompilerParams(
                collective_id=0, has_side_effects=True, vmem_limit_bytes=63 * 2**20),
            name='pair_attention',
        )(*(to_heads(x) for x in (q_in, k_in, v_in, do_in)))
        return tuple(to_heads(x) for x in res[:4])

    return jax.shard_map(local_attn, mesh=mesh, in_specs=(spec,) * 4, out_specs=(spec,) * 4, check_vma=False)
```

```python
import functools
import math
import jax
import jax.numpy as jnp
from jax import lax
from jax.experimental import pallas as pl
from jax.experimental.pallas import tpu as pltpu
from jax.sharding import PartitionSpec as P

CTX_AXES = ('ctxo', 'ctx')
MESH = pl.DeviceIdType.MESH
f32 = jnp.float32
bf16 = jnp.bfloat16
CHUNK = 768
SUB = 256
LEADS = (20, 10, 14, 6, 10)
KIND_1 = ((1, 3, 7), (0, 3, 4, 6))
LAG = 2
OUT_SLOTS = 4


def dot(a, b):
    return jnp.dot(a, b, preferred_element_type=f32)


def fold(x, op):
    return op(x.reshape(x.shape[0] // 8, 8, x.shape[1]), axis=0)


def tile(i):
    return slice(i * SUB, (i + 1) * SUB)


def attend_chunk(c, q, do, kv, o, dq, g, s, scale, hooks):
    kT, vT, qT, doT, sc_ref, dp_ref, oT, dqT, pb, sb = s
    score_scale = scale * math.log2(math.e)
    n_sub = CHUNK // SUB
    n_heads = q.shape[0]

    def cols(ki, diag):
        return range(ki, n_sub) if diag else range(n_sub)

    lowest = tuple(jnp.full((8, SUB), -jnp.inf, f32) for _ in range(n_sub))

    def load_heads(h, b):
        for i in range(n_sub):
            qT[b, :, tile(i)] = q[h, tile(i), :].T
            doT[b, :, tile(i)] = do[h, tile(i), :].T

    def scores(j, b, m, ki, diag):
        for qi in cols(ki, diag):
            x = dot(kv[j, 0, tile(ki), :], qT[b, :, tile(qi)]) * score_scale
            if diag and ki == qi:
                key = lax.broadcasted_iota(jnp.int32, (SUB, SUB), 0)
                query = lax.broadcasted_iota(jnp.int32, (SUB, SUB), 1)
                x = jnp.where(key <= query, x, -jnp.inf)
            sc_ref[b, j, tile(ki), tile(qi)] = x
            m[qi] = jnp.maximum(m[qi], fold(x, jnp.max))

    def score_pass(b):
        def body(j, m, diag=False):
            m = list(m)
            for ki in range(n_sub):
                scores(j, b, m, ki, diag)
            return tuple(m)
        return body(c, lax.fori_loop(0, c, body, lowest), True)

    def forward_pass(b, m):
        top = [jnp.max(x, axis=0, keepdims=True) for x in m]
        oT[...] = jnp.zeros_like(oT)

        def body(j, l, diag=False):
            l, acc = list(l), [None] * n_sub

            def probs(ki):
                for qi in cols(ki, diag):
                    e = jnp.exp2(sc_ref[b, j, tile(ki), tile(qi)] - top[qi])
                    sc_ref[b, j, tile(ki), tile(qi)] = e
                    l[qi] = l[qi] + fold(e, jnp.sum)
                    pb[ki % 2, :, tile(qi)] = e.astype(bf16)

            def prob_grads(ki):
                for qi in cols(ki, diag):
                    dp_ref[j, tile(ki), tile(qi)] = dot(kv[j, 1, tile(ki), :], doT[b, :, tile(qi)])

            def outputs(ki):
                for qi in cols(ki, diag):
                    d = dot(vT[j, :, tile(ki)], pb[ki % 2, :, tile(qi)])
                    acc[qi] = d if acc[qi] is None else acc[qi] + d

            for ki in range(n_sub + 1):
                if ki < n_sub:
                    prob_grads(ki)
                    probs(ki)
                if ki:
                    outputs(ki - 1)
            for qi in range(n_sub):
                oT[:, tile(qi)] += acc[qi]
            return tuple(l)

        l = tuple(jnp.zeros((8, SUB), f32) for _ in range(n_sub))
        l = body(c, lax.fori_loop(0, c, body, l), True)
        return [1.0 / jnp.sum(x, axis=0, keepdims=True) for x in l]

    def finish_outputs(h, b, inv):
        drow = []
        for qi in range(n_sub):
            out = oT[:, tile(qi)] * inv[qi]
            drow.append(jnp.sum(out * doT[b, :, tile(qi)].astype(f32), axis=0, keepdims=True))
            o[h, tile(qi), :] = out.astype(bf16).T
        return drow

    def backward_pass(h, b, inv, drow, more):
        dqT[...] = jnp.zeros_like(dqT)

        def body(j, m, diag=False):
            m, acc = list(m), [None] * n_sub

            def score_grads(ki):
                for qi in cols(ki, diag):
                    p = sc_ref[b, j, tile(ki), tile(qi)] * inv[qi]
                    ds = p * (dp_ref[j, tile(ki), tile(qi)] - drow[qi])
                    pb[ki % 2, :, tile(qi)] = p.astype(bf16)
                    sb[ki % 2, :, tile(qi)] = ds.astype(bf16)

            def grads(ki):
                first = ki * SUB if diag else 0
                for qi in cols(ki, diag):
                    d = dot(kT[j, :, tile(ki)], sb[ki % 2, :, tile(qi)])
                    acc[qi] = d if acc[qi] is None else acc[qi] + d
                g[j, 1, tile(ki), :] += dot(pb[ki % 2, :, first:], do[h, first:, :])
                g[j, 0, tile(ki), :] += dot(sb[ki % 2, :, first:], q[h, first:, :])

            if more:
                scores(j, 1 - b, m, 0, diag)
            score_grads(0)
            for ki in range(1, n_sub):
                score_grads(ki)
                grads(ki - 1)
                if more:
                    scores(j, 1 - b, m, ki, diag)
            grads(n_sub - 1)
            for qi in range(n_sub):
                dqT[:, tile(qi)] += acc[qi]
            return tuple(m)

        m = body(c, lax.fori_loop(0, c, body, lowest), True)
        for qi in range(n_sub):
            dq[h, tile(qi), :] = (dqT[:, tile(qi)] * scale).astype(bf16).T
        return m

    load_heads(0, 0)
    m = score_pass(0)
    for h in range(n_heads):
        b = h % 2
        inv = forward_pass(b, m)
        drow = finish_outputs(h, b, inv)
        if h + 1 < n_heads:
            load_heads(h + 1, 1 - b)
        m = backward_pass(h, b, inv, drow, h + 1 < n_heads)
        if h < len(hooks):
            hooks[h]()


def kernel(q, k, v, do, o, dq, dk, dv, qd_l, kv_l, g_l,
           qd_v, kv_v, od_v, acc, g_in, g_out, kT, vT, *rest):
    scratch, sems = rest[:8], rest[8:]
    own_send, fed_send, kv_send, relay_send, qd_recv, kv_recv, g_send, g_recv, out_send, out_recv, grad_send, qd_load, kv_load, g_load = sems
    y, b = lax.axis_index('ctxo'), lax.axis_index('ctx')
    x, e = b // 2, b % 2
    n_rows, n_heads, blk, dim = q.shape
    n_kv = k.shape[1]
    grp = n_heads // n_kv
    lane_rows = n_rows // 2
    n_units = lane_rows
    c_own = 2 * y + x
    scale = 1.0 / math.sqrt(dim)

    def core(cy, cx, ce):
        return (0, cy, 2 * cx + ce)

    def both(kind, even, odd):
        return jnp.where(kind == 0, even, odd)

    def kind_of(w, lane):
        return sum(jnp.where((lane == c) & (w == i), 1, 0) for c in range(2) for i in KIND_1[c])

    def feeder(kind):
        return both(kind, 1 - y, y), both(kind, x, 1 - x)

    def partner(kind):
        return both(kind, y, 1 - y), both(kind, 1 - x, x)

    def chunk_of(kind, t):
        return both(kind, x + 2 * t, 2 * y + t)

    def row_of(w, lane):
        return lane * lane_rows + w

    def head_of(kind):
        return both(kind, y, x)

    def half(h):
        return pl.ds(pl.multiple_of(h * blk, blk), blk)

    def remote(src, dst, send, recv, dev):
        pltpu.make_async_remote_copy(src, dst, send, recv, device_id=dev, device_id_type=MESH).start()

    def drain(ref, sem):
        pltpu.make_async_copy(ref, ref, sem).wait()

    barrier = pltpu.get_barrier_semaphore()
    peers = [core(y, x, 1 - e)] + [core(1 - y, x, c) for c in range(2)] + [core(y, 1 - x, c) for c in range(2)]
    for dev in peers:
        pl.semaphore_signal(barrier, inc=1, device_id=dev, device_id_type=MESH)
    pl.semaphore_wait(barrier, len(peers))

    def first_has_kv(kind):
        return both(kind, x + y < 2, y == 0)

    def fed_goes_on(kind):
        return both(kind, (x == 0) | (y == 1), y == 0)

    def block(src, row, head, n):
        return src.at[row, pl.ds(head * n, n)]

    def send_own(w, lane, kind):
        mine, row, dev = head_of(kind), row_of(w, lane), core(y, x, lane)
        for a, src in enumerate((q, do)):
            remote(block(src, row, mine, grp), qd_l.at[w, 0, a, :, half(e), :], own_send.at[a], qd_recv.at[w, 0], dev)
        for a, src in enumerate((k, v)):
            remote(src.at[row, mine], kv_l.at[w, c_own, a, half(e), :], own_send.at[2 + a], kv_recv.at[w, c_own], dev)

    def feed_keys(w, lane, kind):
        for a, src in enumerate((k, v)):
            remote(src.at[row_of(w, lane), 1 - head_of(kind)], kv_l.at[w, c_own, a, half(e), :],
                   fed_send.at[2 + a], kv_recv.at[w, c_own], core(*feeder(kind), lane))

    def feed_queries(w, lane, kind):
        for a, src in enumerate((q, do)):
            remote(block(src, row_of(w, lane), 1 - head_of(kind), grp), qd_l.at[w, 1, a, :, half(e), :],
                   fed_send.at[a], qd_recv.at[w, 1], core(*feeder(kind), lane))

    def share_keys(w, lane, kind):
        @pl.when(first_has_kv(kind))
        def _():
            for a, src in enumerate((k, v)):
                remote(src.at[row_of(w, lane), head_of(kind)], kv_l.at[w, c_own, a, half(e), :],
                       kv_send.at[a], kv_recv.at[w, c_own], core(*partner(kind), lane))

    def fed_chunk(kind):
        fy, fx = feeder(kind)
        return 2 * fy + fx

    def pass_on(w, lane, kind):
        c = fed_chunk(kind)

        @pl.when(fed_goes_on(kind))
        def _():
            drain(kv_l.at[w, c], kv_recv.at[w, c])
            remote(kv_l.at[w, c], kv_l.at[w, c], relay_send, kv_recv.at[w, c], core(*partner(kind), lane))

    def new_chunks(kind, t):
        return both(t, 0, chunk_of(kind, 0) + 1), chunk_of(kind, t) + 1

    def fetch(s):
        w, t = s // 2, s % 2
        kind, slot = kind_of(w, e), s % 2
        c = chunk_of(kind, t)
        own = c == c_own
        row, mine = row_of(w, e), head_of(kind)
        lo, hi = new_chunks(kind, t)

        def keys(j, _):
            dst = kv_v.at[w % 2, j]

            @pl.when(j == c_own)
            def _():
                other = kv_l.at[w, j, :, half(1 - e), :]
                drain(other, kv_recv.at[w, j])
                pltpu.make_async_copy(other, dst.at[:, half(1 - e), :], kv_load.at[w % 2, j]).start()
                for a, src in enumerate((k, v)):
                    pltpu.make_async_copy(src.at[row, mine], dst.at[a, half(e), :], kv_load.at[w % 2, j]).start()

            @pl.when(j != c_own)
            def _():
                @pl.when((j != fed_chunk(kind)) | jnp.logical_not(fed_goes_on(kind)))
                def _():
                    drain(kv_l.at[w, j], kv_recv.at[w, j])
                pltpu.make_async_copy(kv_l.at[w, j], dst, kv_load.at[w % 2, j]).start()
            return 0
        lax.fori_loop(lo, hi, keys, 0)

        @pl.when(own)
        def _():
            other = qd_l.at[w, 0, :, :, half(1 - e), :]
            drain(other, qd_recv.at[w, 0])
            pltpu.make_async_copy(other, qd_v.at[slot, :, :, half(1 - e), :], qd_load.at[slot]).start()
            for a, src in enumerate((q, do)):
                pltpu.make_async_copy(block(src, row, mine, grp), qd_v.at[slot, a, :, half(e), :], qd_load.at[slot]).start()

        @pl.when(jnp.logical_not(own))
        def _():
            drain(qd_l.at[w, 1], qd_recv.at[w, 1])
            pltpu.make_async_copy(qd_l.at[w, 1], qd_v.at[slot], qd_load.at[slot]).start()

    def place(kind, c, send, pieces):
        fy, fx = feeder(kind)
        own = c == c_own
        oy, ox = jnp.where(own, y, fy), jnp.where(own, x, fx)
        for h in range(2):
            here = own & (e == h)
            for src, dst, recv in pieces(h):
                @pl.when(here)
                def _():
                    pltpu.make_async_copy(src, dst, send).start()

                @pl.when(jnp.logical_not(here))
                def _():
                    remote(src, dst, send, recv, core(oy, ox, h))

    def incoming(kind, a):
        return both(kind, (x == 0) | (a == 0), y == 0)

    def fetch_sums(w):
        kind = kind_of(w, e)
        for a in range(2):
            @pl.when(incoming(kind, a))
            def _():
                drain(g_l.at[w, a], g_recv.at[w, a])
                pltpu.make_async_copy(g_l.at[w, a], g_in.at[a], g_load.at[a]).start()

    def merge(w):
        kind, slot = kind_of(w, e), w % (LAG + 1)
        row, mine = row_of(w, e), head_of(kind)
        for a in range(2):
            c = chunk_of(kind, a)

            @pl.when(w >= 2)
            def _():
                drain(g_out.at[w % 2, a], grad_send.at[w % 2, a])

            @pl.when(incoming(kind, a))
            def _():
                drain(g_in.at[a], g_load.at[a])
                g_out[w % 2, a, 0] = ((acc[slot, c, 0] + g_in[a, 0]) * scale).astype(bf16)
                g_out[w % 2, a, 1] = (acc[slot, c, 1] + g_in[a, 1]).astype(bf16)

            @pl.when(jnp.logical_not(incoming(kind, a)))
            def _():
                g_out[w % 2, a, 0] = (acc[slot, c, 0] * scale).astype(bf16)
                g_out[w % 2, a, 1] = acc[slot, c, 1].astype(bf16)
            place(kind, c, grad_send.at[w % 2, a], lambda h: [
                (g_out.at[w % 2, a, i, h * blk:(h + 1) * blk, :], dst.at[row, mine], out_recv.at[2 + i]) for i, dst in enumerate((dk, dv))])

    def n_sums_out(kind):
        return both(kind, 1 + x, 2 * y)

    def send_sums(w):
        kind, slot = kind_of(w, e), w % (LAG + 1)
        dev = core(*partner(kind), e)

        def one(c, a):
            remote(acc.at[slot, c], g_l.at[w, a], g_send.at[slot], g_recv.at[w, a], dev)

        @pl.when((kind == 0) & (x == 0))
        def _():
            one(1, 0)

        @pl.when((kind == 0) & (x == 1))
        def _():
            one(2, 1)
            one(0, 0)

        @pl.when((kind == 1) & (y == 1))
        def _():
            one(0, 0)
            one(1, 1)

    def sums_left(w):
        kind, slot = kind_of(w, e), w % (LAG + 1)
        n = n_sums_out(kind)
        for m in (1, 2):
            @pl.when(n == m)
            def _():
                drain(acc.at[slot, 0:m], g_send.at[slot])

    jobs = ((send_own, (1 - e,)), (share_keys, (0, 1)), (feed_keys, (0, 1)), (pass_on, (e,)), (feed_queries, (0, 1)))

    def run_due(h):
        for (job, lanes), lead in zip(jobs, LEADS):
            later = h + lead
            w = later // 4

            @pl.when((later % 4 == 0) & (w < n_units))
            def _():
                for lane in lanes:
                    job(w, lane, kind_of(w, lane))

    first = [(4 * w - LEADS[j], w, j) for w in range(n_units) for j in range(len(jobs))]
    for h, w, j in sorted(first):
        if h < 0:
            job, lanes = jobs[j]
            for lane in lanes:
                job(w, lane, kind_of(w, lane))
    fetch(0)
    n_tasks = 2 * n_units

    def task(s, _):
        w, t = s // 2, s % 2
        kind, slot, a_slot = kind_of(w, e), s % 2, w % (LAG + 1)
        c = chunk_of(kind, t)

        @pl.when(t == 0)
        def _():
            @pl.when(w >= LAG + 1)
            def _():
                sums_left(w - LAG - 1)
            acc[a_slot] = jnp.zeros(acc.shape[1:], f32)
        lo, hi = new_chunks(kind, t)

        def turn(j, _):
            drain(kv_v.at[w % 2, j], kv_load.at[w % 2, j])
            kT[j] = kv_v[w % 2, j, 0].T
            vT[j] = kv_v[w % 2, j, 1].T
            return 0
        lax.fori_loop(lo, hi, turn, 0)
        drain(qd_v.at[slot], qd_load.at[slot])

        o_slot = s % OUT_SLOTS

        @pl.when(s >= OUT_SLOTS)
        def _():
            drain(od_v.at[o_slot], out_send.at[o_slot])

        def early():
            run_due(2 * s)

        def late():
            run_due(2 * s + 1)

            @pl.when(s + 1 < n_tasks)
            def _():
                fetch(s + 1)

            @pl.when((t == 1) & (w >= LAG))
            def _():
                fetch_sums(w - LAG)
        attend_chunk(c, qd_v.at[slot, 0], qd_v.at[slot, 1], kv_v.at[w % 2], od_v.at[o_slot, 0], od_v.at[o_slot, 1],
                     acc.at[a_slot], (kT, vT, *scratch), scale, (early, late))
        row, mine = row_of(w, e), head_of(kind)
        place(kind, c, out_send.at[o_slot], lambda h: [
            (od_v.at[o_slot, i, :, h * blk:(h + 1) * blk, :], block(dst, row, mine, grp), out_recv.at[i]) for i, dst in enumerate((o, dq))])

        @pl.when(t == 1)
        def _():
            send_sums(w)

            @pl.when(w >= LAG)
            def _():
                merge(w - LAG)
        return 0
    lax.fori_loop(0, n_tasks, task, 0)
    for w in range(n_units - LAG, n_units):
        fetch_sums(w)
        merge(w)

    for slot in range(OUT_SLOTS):
        drain(od_v.at[slot], out_send.at[slot])
    for slot in range(2):
        for a in range(2):
            drain(g_out.at[slot, a], grad_send.at[slot, a])
    for w in range(n_units - LAG - 1, n_units):
        sums_left(w)
    part = n_units // 2
    for a, src in enumerate((q, do, k, v)):
        drain(src.at[0:part], own_send.at[a])
        drain(src.at[0:2 * part], fed_send.at[a])
    n_odd = [len(units) for units in KIND_1]
    for kind in range(2):
        n_kind = [n if kind else n_units - n for n in n_odd]

        @pl.when(first_has_kv(kind))
        def _():
            for a, src in enumerate((k, v)):
                drain(src.at[0:sum(n_kind), 0], kv_send.at[a])

        for lane in range(2):
            @pl.when(fed_goes_on(kind) & (e == lane))
            def _():
                drain(kv_l.at[0:n_kind[lane], 0], relay_send)
    for a, dst in enumerate((o, dq, dk, dv)):
        drain(dst.at[0:3 * part], out_recv.at[a])


def finish_kernel(o, dq, dk, dv, o_out, dq_out, dk_out, dv_out, ring, g_in, g_out, ring_in, ring_out, g_load, g_store):
    n_rows, n_kv, blk, _ = dk.shape
    half = SUB // n_kv
    at = lax.broadcasted_iota(jnp.int32, (SUB, SUB), 0)
    take = lax.broadcasted_iota(jnp.int32, (SUB, SUB), 1)
    perm = jnp.where(take == (at % n_kv) * half + at // n_kv, 1.0, 0.0).astype(bf16)
    pairs = ((o, o_out), (dq, dq_out))
    grads = ((dk, dk_out), (dv, dv_out))

    def move(i, out):
        src, dst = pairs[i % 2]
        if out:
            return pltpu.make_async_copy(ring.at[i], dst.at[i // 2], ring_out.at[i])
        return pltpu.make_async_copy(src.at[i // 2], ring.at[i], ring_in.at[i])

    def grad_rows(r):
        return pl.ds(4 * (r // 4), 4)

    def load(a, r):
        return pltpu.make_async_copy(grads[a][0].at[grad_rows(r)], g_in.at[a, grad_rows(r)], g_load.at[a, r // 4])

    def store(a, r):
        return pltpu.make_async_copy(g_out.at[a, grad_rows(r)], grads[a][1].at[grad_rows(r)], g_store.at[a, r // 4])

    n = 2 * n_rows
    for i in range(4):
        move(i, False).start()
    for r in range(0, n_rows, 4):
        load(0, r).start()
        load(1, r).start()
    for i in range(4, n):
        move(i, False).start()
    for i in range(n):
        move(i, False).wait()
        move(i, True).start()
        a, r = i % 2, i // 2
        if r % 4 == 0:
            load(a, r).wait()
        for p in range(blk // half):
            x = jnp.concatenate([g_in[a, r, h, p * half:(p + 1) * half, :] for h in range(n_kv)], 0)
            g_out[a, r, p * SUB:(p + 1) * SUB, :] = dot(perm, x).astype(bf16)
        if r % 4 == 3:
            store(a, r).start()
    for i in range(n):
        move(i, True).wait()
    for r in range(0, n_rows, 4):
        store(0, r).wait()
        store(1, r).wait()


def solution(mesh):
    spec = P('data', CTX_AXES, None, None)

    def local_attn(q_in, k_in, v_in, do_in):
        n_rows, blk, n_heads, dim = q_in.shape
        n_kv = k_in.shape[2]
        grp = n_heads // n_kv
        n_units = n_rows // 2
        n_chunks = 4
        to_heads = lambda x: jnp.swapaxes(x, 1, 2)
        any_spec = pl.BlockSpec(memory_space=pl.ANY)
        shape = jax.ShapeDtypeStruct
        q_shape = shape((n_rows, n_heads, blk, dim), bf16)
        k_shape = shape((n_rows, n_kv, blk, dim), bf16)
        landing = (shape((n_units, 2, 2, grp, CHUNK, dim), bf16), shape((n_units, n_chunks, 2, CHUNK, dim), bf16),
                   shape((n_units, 2, 2, CHUNK, dim), f32))
        vmem, dma = pltpu.VMEM, pltpu.SemaphoreType.DMA
        res = pl.pallas_call(
            kernel,
            out_shape=(q_shape, q_shape, k_shape, k_shape, *landing),
            in_specs=[any_spec] * 4,
            out_specs=(any_spec,) * 7,
            scratch_shapes=[
                vmem((2, 2, grp, CHUNK, dim), bf16), vmem((2, n_chunks, 2, CHUNK, dim), bf16),
                vmem((OUT_SLOTS, 2, grp, CHUNK, dim), bf16),
                vmem((LAG + 1, n_chunks, 2, CHUNK, dim), f32),
                vmem((2, 2, CHUNK, dim), f32), vmem((2, 2, 2, CHUNK, dim), bf16),
                vmem((n_chunks, dim, CHUNK), bf16), vmem((n_chunks, dim, CHUNK), bf16),
                vmem((2, dim, CHUNK), bf16), vmem((2, dim, CHUNK), bf16),
                vmem((2, n_chunks, CHUNK, CHUNK), f32), vmem((n_chunks, CHUNK, CHUNK), f32),
                vmem((dim, CHUNK), f32), vmem((dim, CHUNK), f32),
                vmem((2, SUB, CHUNK), bf16), vmem((2, SUB, CHUNK), bf16),
                dma((4,)), dma((4,)), dma((2,)), dma,
                dma((n_units, 2)), dma((n_units, n_chunks)),
                dma((LAG + 1,)), dma((n_units, 2)),
                dma((OUT_SLOTS,)), dma((4,)), dma((2, 2)), dma((2,)), dma((2, n_chunks)), dma((2,)),
            ],
            compiler_params=pltpu.CompilerParams(
                collective_id=0, has_side_effects=True, vmem_limit_bytes=63 * 2**20),
            name='pair_attention',
        )(*(to_heads(x) for x in (q_in, k_in, v_in, do_in)))
        joined = shape((n_rows, blk * n_kv, dim), bf16)
        o, dq, dk, dv = pl.pallas_call(
            finish_kernel,
            out_shape=(q_shape, q_shape, joined, joined),
            in_specs=[any_spec] * 4,
            out_specs=(any_spec,) * 4,
            scratch_shapes=[
                vmem((2 * n_rows, n_heads, blk, dim), bf16),
                vmem((2, n_rows, n_kv, blk, dim), bf16), vmem((2, n_rows, n_kv * blk, dim), bf16),
                dma((2 * n_rows,)), dma((2 * n_rows,)), dma((2, n_rows // 4)), dma((2, n_rows // 4)),
            ],
            compiler_params=pltpu.CompilerParams(vmem_limit_bytes=62 * 2**20),
            name='finish',
        )(*res[:4])
        return to_heads(o), to_heads(dq), dk.reshape(k_in.shape), dv.reshape(k_in.shape)

    return jax.shard_map(local_attn, mesh=mesh, in_specs=(spec,) * 4, out_specs=(spec,) * 4, check_vma=False)
```

```python
import functools
import math
import jax
import jax.numpy as jnp
from jax import lax
from jax.experimental import pallas as pl
from jax.experimental.pallas import tpu as pltpu
from jax.sharding import PartitionSpec as P

CTX_AXES = ('ctxo', 'ctx')
MESH = pl.DeviceIdType.MESH
f32 = jnp.float32
bf16 = jnp.bfloat16
CHUNK = 768
SUB = 256
LEADS = (20, 10, 14, 6, 10)
KIND_1 = ((1, 3, 7), (0, 3, 4, 6))
LAG = 2
OUT_SLOTS = 4


def dot(a, b):
    return jnp.dot(a, b, preferred_element_type=f32)


def fold(x, op):
    return op(x.reshape(x.shape[0] // 8, 8, x.shape[1]), axis=0)


def tile(i):
    return slice(i * SUB, (i + 1) * SUB)


def attend_chunk(c, q, do, kv, o, dq, g, s, scale, hooks):
    kT, vT, qT, doT, sc_ref, dp_ref, oT, dqT, pb, sb = s
    score_scale = scale * math.log2(math.e)
    n_sub = CHUNK // SUB
    n_heads = q.shape[0]

    def cols(ki, diag):
        return range(ki, n_sub) if diag else range(n_sub)

    lowest = tuple(jnp.full((8, SUB), -jnp.inf, f32) for _ in range(n_sub))

    def load_heads(h, b):
        for i in range(n_sub):
            qT[b, :, tile(i)] = q[h, tile(i), :].T
            doT[b, :, tile(i)] = do[h, tile(i), :].T

    def scores(j, b, m, ki, diag):
        for qi in cols(ki, diag):
            x = dot(kv[j, 0, tile(ki), :], qT[b, :, tile(qi)]) * score_scale
            if diag and ki == qi:
                key = lax.broadcasted_iota(jnp.int32, (SUB, SUB), 0)
                query = lax.broadcasted_iota(jnp.int32, (SUB, SUB), 1)
                x = jnp.where(key <= query, x, -jnp.inf)
            sc_ref[b, j, tile(ki), tile(qi)] = x
            m[qi] = jnp.maximum(m[qi], fold(x, jnp.max))

    def score_pass(b):
        def body(j, m, diag=False):
            m = list(m)
            for ki in range(n_sub):
                scores(j, b, m, ki, diag)
            return tuple(m)
        return body(c, lax.fori_loop(0, c, body, lowest), True)

    def forward_pass(b, m):
        top = [jnp.max(x, axis=0, keepdims=True) for x in m]
        oT[...] = jnp.zeros_like(oT)

        def body(j, l, diag=False):
            l, acc = list(l), [None] * n_sub

            def probs(ki):
                for qi in cols(ki, diag):
                    e = jnp.exp2(sc_ref[b, j, tile(ki), tile(qi)] - top[qi])
                    sc_ref[b, j, tile(ki), tile(qi)] = e
                    l[qi] = l[qi] + fold(e, jnp.sum)
                    pb[ki % 2, :, tile(qi)] = e.astype(bf16)

            def prob_grads(ki):
                for qi in cols(ki, diag):
                    dp_ref[j, tile(ki), tile(qi)] = dot(kv[j, 1, tile(ki), :], doT[b, :, tile(qi)])

            def outputs(ki):
                for qi in cols(ki, diag):
                    d = dot(vT[j, :, tile(ki)], pb[ki % 2, :, tile(qi)])
                    acc[qi] = d if acc[qi] is None else acc[qi] + d

            for ki in range(n_sub + 1):
                if ki < n_sub:
                    prob_grads(ki)
                    probs(ki)
                if ki:
                    outputs(ki - 1)
            for qi in range(n_sub):
                oT[:, tile(qi)] += acc[qi]
            return tuple(l)

        l = tuple(jnp.zeros((8, SUB), f32) for _ in range(n_sub))
        l = body(c, lax.fori_loop(0, c, body, l), True)
        return [1.0 / jnp.sum(x, axis=0, keepdims=True) for x in l]

    def finish_outputs(h, b, inv):
        drow = []
        for qi in range(n_sub):
            out = oT[:, tile(qi)] * inv[qi]
            drow.append(jnp.sum(out * doT[b, :, tile(qi)].astype(f32), axis=0, keepdims=True))
            o[h, tile(qi), :] = out.astype(bf16).T
        return drow

    def backward_pass(h, b, inv, drow, more):
        dqT[...] = jnp.zeros_like(dqT)

        def body(j, m, diag=False):
            m, acc = list(m), [None] * n_sub

            def score_grads(ki):
                for qi in cols(ki, diag):
                    p = sc_ref[b, j, tile(ki), tile(qi)] * inv[qi]
                    ds = p * (dp_ref[j, tile(ki), tile(qi)] - drow[qi])
                    pb[ki % 2, :, tile(qi)] = p.astype(bf16)
                    sb[ki % 2, :, tile(qi)] = ds.astype(bf16)

            def grads(ki):
                first = ki * SUB if diag else 0
                for qi in cols(ki, diag):
                    d = dot(kT[j, :, tile(ki)], sb[ki % 2, :, tile(qi)])
                    acc[qi] = d if acc[qi] is None else acc[qi] + d
                g[j, 1, tile(ki), :] += dot(pb[ki % 2, :, first:], do[h, first:, :])
                g[j, 0, tile(ki), :] += dot(sb[ki % 2, :, first:], q[h, first:, :])

            if more:
                scores(j, 1 - b, m, 0, diag)
            score_grads(0)
            for ki in range(1, n_sub):
                score_grads(ki)
                grads(ki - 1)
                if more:
                    scores(j, 1 - b, m, ki, diag)
            grads(n_sub - 1)
            for qi in range(n_sub):
                dqT[:, tile(qi)] += acc[qi]
            return tuple(m)

        m = body(c, lax.fori_loop(0, c, body, lowest), True)
        for qi in range(n_sub):
            dq[h, tile(qi), :] = (dqT[:, tile(qi)] * scale).astype(bf16).T
        return m

    load_heads(0, 0)
    m = score_pass(0)
    for h in range(n_heads):
        b = h % 2
        inv = forward_pass(b, m)
        drow = finish_outputs(h, b, inv)
        if h + 1 < n_heads:
            load_heads(h + 1, 1 - b)
        m = backward_pass(h, b, inv, drow, h + 1 < n_heads)
        if h < len(hooks):
            hooks[h]()


def kernel(q, k_raw, v_raw, do, o, dq, dk, dv, k, v, qd_l, kv_l, g_l,
           qd_v, kv_v, od_v, acc, g_in, g_out, kT, vT, *rest):
    scratch, sems = rest[:8], rest[8:]
    own_send, fed_send, kv_send, relay_send, qd_recv, kv_recv, g_send, g_recv, out_send, out_recv, grad_send, qd_load, kv_load, g_load = sems
    y, b = lax.axis_index('ctxo'), lax.axis_index('ctx')
    x, e = b // 2, b % 2
    n_rows, n_heads, blk, dim = q.shape
    n_kv = k.shape[1] // blk
    grp = n_heads // n_kv
    lane_rows = n_rows // 2
    n_units = lane_rows
    c_own = 2 * y + x
    scale = 1.0 / math.sqrt(dim)

    def core(cy, cx, ce):
        return (0, cy, 2 * cx + ce)

    def both(kind, even, odd):
        return jnp.where(kind == 0, even, odd)

    def kind_of(w, lane):
        return sum(jnp.where((lane == c) & (w == i), 1, 0) for c in range(2) for i in KIND_1[c])

    def feeder(kind):
        return both(kind, 1 - y, y), both(kind, x, 1 - x)

    def partner(kind):
        return both(kind, y, 1 - y), both(kind, 1 - x, x)

    def chunk_of(kind, t):
        return both(kind, x + 2 * t, 2 * y + t)

    def row_of(w, lane):
        return lane * lane_rows + w

    def head_of(kind):
        return both(kind, y, x)

    def half(h):
        return pl.ds(pl.multiple_of(h * blk, blk), blk)

    def remote(src, dst, send, recv, dev):
        pltpu.make_async_remote_copy(src, dst, send, recv, device_id=dev, device_id_type=MESH).start()

    def drain(ref, sem):
        pltpu.make_async_copy(ref, ref, sem).wait()

    barrier = pltpu.get_barrier_semaphore()
    peers = [core(y, x, 1 - e)] + [core(1 - y, x, c) for c in range(2)] + [core(y, 1 - x, c) for c in range(2)]
    for dev in peers:
        pl.semaphore_signal(barrier, inc=1, device_id=dev, device_id_type=MESH)
    pl.semaphore_wait(barrier, len(peers))

    def first_has_kv(kind):
        return both(kind, x + y < 2, y == 0)

    def fed_goes_on(kind):
        return both(kind, (x == 0) | (y == 1), y == 0)

    def block(src, row, head, n):
        return src.at[row, pl.ds(head * n, n)]

    def split_heads():
        part = SUB // n_kv
        at = lax.broadcasted_iota(jnp.int32, (SUB, SUB), 0)
        take = lax.broadcasted_iota(jnp.int32, (SUB, SUB), 1)
        perm = jnp.where(take == (at % part) * n_kv + at // part, 1.0, 0.0).astype(bf16)

        def room(a, r):
            return od_v.at[r // 6, r // 3 % 2, r % 3] if a else kv_v.at[r // 8, r // 2 % 4, r % 2]

        for a, raw in enumerate((k_raw, v_raw)):
            for r in range(n_rows):
                pltpu.make_async_copy(raw.at[r], room(a, r), kv_load.at[a, r // 4]).start()
        for a, (raw, dst) in enumerate(((k_raw, k), (v_raw, v))):
            def sort(r, _):
                @pl.when(r % 4 == 0)
                def _():
                    drain(raw.at[0:4], kv_load.at[a, r // 4])
                x = room(a, r)
                y = [dot(perm, x[tile(p), :]).astype(bf16) for p in range(n_kv * blk // SUB)]
                for p, rows in enumerate(y):
                    for h in range(n_kv):
                        x[h * blk + p * part:h * blk + (p + 1) * part, :] = rows[h * part:(h + 1) * part]
                return 0
            lax.fori_loop(0, n_rows, sort, 0)
            for r in range(n_rows):
                pltpu.make_async_copy(room(a, r), dst.at[r], qd_load.at[a]).start()
        for a, dst in enumerate((k, v)):
            drain(dst, qd_load.at[a])

    def send_own(w, lane, kind):
        mine, row, dev = head_of(kind), row_of(w, lane), core(y, x, lane)
        for a, src in enumerate((q, do)):
            remote(block(src, row, mine, grp), qd_l.at[w, 0, a, :, half(e), :], own_send.at[a], qd_recv.at[w, 0], dev)
        for a, src in enumerate((k, v)):
            remote(src.at[row, half(mine)], kv_l.at[w, c_own, a, half(e), :], own_send.at[2 + a], kv_recv.at[w, c_own], dev)

    def feed_keys(w, lane, kind):
        for a, src in enumerate((k, v)):
            remote(src.at[row_of(w, lane), half(1 - head_of(kind))], kv_l.at[w, c_own, a, half(e), :],
                   fed_send.at[2 + a], kv_recv.at[w, c_own], core(*feeder(kind), lane))

    def feed_queries(w, lane, kind):
        for a, src in enumerate((q, do)):
            remote(block(src, row_of(w, lane), 1 - head_of(kind), grp), qd_l.at[w, 1, a, :, half(e), :],
                   fed_send.at[a], qd_recv.at[w, 1], core(*feeder(kind), lane))

    def share_keys(w, lane, kind):
        @pl.when(first_has_kv(kind))
        def _():
            for a, src in enumerate((k, v)):
                remote(src.at[row_of(w, lane), half(head_of(kind))], kv_l.at[w, c_own, a, half(e), :],
                       kv_send.at[a], kv_recv.at[w, c_own], core(*partner(kind), lane))

    def fed_chunk(kind):
        fy, fx = feeder(kind)
        return 2 * fy + fx

    def pass_on(w, lane, kind):
        c = fed_chunk(kind)

        @pl.when(fed_goes_on(kind))
        def _():
            drain(kv_l.at[w, c], kv_recv.at[w, c])
            remote(kv_l.at[w, c], kv_l.at[w, c], relay_send, kv_recv.at[w, c], core(*partner(kind), lane))

    def new_chunks(kind, t):
        return both(t, 0, chunk_of(kind, 0) + 1), chunk_of(kind, t) + 1

    def fetch(s):
        w, t = s // 2, s % 2
        kind, slot = kind_of(w, e), s % 2
        c = chunk_of(kind, t)
        own = c == c_own
        row, mine = row_of(w, e), head_of(kind)
        lo, hi = new_chunks(kind, t)

        def keys(j, _):
            dst = kv_v.at[w % 2, j]

            @pl.when(j == c_own)
            def _():
                other = kv_l.at[w, j, :, half(1 - e), :]
                drain(other, kv_recv.at[w, j])
                pltpu.make_async_copy(other, dst.at[:, half(1 - e), :], kv_load.at[w % 2, j]).start()
                for a, src in enumerate((k, v)):
                    pltpu.make_async_copy(src.at[row, half(mine)], dst.at[a, half(e), :], kv_load.at[w % 2, j]).start()

            @pl.when(j != c_own)
            def _():
                @pl.when((j != fed_chunk(kind)) | jnp.logical_not(fed_goes_on(kind)))
                def _():
                    drain(kv_l.at[w, j], kv_recv.at[w, j])
                pltpu.make_async_copy(kv_l.at[w, j], dst, kv_load.at[w % 2, j]).start()
            return 0
        lax.fori_loop(lo, hi, keys, 0)

        @pl.when(own)
        def _():
            other = qd_l.at[w, 0, :, :, half(1 - e), :]
            drain(other, qd_recv.at[w, 0])
            pltpu.make_async_copy(other, qd_v.at[slot, :, :, half(1 - e), :], qd_load.at[slot]).start()
            for a, src in enumerate((q, do)):
                pltpu.make_async_copy(block(src, row, mine, grp), qd_v.at[slot, a, :, half(e), :], qd_load.at[slot]).start()

        @pl.when(jnp.logical_not(own))
        def _():
            drain(qd_l.at[w, 1], qd_recv.at[w, 1])
            pltpu.make_async_copy(qd_l.at[w, 1], qd_v.at[slot], qd_load.at[slot]).start()

    def place(kind, c, send, pieces):
        fy, fx = feeder(kind)
        own = c == c_own
        oy, ox = jnp.where(own, y, fy), jnp.where(own, x, fx)
        for h in range(2):
            here = own & (e == h)
            for src, dst, recv in pieces(h):
                @pl.when(here)
                def _():
                    pltpu.make_async_copy(src, dst, send).start()

                @pl.when(jnp.logical_not(here))
                def _():
                    remote(src, dst, send, recv, core(oy, ox, h))

    def incoming(kind, a):
        return both(kind, (x == 0) | (a == 0), y == 0)

    def fetch_sums(w):
        kind = kind_of(w, e)
        for a in range(2):
            @pl.when(incoming(kind, a))
            def _():
                drain(g_l.at[w, a], g_recv.at[w, a])
                pltpu.make_async_copy(g_l.at[w, a], g_in.at[a], g_load.at[a]).start()

    def merge(w):
        kind, slot = kind_of(w, e), w % (LAG + 1)
        row, mine = row_of(w, e), head_of(kind)
        for a in range(2):
            c = chunk_of(kind, a)

            @pl.when(w >= 2)
            def _():
                drain(g_out.at[w % 2, a], grad_send.at[w % 2, a])

            @pl.when(incoming(kind, a))
            def _():
                drain(g_in.at[a], g_load.at[a])
                g_out[w % 2, a, 0] = ((acc[slot, c, 0] + g_in[a, 0]) * scale).astype(bf16)
                g_out[w % 2, a, 1] = (acc[slot, c, 1] + g_in[a, 1]).astype(bf16)

            @pl.when(jnp.logical_not(incoming(kind, a)))
            def _():
                g_out[w % 2, a, 0] = (acc[slot, c, 0] * scale).astype(bf16)
                g_out[w % 2, a, 1] = acc[slot, c, 1].astype(bf16)
            place(kind, c, grad_send.at[w % 2, a], lambda h: [
                (g_out.at[w % 2, a, i, h * blk:(h + 1) * blk, :], dst.at[row, mine], out_recv.at[2 + i]) for i, dst in enumerate((dk, dv))])

    def n_sums_out(kind):
        return both(kind, 1 + x, 2 * y)

    def send_sums(w):
        kind, slot = kind_of(w, e), w % (LAG + 1)
        dev = core(*partner(kind), e)

        def one(c, a):
            remote(acc.at[slot, c], g_l.at[w, a], g_send.at[slot], g_recv.at[w, a], dev)

        @pl.when((kind == 0) & (x == 0))
        def _():
            one(1, 0)

        @pl.when((kind == 0) & (x == 1))
        def _():
            one(2, 1)
            one(0, 0)

        @pl.when((kind == 1) & (y == 1))
        def _():
            one(0, 0)
            one(1, 1)

    def sums_left(w):
        kind, slot = kind_of(w, e), w % (LAG + 1)
        n = n_sums_out(kind)
        for m in (1, 2):
            @pl.when(n == m)
            def _():
                drain(acc.at[slot, 0:m], g_send.at[slot])

    jobs = ((send_own, (1 - e,)), (share_keys, (0, 1)), (feed_keys, (0, 1)), (pass_on, (e,)), (feed_queries, (0, 1)))

    def run_due(h):
        for (job, lanes), lead in zip(jobs, LEADS):
            later = h + lead
            w = later // 4

            @pl.when((later % 4 == 0) & (w < n_units))
            def _():
                for lane in lanes:
                    job(w, lane, kind_of(w, lane))

    for lane in range(2):
        feed_queries(0, lane, kind_of(0, lane))
    split_heads()
    first = [(4 * w - LEADS[j], w, j) for w in range(n_units) for j in range(len(jobs))]
    for h, w, j in sorted(first):
        job, lanes = jobs[j]
        if h < 0 and (w, job) != (0, feed_queries):
            for lane in lanes:
                job(w, lane, kind_of(w, lane))
    fetch(0)
    n_tasks = 2 * n_units

    def task(s, _):
        w, t = s // 2, s % 2
        kind, slot, a_slot = kind_of(w, e), s % 2, w % (LAG + 1)
        c = chunk_of(kind, t)

        @pl.when(t == 0)
        def _():
            @pl.when(w >= LAG + 1)
            def _():
                sums_left(w - LAG - 1)
            acc[a_slot] = jnp.zeros(acc.shape[1:], f32)
        lo, hi = new_chunks(kind, t)

        def turn(j, _):
            drain(kv_v.at[w % 2, j], kv_load.at[w % 2, j])
            kT[j] = kv_v[w % 2, j, 0].T
            vT[j] = kv_v[w % 2, j, 1].T
            return 0
        lax.fori_loop(lo, hi, turn, 0)
        drain(qd_v.at[slot], qd_load.at[slot])

        o_slot = s % OUT_SLOTS

        @pl.when(s >= OUT_SLOTS)
        def _():
            drain(od_v.at[o_slot], out_send.at[o_slot])

        def early():
            run_due(2 * s)

        def late():
            run_due(2 * s + 1)

            @pl.when(s + 1 < n_tasks)
            def _():
                fetch(s + 1)

            @pl.when((t == 1) & (w >= LAG))
            def _():
                fetch_sums(w - LAG)
        attend_chunk(c, qd_v.at[slot, 0], qd_v.at[slot, 1], kv_v.at[w % 2], od_v.at[o_slot, 0], od_v.at[o_slot, 1],
                     acc.at[a_slot], (kT, vT, *scratch), scale, (early, late))
        row, mine = row_of(w, e), head_of(kind)
        place(kind, c, out_send.at[o_slot], lambda h: [
            (od_v.at[o_slot, i, :, h * blk:(h + 1) * blk, :], block(dst, row, mine, grp), out_recv.at[i]) for i, dst in enumerate((o, dq))])

        @pl.when(t == 1)
        def _():
            send_sums(w)

            @pl.when(w >= LAG)
            def _():
                merge(w - LAG)
        return 0
    lax.fori_loop(0, n_tasks, task, 0)
    for w in range(n_units - LAG, n_units):
        fetch_sums(w)
        merge(w)

    for slot in range(OUT_SLOTS):
        drain(od_v.at[slot], out_send.at[slot])
    for slot in range(2):
        for a in range(2):
            drain(g_out.at[slot, a], grad_send.at[slot, a])
    for w in range(n_units - LAG - 1, n_units):
        sums_left(w)
    part = n_units // 2
    for a, src in enumerate((q, do, k, v)):
        drain(src.at[0:part], own_send.at[a])
        drain(src.at[0:2 * part], fed_send.at[a])
    n_odd = [len(units) for units in KIND_1]
    for kind in range(2):
        n_kind = [n if kind else n_units - n for n in n_odd]

        @pl.when(first_has_kv(kind))
        def _():
            for a, src in enumerate((k, v)):
                drain(src.at[0:sum(n_kind), 0:blk], kv_send.at[a])

        for lane in range(2):
            @pl.when(fed_goes_on(kind) & (e == lane))
            def _():
                drain(kv_l.at[0:n_kind[lane], 0], relay_send)
    for a, dst in enumerate((o, dq, dk, dv)):
        drain(dst.at[0:3 * part], out_recv.at[a])


def finish_kernel(o, dq, dk, dv, o_out, dq_out, dk_out, dv_out, ring, g_in, g_out, ring_in, ring_out, g_load, g_store):
    n_rows, n_kv, blk, _ = dk.shape
    half = SUB // n_kv
    at = lax.broadcasted_iota(jnp.int32, (SUB, SUB), 0)
    take = lax.broadcasted_iota(jnp.int32, (SUB, SUB), 1)
    perm = jnp.where(take == (at % n_kv) * half + at // n_kv, 1.0, 0.0).astype(bf16)
    pairs = ((o, o_out), (dq, dq_out))
    grads = ((dk, dk_out), (dv, dv_out))

    def move(i, out):
        src, dst = pairs[i % 2]
        if out:
            return pltpu.make_async_copy(ring.at[i], dst.at[i // 2], ring_out.at[i])
        return pltpu.make_async_copy(src.at[i // 2], ring.at[i], ring_in.at[i])

    def grad_rows(r):
        return pl.ds(4 * (r // 4), 4)

    def load(a, r):
        return pltpu.make_async_copy(grads[a][0].at[grad_rows(r)], g_in.at[a, grad_rows(r)], g_load.at[a, r // 4])

    def store(a, r):
        return pltpu.make_async_copy(g_out.at[a, grad_rows(r)], grads[a][1].at[grad_rows(r)], g_store.at[a, r // 4])

    n = 2 * n_rows
    for i in range(4):
        move(i, False).start()
    for r in range(0, n_rows, 4):
        load(0, r).start()
        load(1, r).start()
    for i in range(4, n):
        move(i, False).start()
    for i in range(n):
        move(i, False).wait()
        move(i, True).start()
        a, r = i % 2, i // 2
        if r % 4 == 0:
            load(a, r).wait()
        for p in range(blk // half):
            x = jnp.concatenate([g_in[a, r, h, p * half:(p + 1) * half, :] for h in range(n_kv)], 0)
            g_out[a, r, p * SUB:(p + 1) * SUB, :] = dot(perm, x).astype(bf16)
        if r % 4 == 3:
            store(a, r).start()
    for i in range(n):
        move(i, True).wait()
    for r in range(0, n_rows, 4):
        store(0, r).wait()
        store(1, r).wait()


def solution(mesh):
    spec = P('data', CTX_AXES, None, None)

    def local_attn(q_in, k_in, v_in, do_in):
        n_rows, blk, n_heads, dim = q_in.shape
        n_kv = k_in.shape[2]
        grp = n_heads // n_kv
        n_units = n_rows // 2
        n_chunks = 4
        to_heads = lambda x: jnp.swapaxes(x, 1, 2)
        any_spec = pl.BlockSpec(memory_space=pl.ANY)
        shape = jax.ShapeDtypeStruct
        q_shape = shape((n_rows, n_heads, blk, dim), bf16)
        k_shape = shape((n_rows, n_kv, blk, dim), bf16)
        joined = shape((n_rows, blk * n_kv, dim), bf16)
        landing = (shape((n_units, 2, 2, grp, CHUNK, dim), bf16), shape((n_units, n_chunks, 2, CHUNK, dim), bf16),
                   shape((n_units, 2, 2, CHUNK, dim), f32))
        vmem, dma = pltpu.VMEM, pltpu.SemaphoreType.DMA
        res = pl.pallas_call(
            kernel,
            out_shape=(q_shape, q_shape, k_shape, k_shape, joined, joined, *landing),
            in_specs=[any_spec] * 4,
            out_specs=(any_spec,) * 9,
            scratch_shapes=[
                vmem((2, 2, grp, CHUNK, dim), bf16), vmem((2, n_chunks, 2, CHUNK, dim), bf16),
                vmem((OUT_SLOTS, 2, grp, CHUNK, dim), bf16),
                vmem((LAG + 1, n_chunks, 2, CHUNK, dim), f32),
                vmem((2, 2, CHUNK, dim), f32), vmem((2, 2, 2, CHUNK, dim), bf16),
                vmem((n_chunks, dim, CHUNK), bf16), vmem((n_chunks, dim, CHUNK), bf16),
                vmem((2, dim, CHUNK), bf16), vmem((2, dim, CHUNK), bf16),
                vmem((2, n_chunks, CHUNK, CHUNK), f32), vmem((n_chunks, CHUNK, CHUNK), f32),
                vmem((dim, CHUNK), f32), vmem((dim, CHUNK), f32),
                vmem((2, SUB, CHUNK), bf16), vmem((2, SUB, CHUNK), bf16),
                dma((4,)), dma((4,)), dma((2,)), dma,
                dma((n_units, 2)), dma((n_units, n_chunks)),
                dma((LAG + 1,)), dma((n_units, 2)),
                dma((OUT_SLOTS,)), dma((4,)), dma((2, 2)), dma((2,)), dma((2, n_chunks)), dma((2,)),
            ],
            compiler_params=pltpu.CompilerParams(
                collective_id=0, has_side_effects=True, vmem_limit_bytes=63 * 2**20),
            name='pair_attention',
        )(to_heads(q_in), k_in.reshape(joined.shape), v_in.reshape(joined.shape), to_heads(do_in))
        o, dq, dk, dv = pl.pallas_call(
            finish_kernel,
            out_shape=(q_shape, q_shape, joined, joined),
            in_specs=[any_spec] * 4,
            out_specs=(any_spec,) * 4,
            scratch_shapes=[
                vmem((2 * n_rows, n_heads, blk, dim), bf16),
                vmem((2, n_rows, n_kv, blk, dim), bf16), vmem((2, n_rows, n_kv * blk, dim), bf16),
                dma((2 * n_rows,)), dma((2 * n_rows,)), dma((2, n_rows // 4)), dma((2, n_rows // 4)),
            ],
            compiler_params=pltpu.CompilerParams(vmem_limit_bytes=62 * 2**20),
            name='finish',
        )(*res[:4])
        return to_heads(o), to_heads(dq), dk.reshape(k_in.shape), dv.reshape(k_in.shape)

    return jax.shard_map(local_attn, mesh=mesh, in_specs=(spec,) * 4, out_specs=(spec,) * 4, check_vma=False)
```

```python
import functools
import math
import jax
import jax.numpy as jnp
from jax import lax
from jax.experimental import pallas as pl
from jax.experimental.pallas import tpu as pltpu
from jax.sharding import PartitionSpec as P

CTX_AXES = ('ctxo', 'ctx')
MESH = pl.DeviceIdType.MESH
f32 = jnp.float32
bf16 = jnp.bfloat16
CHUNK = 768
SUB = 256
def by_chip(rows, read):
    return {kind: {c: read(word) for c, word in enumerate(words.split()) if word != '-'} for kind, words in rows.items()}


def digits(word):
    return tuple(int(z) for z in word)


WORK = by_chip({'T': '02 13 - -', 'Y': '0 - 2 13', 'X': '01 - 23 -', 'V': '0 1 - 23'}, digits)
FEED = by_chip({'T': '- - 0 1', 'Y': '- 3 - -', 'X': '- 0 - 2', 'V': '- - 3 -'}, int)
SHARE = by_chip({'T': '1 0 - -', 'Y': '2 - 3 -', 'X': '2 - - -', 'V': '1 3 - -'}, digits)
RELAY = by_chip({'T': '21 - - -', 'Y': '- - 03 12', 'X': '12 - - -', 'V': '- 03 - -'}, digits)
SUMS = by_chip({'T': '110 201000 - -', 'Y': '022 - 130 221020', 'X': '- - 000101 -', 'V': '012 - - 010111'},
               lambda word: tuple(digits(word[i:i + 3]) for i in range(0, len(word), 3)))
FINISH = by_chip({'T': '02:0:1 13:0: - -', 'Y': '- - 02:02:1 13:0:', 'X': '01:0:1 - 23:: -', 'V': '- 01:02:1 - 23::'},
                 lambda word: tuple(digits(part) for part in word.split(':')))
KINDS = 'TYXV'
UNITS = ('VTYXYTTVXXTVTVYX', 'VXYTTYXVXYTTVXTV')
LEADS = (20, 27, 20, 10, 10)
LAG = 2
OUT_SLOTS = 4


def dot(a, b):
    return jnp.dot(a, b, preferred_element_type=f32)


def fold(x, op):
    return op(x.reshape(x.shape[0] // 8, 8, x.shape[1]), axis=0)


def tile(i):
    return slice(i * SUB, (i + 1) * SUB)


def attend_chunk(c, q, do, kv, o, dq, g, base, s, scale, hooks):
    kT, vT, qT, doT, sc_ref, dp_ref, oT, dqT, pb, sb = s
    score_scale = scale * math.log2(math.e)
    n_sub = CHUNK // SUB
    n_heads = q.shape[0]

    def cols(ki, diag):
        return range(ki, n_sub) if diag else range(n_sub)

    lowest = tuple(jnp.full((8, SUB), -jnp.inf, f32) for _ in range(n_sub))

    def load_heads(h, b):
        for i in range(n_sub):
            qT[b, :, tile(i)] = q[h, tile(i), :].T
            doT[b, :, tile(i)] = do[h, tile(i), :].T

    def scores(j, b, m, ki, diag):
        for qi in cols(ki, diag):
            x = dot(kv[j, 0, tile(ki), :], qT[b, :, tile(qi)]) * score_scale
            if diag and ki == qi:
                key = lax.broadcasted_iota(jnp.int32, (SUB, SUB), 0)
                query = lax.broadcasted_iota(jnp.int32, (SUB, SUB), 1)
                x = jnp.where(key <= query, x, -jnp.inf)
            sc_ref[b, j, tile(ki), tile(qi)] = x
            m[qi] = jnp.maximum(m[qi], fold(x, jnp.max))

    def score_pass(b):
        def body(j, m, diag=False):
            m = list(m)
            for ki in range(n_sub):
                scores(j, b, m, ki, diag)
            return tuple(m)
        return body(c, lax.fori_loop(0, c, body, lowest), True)

    def forward_pass(b, m):
        top = [jnp.max(x, axis=0, keepdims=True) for x in m]
        oT[...] = jnp.zeros_like(oT)

        def body(j, l, diag=False):
            l, acc = list(l), [None] * n_sub

            def probs(ki):
                for qi in cols(ki, diag):
                    e = jnp.exp2(sc_ref[b, j, tile(ki), tile(qi)] - top[qi])
                    sc_ref[b, j, tile(ki), tile(qi)] = e
                    l[qi] = l[qi] + fold(e, jnp.sum)
                    pb[ki % 2, :, tile(qi)] = e.astype(bf16)

            def prob_grads(ki):
                for qi in cols(ki, diag):
                    dp_ref[j, tile(ki), tile(qi)] = dot(kv[j, 1, tile(ki), :], doT[b, :, tile(qi)])

            def outputs(ki):
                for qi in cols(ki, diag):
                    d = dot(vT[j, :, tile(ki)], pb[ki % 2, :, tile(qi)])
                    acc[qi] = d if acc[qi] is None else acc[qi] + d

            for ki in range(n_sub + 1):
                if ki < n_sub:
                    prob_grads(ki)
                    probs(ki)
                if ki:
                    outputs(ki - 1)
            for qi in range(n_sub):
                oT[:, tile(qi)] += acc[qi]
            return tuple(l)

        l = tuple(jnp.zeros((8, SUB), f32) for _ in range(n_sub))
        l = body(c, lax.fori_loop(0, c, body, l), True)
        return [1.0 / jnp.sum(x, axis=0, keepdims=True) for x in l]

    def finish_outputs(h, b, inv):
        drow = []
        for qi in range(n_sub):
            out = oT[:, tile(qi)] * inv[qi]
            drow.append(jnp.sum(out * doT[b, :, tile(qi)].astype(f32), axis=0, keepdims=True))
            o[h, tile(qi), :] = out.astype(bf16).T
        return drow

    def backward_pass(h, b, inv, drow, more):
        dqT[...] = jnp.zeros_like(dqT)

        def body(j, m, diag=False):
            m, acc = list(m), [None] * n_sub

            def score_grads(ki):
                for qi in cols(ki, diag):
                    p = sc_ref[b, j, tile(ki), tile(qi)] * inv[qi]
                    ds = p * (dp_ref[j, tile(ki), tile(qi)] - drow[qi])
                    pb[ki % 2, :, tile(qi)] = p.astype(bf16)
                    sb[ki % 2, :, tile(qi)] = ds.astype(bf16)

            def grads(ki):
                first = ki * SUB if diag else 0
                for qi in cols(ki, diag):
                    d = dot(kT[j, :, tile(ki)], sb[ki % 2, :, tile(qi)])
                    acc[qi] = d if acc[qi] is None else acc[qi] + d
                g[base + j, 1, tile(ki), :] += dot(pb[ki % 2, :, first:], do[h, first:, :])
                g[base + j, 0, tile(ki), :] += dot(sb[ki % 2, :, first:], q[h, first:, :])

            if more:
                scores(j, 1 - b, m, 0, diag)
            score_grads(0)
            for ki in range(1, n_sub):
                score_grads(ki)
                grads(ki - 1)
                if more:
                    scores(j, 1 - b, m, ki, diag)
            grads(n_sub - 1)
            for qi in range(n_sub):
                dqT[:, tile(qi)] += acc[qi]
            return tuple(m)

        m = body(c, lax.fori_loop(0, c, body, lowest), True)
        for qi in range(n_sub):
            dq[h, tile(qi), :] = (dqT[:, tile(qi)] * scale).astype(bf16).T
        return m

    load_heads(0, 0)
    m = score_pass(0)
    for h in range(n_heads):
        b = h % 2
        inv = forward_pass(b, m)
        drow = finish_outputs(h, b, inv)
        if h + 1 < n_heads:
            load_heads(h + 1, 1 - b)
        m = backward_pass(h, b, inv, drow, h + 1 < n_heads)
        if h < len(hooks):
            hooks[h]()


def kernel(q, k_raw, v_raw, do, o, dq, dk, dv, k, v, qd_l, kv_l, g_l,
           qd_v, kv_v, od_v, acc, g_in, g_out, kT, vT, *rest):
    scratch, sems = rest[:8], rest[8:]
    own_send, fed_send, kv_send, relay_send, qd_recv, kv_recv, g_send, g_recv, out_send, out_recv, grad_send, qd_load, kv_load, g_load = sems
    y, b = lax.axis_index('ctxo'), lax.axis_index('ctx')
    x, e = b // 2, b % 2
    chip = 2 * y + x
    n_rows, n_heads, blk, dim = q.shape
    n_kv = k.shape[1] // blk
    grp = n_heads // n_kv
    lane_rows = n_rows // 2
    n_units = lane_rows * n_kv
    chips, lanes = range(4), range(2)
    scale = 1.0 / math.sqrt(dim)
    depth = LAG + 1

    def core(c, ce):
        return (0, c // 2, 2 * (c % 2) + ce)

    def row_of(n, lane):
        return lane * lane_rows + n // n_kv

    def half(h):
        return pl.ds(pl.multiple_of(h * blk, blk), blk)

    def remote(src, dst, send, recv, dev):
        pltpu.make_async_remote_copy(src, dst, send, recv, device_id=dev, device_id_type=MESH).start()

    def drain(ref, sem):
        pltpu.make_async_copy(ref, ref, sem).wait()

    def choose(values, index):
        return functools.reduce(lambda r, i: jnp.where(index == i, values[i], r), range(1, len(values)), values[0])

    def tasks_of(c, lane):
        return [(n, j) for n in range(n_units) for j in WORK[UNITS[lane][n]].get(c, ())]

    def finished_of(c, lane):
        return [n for n in range(n_units) if c in FINISH[UNITS[lane][n]]]

    def here(value):
        return choose([value(c, lane) for c in chips for lane in lanes], 2 * chip + e)

    def padded(items, i):
        return items[i] if i < len(items) else 0
    most = max(len(tasks_of(c, lane)) for c in chips for lane in lanes)
    n_tasks = here(lambda c, lane: len(tasks_of(c, lane)))
    task_tab = [here(lambda c, lane: padded([4 * n + j for n, j in tasks_of(c, lane)], i)) for i in range(most + 1)]
    start_tab = [here(lambda c, lane: sum(m < n for m, _ in tasks_of(c, lane))) for n in range(n_units)]
    n_finished = here(lambda c, lane: len(finished_of(c, lane)))
    fin_tab = [here(lambda c, lane: padded(finished_of(c, lane), i)) for i in range(n_units)]

    def units_before(c, lane, i, finished):
        tasks = tasks_of(c, lane)
        now = tasks[i][0] if i < len(tasks) else n_units
        return sum((n in finished_of(c, lane)) == finished for n in {m for m, _ in tasks if m < now})
    fin_before = [here(lambda c, lane: units_before(c, lane, i, True)) for i in range(most)]
    oth_before = [here(lambda c, lane: units_before(c, lane, i, False)) for i in range(most)]

    def kind_of(n, lane):
        return jnp.where(lane == 0, *(choose([KINDS.index(u) for u in UNITS[c]], n) for c in lanes))

    def role(table, kind, c=chip):
        return choose([table(u, i) for u in KINDS for i in chips], 4 * kind + c)

    def own(kind):
        return role(lambda u, c: int(c in WORK[u].get(c, ())), kind) == 1

    def relayed(kind):
        return role(lambda u, c: RELAY[u].get(c, (-1, 0))[0], kind)

    barrier = pltpu.get_barrier_semaphore()
    peers = [core(chip, 1 - e)] + [core(c, ce) for c in (2 * (1 - y) + x, 2 * y + 1 - x) for ce in lanes]
    for dev in peers:
        pl.semaphore_signal(barrier, inc=1, device_id=dev, device_id_type=MESH)
    pl.semaphore_wait(barrier, len(peers))

    def block(src, n, lane, a):
        if a < 2:
            return src.at[row_of(n, lane), pl.ds((n % n_kv) * grp, grp)]
        return src.at[row_of(n, lane), half(n % n_kv)]

    def split_heads():
        part = SUB // n_kv
        at = lax.broadcasted_iota(jnp.int32, (SUB, SUB), 0)
        take = lax.broadcasted_iota(jnp.int32, (SUB, SUB), 1)
        perm = jnp.where(take == (at % part) * n_kv + at // part, 1.0, 0.0).astype(bf16)

        def room(a, r):
            return od_v.at[r // 6, r // 3 % 2, r % 3] if a else kv_v.at[r // 8, r // 2 % 4, r % 2]

        for a, raw in enumerate((k_raw, v_raw)):
            for r in range(n_rows):
                pltpu.make_async_copy(raw.at[r], room(a, r), kv_load.at[a, r // 4]).start()
        for a, (raw, dst) in enumerate(((k_raw, k), (v_raw, v))):
            def sort(r, _):
                @pl.when(r % 4 == 0)
                def _():
                    drain(raw.at[0:4], kv_load.at[a, r // 4])
                x = room(a, r)
                y = [dot(perm, x[tile(p), :]).astype(bf16) for p in range(n_kv * blk // SUB)]
                for p, rows in enumerate(y):
                    for h in range(n_kv):
                        x[h * blk + p * part:h * blk + (p + 1) * part, :] = rows[h * part:(h + 1) * part]
                return 0
            lax.fori_loop(0, n_rows, sort, 0)
            for r in range(n_rows):
                pltpu.make_async_copy(room(a, r), dst.at[r], qd_load.at[a]).start()
        for a, dst in enumerate((k, v)):
            drain(dst, qd_load.at[a])

    def send_keys(n, lane, c, send):
        for a, src in enumerate((k, v)):
            remote(block(src, n, lane, 2), kv_l.at[n, chip, a, half(e), :], send(a), kv_recv.at[n, chip], core(c, lane))

    def send_queries(n, lane, c, place, send):
        for a, src in enumerate((q, do)):
            remote(block(src, n, lane, 0), qd_l.at[n, place, a, :, half(e), :], send(a), qd_recv.at[n, place], core(c, lane))

    def send_own(n):
        lane = 1 - e

        @pl.when(own(kind_of(n, lane)))
        def _():
            send_queries(n, lane, chip, 0, lambda a: own_send.at[a])
            send_keys(n, lane, chip, lambda a: own_send.at[2 + a])

    def feed_keys(n):
        for lane in lanes:
            c = role(lambda u, i: FEED[u].get(i, -1), kind_of(n, lane))

            @pl.when(c >= 0)
            def _():
                send_keys(n, lane, c, lambda a: fed_send.at[2 + a, lane])

    def feed_queries(n):
        for lane in lanes:
            c = role(lambda u, i: FEED[u].get(i, -1), kind_of(n, lane))

            @pl.when(c >= 0)
            def _():
                send_queries(n, lane, c, 1, lambda a: fed_send.at[a, lane])

    def share_keys(n):
        for lane in lanes:
            c = role(lambda u, i: SHARE[u].get(i, (-1,))[0], kind_of(n, lane))

            @pl.when(c >= 0)
            def _():
                send_keys(n, lane, c, lambda a: kv_send.at[a, lane])

    def pass_on(n):
        kind = kind_of(n, e)
        j = relayed(kind)

        @pl.when(j >= 0)
        def _():
            drain(kv_l.at[n, j], kv_recv.at[n, j])
            c = role(lambda u, i: RELAY[u].get(i, (0, 0))[1], kind)
            remote(kv_l.at[n, j], kv_l.at[n, j], relay_send, kv_recv.at[n, j], core(c, e))

    jobs = (send_own, share_keys, feed_keys, pass_on, feed_queries)
    early_units = n_kv

    def run_due(h):
        for job, lead in zip(jobs, LEADS):
            lo = sum(jnp.where(2 * t - lead < h, 1, 0) for t in start_tab)
            hi = sum(jnp.where(2 * t - lead < h + 1, 1, 0) for t in start_tab)
            if job is feed_queries:
                lo = jnp.where(lo < early_units, early_units, lo)

            def one(n, _):
                job(n)
                return 0
            lax.fori_loop(lo, hi, one, 0)

    def fetch(s, slot_kv, first, prev):
        code = choose(task_tab, s)
        n, c = code // 4, code % 4
        kind, slot = kind_of(n, e), s % 2

        def keys(j, _):
            dst, sem = kv_v.at[slot_kv, j], kv_load.at[slot_kv, j]

            @pl.when(j == chip)
            def _():
                other = kv_l.at[n, j, :, half(1 - e), :]
                drain(other, kv_recv.at[n, j])
                pltpu.make_async_copy(other, dst.at[:, half(1 - e), :], sem).start()
                for a, src in enumerate((k, v)):
                    pltpu.make_async_copy(block(src, n, e, 2), dst.at[a, half(e), :], sem).start()

            @pl.when(j != chip)
            def _():
                @pl.when(j != relayed(kind))
                def _():
                    drain(kv_l.at[n, j], kv_recv.at[n, j])
                pltpu.make_async_copy(kv_l.at[n, j], dst, sem).start()
            return 0
        lax.fori_loop(jnp.where(first, 0, prev + 1), c + 1, keys, 0)

        @pl.when(c == chip)
        def _():
            other = qd_l.at[n, 0, :, :, half(1 - e), :]
            drain(other, qd_recv.at[n, 0])
            pltpu.make_async_copy(other, qd_v.at[slot, :, :, half(1 - e), :], qd_load.at[slot]).start()
            for a, src in enumerate((q, do)):
                pltpu.make_async_copy(block(src, n, e, 0), qd_v.at[slot, a, :, half(e), :], qd_load.at[slot]).start()

        @pl.when(c != chip)
        def _():
            drain(qd_l.at[n, 1], qd_recv.at[n, 1])
            pltpu.make_async_copy(qd_l.at[n, 1], qd_v.at[slot], qd_load.at[slot]).start()

    def place(c, send, pieces):
        for h in range(2):
            local = (c == chip) & (e == h)
            for src, dst, recv in pieces(h):
                @pl.when(local)
                def _():
                    pltpu.make_async_copy(src, dst, send).start()

                @pl.when(jnp.logical_not(local))
                def _():
                    remote(src, dst, send, recv, core(c, h))

    def n_in(kind, f):
        return role(lambda u, c: len(FINISH[u][c][1 + f]) if c in FINISH[u] else 0, kind)

    def get_sums(n, a):
        drain(g_l.at[n, a], g_recv.at[n, a])
        pltpu.make_async_copy(g_l.at[n, a], g_in.at[a], g_load.at[a]).start()

    def fetch_sums(i):
        n = choose(fin_tab, i)
        kind = kind_of(n, e)
        for a, f, least in ((0, 0, 1), (2, 0, 2), (1, 1, 1)):
            @pl.when(n_in(kind, f) >= least)
            def _():
                get_sums(n, a)

    def merge(i):
        n = choose(fin_tab, i)
        kind, base, slot = kind_of(n, e), 4 * (i % depth), i % 2
        for f in range(2):
            c = role(lambda u, j: FINISH[u][j][0][f] if j in FINISH[u] else 0, kind)

            @pl.when(i >= 2)
            def _():
                drain(g_out.at[slot, f], grad_send.at[slot, f])
            for places in ((), (0,), (0, 2)) if f == 0 else ((), (1,)):
                @pl.when(n_in(kind, f) == len(places))
                def _():
                    for a in places:
                        drain(g_in.at[a], g_load.at[a])
                    for i_kv, factor in enumerate((scale, None)):
                        total = acc[base + c, i_kv]
                        for a in places:
                            total = total + g_in[a, i_kv]
                        g_out[slot, f, i_kv] = (total if factor is None else total * factor).astype(bf16)
            place(c, grad_send.at[slot, f], lambda h: [
                (g_out.at[slot, f, i_kv, h * blk:(h + 1) * blk, :], dst.at[row_of(n, e), n % n_kv], out_recv.at[2 + i_kv, e])
                for i_kv, dst in enumerate((dk, dv))])

    def n_sums(kind):
        return role(lambda u, c: len(SUMS[u].get(c, ())), kind)

    def send_sums(n, base, sem):
        kind = kind_of(n, e)
        for m in range(2):
            @pl.when(n_sums(kind) > m)
            def _():
                j, c, a = (role(lambda u, i: SUMS[u][i][m][part] if len(SUMS[u].get(i, ())) > m else 0, kind) for part in range(3))
                remote(acc.at[base + j], g_l.at[n, a], sem, g_recv.at[n, a], core(c, e))

    def sums_left(i):
        n = choose(fin_tab, i)
        for m in (1, 2):
            @pl.when(n_sums(kind_of(n, e)) == m)
            def _():
                drain(acc.at[0:m], g_send.at[i % depth])

    lax.fori_loop(0, early_units, lambda n, _: (feed_queries(n), 0)[1], 0)
    split_heads()

    def before(h, _):
        run_due(h - max(LEADS))
        return 0
    lax.fori_loop(0, max(LEADS), before, 0)
    fetch(0, 0, True, 0)

    def task(s, _):
        n_fin, n_oth = choose(fin_before, s), choose(oth_before, s)
        code, after = choose(task_tab, s), choose(task_tab, s + 1)
        n, c = code // 4, code % 4
        prev = choose([task_tab[0]] + task_tab[:-1], s)
        first = (s == 0) | (prev // 4 != n)
        last = (s + 1 == n_tasks) | (after // 4 != n)
        kind = kind_of(n, e)
        fin = role(lambda u, i: int(i in FINISH[u]), kind) == 1
        base = jnp.where(fin, 4 * (n_fin % depth), 4 * depth + n_oth % 2)
        slot, slot_kv, o_slot = s % 2, (n_fin + n_oth) % 2, s % OUT_SLOTS
        lo = jnp.where(first, 0, prev % 4 + 1)

        @pl.when(first & fin & (n_fin >= depth))
        def _():
            sums_left(n_fin - depth)

        @pl.when(first & jnp.logical_not(fin) & (n_oth >= 2))
        def _():
            drain(acc.at[0], g_send.at[depth + n_oth % 2])

        def turn(j, _):
            drain(kv_v.at[slot_kv, j], kv_load.at[slot_kv, j])
            kT[j] = kv_v[slot_kv, j, 0].T
            vT[j] = kv_v[slot_kv, j, 1].T
            acc[base + j] = jnp.zeros(acc.shape[1:], f32)
            return 0
        lax.fori_loop(lo, c + 1, turn, 0)
        drain(qd_v.at[slot], qd_load.at[slot])

        @pl.when(s >= OUT_SLOTS)
        def _():
            drain(od_v.at[o_slot], out_send.at[o_slot])

        def early():
            run_due(2 * s)

        def late():
            run_due(2 * s + 1)

            @pl.when(s + 1 < n_tasks)
            def _():
                fetch(s + 1, (n_fin + n_oth + jnp.where(last, 1, 0)) % 2, last, c)

            @pl.when(last & fin & (n_fin >= LAG))
            def _():
                fetch_sums(n_fin - LAG)
        attend_chunk(c, qd_v.at[slot, 0], qd_v.at[slot, 1], kv_v.at[slot_kv], od_v.at[o_slot, 0], od_v.at[o_slot, 1],
                     acc, base, (kT, vT, *scratch), scale, (early, late))
        place(c, out_send.at[o_slot], lambda h: [
            (od_v.at[o_slot, i, :, h * blk:(h + 1) * blk, :], block(dst, n, e, 0), out_recv.at[i, e]) for i, dst in enumerate((o, dq))])

        @pl.when(last)
        def _():
            send_sums(n, base, g_send.at[jnp.where(fin, n_fin % depth, depth + n_oth % 2)])

            @pl.when(fin & (n_fin >= LAG))
            def _():
                merge(n_fin - LAG)
        return 0

    def task_or_rest(s, _):
        @pl.when(s < n_tasks)
        def _():
            task(s, 0)
        return 0
    lax.fori_loop(0, most, task_or_rest, 0)

    def rest_of(i, _):
        fetch_sums(i)
        merge(i)
        return 0
    lax.fori_loop(n_finished - LAG, n_finished, rest_of, 0)

    for slot in range(OUT_SLOTS):
        drain(od_v.at[slot], out_send.at[slot])
    for slot in range(2):
        for f in range(2):
            drain(g_out.at[slot, f], grad_send.at[slot, f])
    lax.fori_loop(n_finished - depth, n_finished, lambda i, _: (sums_left(i), 0)[1], 0)

    def count(table, c, lane):
        return sum(int(table(UNITS[lane][n], c)) for n in range(n_units))

    def wait_blocks(m, sem, ref):
        if m:
            drain(ref(m), sem)

    for d in range(8):
        c, lane = d // 2, d % 2

        @pl.when(2 * chip + e == d)
        def _():
            queries = [lambda m, src=src: src.at[0:m, pl.ds(0, grp)] for src in (q, do, o, dq)]
            keys = [lambda m, src=src: src.at[0:m, pl.ds(0, blk)] for src in (k, v)]
            grads = [lambda m, src=src: src.at[0:m, 0] for src in (dk, dv)]
            for a, ref in enumerate(queries[:2] + keys):
                wait_blocks(count(lambda u, i: i in WORK[u].get(i, ()), c, 1 - lane), own_send.at[a], ref)
                for ln in lanes:
                    wait_blocks(count(lambda u, i: i in FEED[u], c, ln), fed_send.at[a, ln], ref)
            for a, ref in enumerate(keys):
                for ln in lanes:
                    wait_blocks(count(lambda u, i: i in SHARE[u], c, ln), kv_send.at[a, ln], ref)
            wait_blocks(count(lambda u, i: i in RELAY[u], c, lane), relay_send, lambda m: kv_l.at[0:m, 0])
            for a, ref in enumerate(queries[2:] + grads):
                for ln in lanes:
                    at_home = (lambda u, i: i in WORK[u].get(i, ())) if a < 2 else (lambda u, i: i in FINISH[u] and i in FINISH[u][i][0])
                    wait_blocks(n_units - (count(at_home, c, ln) if ln == lane else 0), out_recv.at[a, ln], ref)
    for d in range(8):
        left = [n for n in range(n_units) if d // 2 in WORK[UNITS[d % 2][n]] and d // 2 not in FINISH[UNITS[d % 2][n]]]
        for i in range(max(len(left) - 2, 0), len(left)):
            @pl.when(2 * chip + e == d)
            def _():
                drain(acc.at[0], g_send.at[depth + i % 2])


def finish_kernel(o, dq, dk, dv, o_out, dq_out, dk_out, dv_out, ring, g_in, g_out, ring_in, ring_out, g_load, g_store):
    n_rows, n_kv, blk, _ = dk.shape
    half = SUB // n_kv
    at = lax.broadcasted_iota(jnp.int32, (SUB, SUB), 0)
    take = lax.broadcasted_iota(jnp.int32, (SUB, SUB), 1)
    perm = jnp.where(take == (at % n_kv) * half + at // n_kv, 1.0, 0.0).astype(bf16)
    pairs = ((o, o_out), (dq, dq_out))
    grads = ((dk, dk_out), (dv, dv_out))

    def move(i, out):
        src, dst = pairs[i % 2]
        if out:
            return pltpu.make_async_copy(ring.at[i], dst.at[i // 2], ring_out.at[i])
        return pltpu.make_async_copy(src.at[i // 2], ring.at[i], ring_in.at[i])

    def grad_rows(r):
        return pl.ds(4 * (r // 4), 4)

    def load(a, r):
        return pltpu.make_async_copy(grads[a][0].at[grad_rows(r)], g_in.at[a, grad_rows(r)], g_load.at[a, r // 4])

    def store(a, r):
        return pltpu.make_async_copy(g_out.at[a, grad_rows(r)], grads[a][1].at[grad_rows(r)], g_store.at[a, r // 4])

    n = 2 * n_rows
    for i in range(4):
        move(i, False).start()
    for r in range(0, n_rows, 4):
        load(0, r).start()
        load(1, r).start()
    for i in range(4, n):
        move(i, False).start()
    for i in range(n):
        move(i, False).wait()
        move(i, True).start()
        a, r = i % 2, i // 2
        if r % 4 == 0:
            load(a, r).wait()
        for p in range(blk // half):
            x = jnp.concatenate([g_in[a, r, h, p * half:(p + 1) * half, :] for h in range(n_kv)], 0)
            g_out[a, r, p * SUB:(p + 1) * SUB, :] = dot(perm, x).astype(bf16)
        if r % 4 == 3:
            store(a, r).start()
    for i in range(n):
        move(i, True).wait()
    for r in range(0, n_rows, 4):
        store(0, r).wait()
        store(1, r).wait()


def solution(mesh):
    spec = P('data', CTX_AXES, None, None)

    def local_attn(q_in, k_in, v_in, do_in):
        n_rows, blk, n_heads, dim = q_in.shape
        n_kv = k_in.shape[2]
        grp = n_heads // n_kv
        n_units = n_rows // 2 * n_kv
        n_chunks = 4
        to_heads = lambda x: jnp.swapaxes(x, 1, 2)
        any_spec = pl.BlockSpec(memory_space=pl.ANY)
        shape = jax.ShapeDtypeStruct
        q_shape = shape((n_rows, n_heads, blk, dim), bf16)
        k_shape = shape((n_rows, n_kv, blk, dim), bf16)
        joined = shape((n_rows, blk * n_kv, dim), bf16)
        landing = (shape((n_units, 2, 2, grp, CHUNK, dim), bf16), shape((n_units, n_chunks, 2, CHUNK, dim), bf16),
                   shape((n_units, 3, 2, CHUNK, dim), f32))
        vmem, dma = pltpu.VMEM, pltpu.SemaphoreType.DMA
        res = pl.pallas_call(
            kernel,
            out_shape=(q_shape, q_shape, k_shape, k_shape, joined, joined, *landing),
            in_specs=[any_spec] * 4,
            out_specs=(any_spec,) * 9,
            scratch_shapes=[
                vmem((2, 2, grp, CHUNK, dim), bf16), vmem((2, n_chunks, 2, CHUNK, dim), bf16),
                vmem((OUT_SLOTS, 2, grp, CHUNK, dim), bf16),
                vmem(((LAG + 1) * n_chunks + 2, 2, CHUNK, dim), f32),
                vmem((3, 2, CHUNK, dim), f32), vmem((2, 2, 2, CHUNK, dim), bf16),
                vmem((n_chunks, dim, CHUNK), bf16), vmem((n_chunks, dim, CHUNK), bf16),
                vmem((2, dim, CHUNK), bf16), vmem((2, dim, CHUNK), bf16),
                vmem((2, n_chunks, CHUNK, CHUNK), f32), vmem((n_chunks, CHUNK, CHUNK), f32),
                vmem((dim, CHUNK), f32), vmem((dim, CHUNK), f32),
                vmem((2, SUB, CHUNK), bf16), vmem((2, SUB, CHUNK), bf16),
                dma((4,)), dma((4, 2)), dma((2, 2)), dma,
                dma((n_units, 2)), dma((n_units, n_chunks)),
                dma((LAG + 3,)), dma((n_units, 3)),
                dma((OUT_SLOTS,)), dma((4, 2)), dma((2, 2)), dma((2,)), dma((2, n_chunks)), dma((3,)),
            ],
            compiler_params=pltpu.CompilerParams(
                collective_id=0, has_side_effects=True, vmem_limit_bytes=63 * 2**20),
            name='pair_attention',
        )(to_heads(q_in), k_in.reshape(joined.shape), v_in.reshape(joined.shape), to_heads(do_in))
        o, dq, dk, dv = pl.pallas_call(
            finish_kernel,
            out_shape=(q_shape, q_shape, joined, joined),
            in_specs=[any_spec] * 4,
            out_specs=(any_spec,) * 4,
            scratch_shapes=[
                vmem((2 * n_rows, n_heads, blk, dim), bf16),
                vmem((2, n_rows, n_kv, blk, dim), bf16), vmem((2, n_rows, n_kv * blk, dim), bf16),
                dma((2 * n_rows,)), dma((2 * n_rows,)), dma((2, n_rows // 4)), dma((2, n_rows // 4)),
            ],
            compiler_params=pltpu.CompilerParams(vmem_limit_bytes=62 * 2**20),
            name='finish',
        )(*res[:4])
        return to_heads(o), to_heads(dq), dk.reshape(k_in.shape), dv.reshape(k_in.shape)

    return jax.shard_map(local_attn, mesh=mesh, in_specs=(spec,) * 4, out_specs=(spec,) * 4, check_vma=False)
```

```python
import functools
import math
import jax
import jax.numpy as jnp
from jax import lax
from jax.experimental import pallas as pl
from jax.experimental.pallas import tpu as pltpu
from jax.sharding import PartitionSpec as P

CTX_AXES = ('ctxo', 'ctx')
MESH = pl.DeviceIdType.MESH
f32 = jnp.float32
bf16 = jnp.bfloat16
CHUNK = 768
SUB = 256
def by_chip(rows, read):
    return {kind: {c: read(word) for c, word in enumerate(words.split()) if word != '-'} for kind, words in rows.items()}


def digits(word):
    return tuple(int(z) for z in word)


WORK = by_chip({'T': '02 13 - -', 'Y': '0 - 2 13', 'X': '01 - 23 -', 'V': '0 1 - 23'}, digits)
FEED = by_chip({'T': '- - 0 1', 'Y': '- 3 - -', 'X': '- 0 - 2', 'V': '- - 3 -'}, int)
SHARE = by_chip({'T': '1 0 - -', 'Y': '2 - 3 -', 'X': '2 - - -', 'V': '1 3 - -'}, digits)
RELAY = by_chip({'T': '21 - - -', 'Y': '- - 03 12', 'X': '12 - - -', 'V': '- 03 - -'}, digits)
SUMS = by_chip({'T': '110 201000 - -', 'Y': '022 - 130 221020', 'X': '- - 000101 -', 'V': '012 - - 010111'},
               lambda word: tuple(digits(word[i:i + 3]) for i in range(0, len(word), 3)))
FINISH = by_chip({'T': '02:0:1 13:0: - -', 'Y': '- - 02:02:1 13:0:', 'X': '01:0:1 - 23:: -', 'V': '- 01:02:1 - 23::'},
                 lambda word: tuple(digits(part) for part in word.split(':')))
KINDS = 'TYXV'
UNITS = ('TVXYTVXTYXTYXYVT', 'XTVXTVYXTYTYXVTX')
LEADS = (20, 25, 21, 10, 7)
LAG = 2
OUT_SLOTS = 4


def dot(a, b):
    return jnp.dot(a, b, preferred_element_type=f32)


def fold(x, op):
    return op(x.reshape(x.shape[0] // 8, 8, x.shape[1]), axis=0)


def tile(i):
    return slice(i * SUB, (i + 1) * SUB)


def attend_chunk(c, q, do, kv, o, dq, g, base, s, scale, hooks):
    kT, vT, qT, doT, sc_ref, dp_ref, oT, dqT, pb, sb = s
    score_scale = scale * math.log2(math.e)
    n_sub = CHUNK // SUB
    n_heads = q.shape[0]

    def cols(ki, diag):
        return range(ki, n_sub) if diag else range(n_sub)

    lowest = tuple(jnp.full((8, SUB), -jnp.inf, f32) for _ in range(n_sub))

    def load_heads(h, b):
        for i in range(n_sub):
            qT[b, :, tile(i)] = q[h, tile(i), :].T
            doT[b, :, tile(i)] = do[h, tile(i), :].T

    def scores(j, b, m, ki, diag):
        for qi in cols(ki, diag):
            x = dot(kv[j, 0, tile(ki), :], qT[b, :, tile(qi)]) * score_scale
            if diag and ki == qi:
                key = lax.broadcasted_iota(jnp.int32, (SUB, SUB), 0)
                query = lax.broadcasted_iota(jnp.int32, (SUB, SUB), 1)
                x = jnp.where(key <= query, x, -jnp.inf)
            sc_ref[b, j, tile(ki), tile(qi)] = x
            m[qi] = jnp.maximum(m[qi], fold(x, jnp.max))

    def score_pass(b):
        def body(j, m, diag=False):
            m = list(m)
            for ki in range(n_sub):
                scores(j, b, m, ki, diag)
            return tuple(m)
        return body(c, lax.fori_loop(0, c, body, lowest), True)

    def forward_pass(b, m):
        top = [jnp.max(x, axis=0, keepdims=True) for x in m]
        oT[...] = jnp.zeros_like(oT)

        def body(j, l, diag=False):
            l, acc = list(l), [None] * n_sub

            def probs(ki):
                for qi in cols(ki, diag):
                    e = jnp.exp2(sc_ref[b, j, tile(ki), tile(qi)] - top[qi])
                    sc_ref[b, j, tile(ki), tile(qi)] = e
                    l[qi] = l[qi] + fold(e, jnp.sum)
                    pb[ki % 2, :, tile(qi)] = e.astype(bf16)

            def prob_grads(ki):
                for qi in cols(ki, diag):
                    dp_ref[j, tile(ki), tile(qi)] = dot(kv[j, 1, tile(ki), :], doT[b, :, tile(qi)])

            def outputs(ki):
                for qi in cols(ki, diag):
                    d = dot(vT[j, :, tile(ki)], pb[ki % 2, :, tile(qi)])
                    acc[qi] = d if acc[qi] is None else acc[qi] + d

            for ki in range(n_sub + 1):
                if ki < n_sub:
                    prob_grads(ki)
                    probs(ki)
                if ki:
                    outputs(ki - 1)
            for qi in range(n_sub):
                oT[:, tile(qi)] += acc[qi]
            return tuple(l)

        l = tuple(jnp.zeros((8, SUB), f32) for _ in range(n_sub))
        l = body(c, lax.fori_loop(0, c, body, l), True)
        return [1.0 / jnp.sum(x, axis=0, keepdims=True) for x in l]

    def finish_outputs(h, b, inv):
        drow = []
        for qi in range(n_sub):
            out = oT[:, tile(qi)] * inv[qi]
            drow.append(jnp.sum(out * doT[b, :, tile(qi)].astype(f32), axis=0, keepdims=True))
            o[h, tile(qi), :] = out.astype(bf16).T
        return drow

    def backward_pass(h, b, inv, drow, more):
        dqT[...] = jnp.zeros_like(dqT)

        def body(j, m, diag=False):
            m, acc = list(m), [None] * n_sub

            def score_grads(ki):
                for qi in cols(ki, diag):
                    p = sc_ref[b, j, tile(ki), tile(qi)] * inv[qi]
                    ds = p * (dp_ref[j, tile(ki), tile(qi)] - drow[qi])
                    pb[ki % 2, :, tile(qi)] = p.astype(bf16)
                    sb[ki % 2, :, tile(qi)] = ds.astype(bf16)

            def grads(ki):
                first = ki * SUB if diag else 0
                for qi in cols(ki, diag):
                    d = dot(kT[j, :, tile(ki)], sb[ki % 2, :, tile(qi)])
                    acc[qi] = d if acc[qi] is None else acc[qi] + d
                g[base + j, 1, tile(ki), :] += dot(pb[ki % 2, :, first:], do[h, first:, :])
                g[base + j, 0, tile(ki), :] += dot(sb[ki % 2, :, first:], q[h, first:, :])

            if more:
                scores(j, 1 - b, m, 0, diag)
            score_grads(0)
            for ki in range(1, n_sub):
                score_grads(ki)
                grads(ki - 1)
                if more:
                    scores(j, 1 - b, m, ki, diag)
            grads(n_sub - 1)
            for qi in range(n_sub):
                dqT[:, tile(qi)] += acc[qi]
            return tuple(m)

        m = body(c, lax.fori_loop(0, c, body, lowest), True)
        for qi in range(n_sub):
            dq[h, tile(qi), :] = (dqT[:, tile(qi)] * scale).astype(bf16).T
        return m

    load_heads(0, 0)
    m = score_pass(0)
    for h in range(n_heads):
        b = h % 2
        inv = forward_pass(b, m)
        drow = finish_outputs(h, b, inv)
        if h + 1 < n_heads:
            load_heads(h + 1, 1 - b)
        m = backward_pass(h, b, inv, drow, h + 1 < n_heads)
        if h < len(hooks):
            hooks[h]()


def kernel(q, k_raw, v_raw, do, o, dq, dk, dv, k, v, qd_l, kv_l, g_l,
           qd_v, kv_v, od_v, acc, g_in, g_out, kT, vT, *rest):
    scratch, sems = rest[:8], rest[8:]
    own_send, fed_send, kv_send, relay_send, qd_recv, kv_recv, g_send, g_recv, out_send, out_recv, grad_send, qd_load, kv_load, g_load = sems
    y, b = lax.axis_index('ctxo'), lax.axis_index('ctx')
    x, e = b // 2, b % 2
    chip = 2 * y + x
    n_rows, n_heads, blk, dim = q.shape
    n_kv = k.shape[1] // blk
    grp = n_heads // n_kv
    lane_rows = n_rows // 2
    n_units = lane_rows * n_kv
    chips, lanes = range(4), range(2)
    scale = 1.0 / math.sqrt(dim)
    depth = LAG + 1

    def core(c, ce):
        return (0, c // 2, 2 * (c % 2) + ce)

    def row_of(n, lane):
        return lane * lane_rows + n // n_kv

    def half(h):
        return pl.ds(pl.multiple_of(h * blk, blk), blk)

    def remote(src, dst, send, recv, dev):
        pltpu.make_async_remote_copy(src, dst, send, recv, device_id=dev, device_id_type=MESH).start()

    def drain(ref, sem):
        pltpu.make_async_copy(ref, ref, sem).wait()

    def choose(values, index):
        return functools.reduce(lambda r, i: jnp.where(index == i, values[i], r), range(1, len(values)), values[0])

    def tasks_of(c, lane):
        return [(n, j) for n in range(n_units) for j in WORK[UNITS[lane][n]].get(c, ())]

    def finished_of(c, lane):
        return [n for n in range(n_units) if c in FINISH[UNITS[lane][n]]]

    def here(value):
        return choose([value(c, lane) for c in chips for lane in lanes], 2 * chip + e)

    def padded(items, i):
        return items[i] if i < len(items) else 0
    most = max(len(tasks_of(c, lane)) for c in chips for lane in lanes)
    n_tasks = here(lambda c, lane: len(tasks_of(c, lane)))
    task_tab = [here(lambda c, lane: padded([4 * n + j for n, j in tasks_of(c, lane)], i)) for i in range(most + 1)]
    start_tab = [here(lambda c, lane: sum(m < n for m, _ in tasks_of(c, lane))) for n in range(n_units)]
    n_finished = here(lambda c, lane: len(finished_of(c, lane)))
    fin_tab = [here(lambda c, lane: padded(finished_of(c, lane), i)) for i in range(n_units)]

    def units_before(c, lane, i, finished):
        tasks = tasks_of(c, lane)
        now = tasks[i][0] if i < len(tasks) else n_units
        return sum((n in finished_of(c, lane)) == finished for n in {m for m, _ in tasks if m < now})
    fin_before = [here(lambda c, lane: units_before(c, lane, i, True)) for i in range(most)]
    oth_before = [here(lambda c, lane: units_before(c, lane, i, False)) for i in range(most)]

    def kind_of(n, lane):
        return jnp.where(lane == 0, *(choose([KINDS.index(u) for u in UNITS[c]], n) for c in lanes))

    def role(table, kind, c=chip):
        return choose([table(u, i) for u in KINDS for i in chips], 4 * kind + c)

    def own(kind):
        return role(lambda u, c: int(c in WORK[u].get(c, ())), kind) == 1

    def relayed(kind):
        return role(lambda u, c: RELAY[u].get(c, (-1, 0))[0], kind)

    barrier = pltpu.get_barrier_semaphore()
    peers = [core(chip, 1 - e)] + [core(c, ce) for c in (2 * (1 - y) + x, 2 * y + 1 - x) for ce in lanes]
    for dev in peers:
        pl.semaphore_signal(barrier, inc=1, device_id=dev, device_id_type=MESH)
    pl.semaphore_wait(barrier, len(peers))

    def block(src, n, lane, a):
        if a < 2:
            return src.at[row_of(n, lane), pl.ds((n % n_kv) * grp, grp)]
        return src.at[row_of(n, lane), half(n % n_kv)]

    def split_heads():
        part = SUB // n_kv
        at = lax.broadcasted_iota(jnp.int32, (SUB, SUB), 0)
        take = lax.broadcasted_iota(jnp.int32, (SUB, SUB), 1)
        perm = jnp.where(take == (at % part) * n_kv + at // part, 1.0, 0.0).astype(bf16)

        def room(a, r):
            return od_v.at[r // 6, r // 3 % 2, r % 3] if a else kv_v.at[r // 8, r // 2 % 4, r % 2]

        for a, raw in enumerate((k_raw, v_raw)):
            for r in range(n_rows):
                pltpu.make_async_copy(raw.at[r], room(a, r), kv_load.at[a, r // 4]).start()
        for a, (raw, dst) in enumerate(((k_raw, k), (v_raw, v))):
            def sort(r, _):
                @pl.when(r % 4 == 0)
                def _():
                    drain(raw.at[0:4], kv_load.at[a, r // 4])
                x = room(a, r)
                y = [dot(perm, x[tile(p), :]).astype(bf16) for p in range(n_kv * blk // SUB)]
                for p, rows in enumerate(y):
                    for h in range(n_kv):
                        x[h * blk + p * part:h * blk + (p + 1) * part, :] = rows[h * part:(h + 1) * part]
                return 0
            lax.fori_loop(0, n_rows, sort, 0)
            for r in range(n_rows):
                pltpu.make_async_copy(room(a, r), dst.at[r], qd_load.at[a]).start()
        for a, dst in enumerate((k, v)):
            drain(dst, qd_load.at[a])

    def send_keys(n, lane, c, send):
        for a, src in enumerate((k, v)):
            remote(block(src, n, lane, 2), kv_l.at[n, chip, a, half(e), :], send(a), kv_recv.at[n, chip], core(c, lane))

    def send_queries(n, lane, c, place, send):
        for a, src in enumerate((q, do)):
            remote(block(src, n, lane, 0), qd_l.at[n, place, a, :, half(e), :], send(a), qd_recv.at[n, place], core(c, lane))

    def send_own(n):
        lane = 1 - e

        @pl.when(own(kind_of(n, lane)))
        def _():
            send_queries(n, lane, chip, 0, lambda a: own_send.at[a])
            send_keys(n, lane, chip, lambda a: own_send.at[2 + a])

    def feed_keys(n):
        for lane in lanes:
            c = role(lambda u, i: FEED[u].get(i, -1), kind_of(n, lane))

            @pl.when(c >= 0)
            def _():
                send_keys(n, lane, c, lambda a: fed_send.at[2 + a, lane])

    def feed_queries(n):
        for lane in lanes:
            c = role(lambda u, i: FEED[u].get(i, -1), kind_of(n, lane))

            @pl.when(c >= 0)
            def _():
                send_queries(n, lane, c, 1, lambda a: fed_send.at[a, lane])

    def share_keys(n):
        for lane in lanes:
            c = role(lambda u, i: SHARE[u].get(i, (-1,))[0], kind_of(n, lane))

            @pl.when(c >= 0)
            def _():
                send_keys(n, lane, c, lambda a: kv_send.at[a, lane])

    def pass_on(n):
        kind = kind_of(n, e)
        j = relayed(kind)

        @pl.when(j >= 0)
        def _():
            drain(kv_l.at[n, j], kv_recv.at[n, j])
            c = role(lambda u, i: RELAY[u].get(i, (0, 0))[1], kind)
            remote(kv_l.at[n, j], kv_l.at[n, j], relay_send, kv_recv.at[n, j], core(c, e))

    jobs = (send_own, share_keys, feed_keys, pass_on, feed_queries)
    early_units = n_kv

    def run_due(h):
        for job, lead in zip(jobs, LEADS):
            lo = sum(jnp.where(2 * t - lead < h, 1, 0) for t in start_tab)
            hi = sum(jnp.where(2 * t - lead < h + 1, 1, 0) for t in start_tab)
            if job is feed_queries:
                lo = jnp.where(lo < early_units, early_units, lo)

            def one(n, _):
                job(n)
                return 0
            lax.fori_loop(lo, hi, one, 0)

    def fetch(s, slot_kv, first, prev):
        code = choose(task_tab, s)
        n, c = code // 4, code % 4
        kind, slot = kind_of(n, e), s % 2

        def keys(j, _):
            dst, sem = kv_v.at[slot_kv, j], kv_load.at[slot_kv, j]

            @pl.when(j == chip)
            def _():
                other = kv_l.at[n, j, :, half(1 - e), :]
                drain(other, kv_recv.at[n, j])
                pltpu.make_async_copy(other, dst.at[:, half(1 - e), :], sem).start()
                for a, src in enumerate((k, v)):
                    pltpu.make_async_copy(block(src, n, e, 2), dst.at[a, half(e), :], sem).start()

            @pl.when(j != chip)
            def _():
                @pl.when(j != relayed(kind))
                def _():
                    drain(kv_l.at[n, j], kv_recv.at[n, j])
                pltpu.make_async_copy(kv_l.at[n, j], dst, sem).start()
            return 0
        lax.fori_loop(jnp.where(first, 0, prev + 1), c + 1, keys, 0)

        @pl.when(c == chip)
        def _():
            other = qd_l.at[n, 0, :, :, half(1 - e), :]
            drain(other, qd_recv.at[n, 0])
            pltpu.make_async_copy(other, qd_v.at[slot, :, :, half(1 - e), :], qd_load.at[slot]).start()
            for a, src in enumerate((q, do)):
                pltpu.make_async_copy(block(src, n, e, 0), qd_v.at[slot, a, :, half(e), :], qd_load.at[slot]).start()

        @pl.when(c != chip)
        def _():
            drain(qd_l.at[n, 1], qd_recv.at[n, 1])
            pltpu.make_async_copy(qd_l.at[n, 1], qd_v.at[slot], qd_load.at[slot]).start()

    def place(c, send, pieces):
        for h in range(2):
            local = (c == chip) & (e == h)
            for src, dst, recv in pieces(h):
                @pl.when(local)
                def _():
                    pltpu.make_async_copy(src, dst, send).start()

                @pl.when(jnp.logical_not(local))
                def _():
                    remote(src, dst, send, recv, core(c, h))

    def n_in(kind, f):
        return role(lambda u, c: len(FINISH[u][c][1 + f]) if c in FINISH[u] else 0, kind)

    def get_sums(n, a):
        drain(g_l.at[n, a], g_recv.at[n, a])
        pltpu.make_async_copy(g_l.at[n, a], g_in.at[a], g_load.at[a]).start()

    def fetch_sums(i):
        n = choose(fin_tab, i)
        kind = kind_of(n, e)
        for a, f, least in ((0, 0, 1), (2, 0, 2), (1, 1, 1)):
            @pl.when(n_in(kind, f) >= least)
            def _():
                get_sums(n, a)

    def merge(i):
        n = choose(fin_tab, i)
        kind, base, slot = kind_of(n, e), 4 * (i % depth), i % 2
        for f in range(2):
            c = role(lambda u, j: FINISH[u][j][0][f] if j in FINISH[u] else 0, kind)

            @pl.when(i >= 2)
            def _():
                drain(g_out.at[slot, f], grad_send.at[slot, f])
            for places in ((), (0,), (0, 2)) if f == 0 else ((), (1,)):
                @pl.when(n_in(kind, f) == len(places))
                def _():
                    for a in places:
                        drain(g_in.at[a], g_load.at[a])
                    for i_kv, factor in enumerate((scale, None)):
                        total = acc[base + c, i_kv]
                        for a in places:
                            total = total + g_in[a, i_kv]
                        g_out[slot, f, i_kv] = (total if factor is None else total * factor).astype(bf16)
            place(c, grad_send.at[slot, f], lambda h: [
                (g_out.at[slot, f, i_kv, h * blk:(h + 1) * blk, :], dst.at[row_of(n, e), n % n_kv], out_recv.at[2 + i_kv, e])
                for i_kv, dst in enumerate((dk, dv))])

    def n_sums(kind):
        return role(lambda u, c: len(SUMS[u].get(c, ())), kind)

    def send_sums(n, base, sem):
        kind = kind_of(n, e)
        for m in range(2):
            @pl.when(n_sums(kind) > m)
            def _():
                j, c, a = (role(lambda u, i: SUMS[u][i][m][part] if len(SUMS[u].get(i, ())) > m else 0, kind) for part in range(3))
                remote(acc.at[base + j], g_l.at[n, a], sem, g_recv.at[n, a], core(c, e))

    def sums_left(i):
        n = choose(fin_tab, i)
        for m in (1, 2):
            @pl.when(n_sums(kind_of(n, e)) == m)
            def _():
                drain(acc.at[0:m], g_send.at[i % depth])

    lax.fori_loop(0, early_units, lambda n, _: (feed_queries(n), 0)[1], 0)
    split_heads()

    def before(h, _):
        run_due(h - max(LEADS))
        return 0
    lax.fori_loop(0, max(LEADS), before, 0)
    fetch(0, 0, True, 0)

    def task(s, _):
        n_fin, n_oth = choose(fin_before, s), choose(oth_before, s)
        code, after = choose(task_tab, s), choose(task_tab, s + 1)
        n, c = code // 4, code % 4
        prev = choose([task_tab[0]] + task_tab[:-1], s)
        first = (s == 0) | (prev // 4 != n)
        last = (s + 1 == n_tasks) | (after // 4 != n)
        kind = kind_of(n, e)
        fin = role(lambda u, i: int(i in FINISH[u]), kind) == 1
        base = jnp.where(fin, 4 * (n_fin % depth), 4 * depth + n_oth % 2)
        slot, slot_kv, o_slot = s % 2, (n_fin + n_oth) % 2, s % OUT_SLOTS
        lo = jnp.where(first, 0, prev % 4 + 1)

        @pl.when(first & fin & (n_fin >= depth))
        def _():
            sums_left(n_fin - depth)

        @pl.when(first & jnp.logical_not(fin) & (n_oth >= 2))
        def _():
            drain(acc.at[0], g_send.at[depth + n_oth % 2])

        def turn(j, _):
            drain(kv_v.at[slot_kv, j], kv_load.at[slot_kv, j])
            kT[j] = kv_v[slot_kv, j, 0].T
            vT[j] = kv_v[slot_kv, j, 1].T
            acc[base + j] = jnp.zeros(acc.shape[1:], f32)
            return 0
        lax.fori_loop(lo, c + 1, turn, 0)
        drain(qd_v.at[slot], qd_load.at[slot])

        @pl.when(s >= OUT_SLOTS)
        def _():
            drain(od_v.at[o_slot], out_send.at[o_slot])

        def early():
            run_due(2 * s)

        def late():
            run_due(2 * s + 1)

            @pl.when(s + 1 < n_tasks)
            def _():
                fetch(s + 1, (n_fin + n_oth + jnp.where(last, 1, 0)) % 2, last, c)

            @pl.when(last & fin & (n_fin >= LAG))
            def _():
                fetch_sums(n_fin - LAG)
        attend_chunk(c, qd_v.at[slot, 0], qd_v.at[slot, 1], kv_v.at[slot_kv], od_v.at[o_slot, 0], od_v.at[o_slot, 1],
                     acc, base, (kT, vT, *scratch), scale, (early, late))
        place(c, out_send.at[o_slot], lambda h: [
            (od_v.at[o_slot, i, :, h * blk:(h + 1) * blk, :], block(dst, n, e, 0), out_recv.at[i, e]) for i, dst in enumerate((o, dq))])

        @pl.when(last)
        def _():
            send_sums(n, base, g_send.at[jnp.where(fin, n_fin % depth, depth + n_oth % 2)])

            @pl.when(fin & (n_fin >= LAG))
            def _():
                merge(n_fin - LAG)
        return 0

    def task_or_rest(s, _):
        @pl.when(s < n_tasks)
        def _():
            task(s, 0)
        return 0
    lax.fori_loop(0, most, task_or_rest, 0)

    def rest_of(i, _):
        fetch_sums(i)
        merge(i)
        return 0
    lax.fori_loop(n_finished - LAG, n_finished, rest_of, 0)

    for slot in range(OUT_SLOTS):
        drain(od_v.at[slot], out_send.at[slot])
    for slot in range(2):
        for f in range(2):
            drain(g_out.at[slot, f], grad_send.at[slot, f])
    lax.fori_loop(n_finished - depth, n_finished, lambda i, _: (sums_left(i), 0)[1], 0)

    def count(table, c, lane):
        return sum(int(table(UNITS[lane][n], c)) for n in range(n_units))

    def wait_blocks(m, sem, ref):
        if m:
            drain(ref(m), sem)

    for d in range(8):
        c, lane = d // 2, d % 2

        @pl.when(2 * chip + e == d)
        def _():
            queries = [lambda m, src=src: src.at[0:m, pl.ds(0, grp)] for src in (q, do, o, dq)]
            keys = [lambda m, src=src: src.at[0:m, pl.ds(0, blk)] for src in (k, v)]
            grads = [lambda m, src=src: src.at[0:m, 0] for src in (dk, dv)]
            for a, ref in enumerate(queries[:2] + keys):
                wait_blocks(count(lambda u, i: i in WORK[u].get(i, ()), c, 1 - lane), own_send.at[a], ref)
                for ln in lanes:
                    wait_blocks(count(lambda u, i: i in FEED[u], c, ln), fed_send.at[a, ln], ref)
            for a, ref in enumerate(keys):
                for ln in lanes:
                    wait_blocks(count(lambda u, i: i in SHARE[u], c, ln), kv_send.at[a, ln], ref)
            wait_blocks(count(lambda u, i: i in RELAY[u], c, lane), relay_send, lambda m: kv_l.at[0:m, 0])
            for a, ref in enumerate(queries[2:] + grads):
                for ln in lanes:
                    at_home = (lambda u, i: i in WORK[u].get(i, ())) if a < 2 else (lambda u, i: i in FINISH[u] and i in FINISH[u][i][0])
                    wait_blocks(n_units - (count(at_home, c, ln) if ln == lane else 0), out_recv.at[a, ln], ref)
    for d in range(8):
        left = [n for n in range(n_units) if d // 2 in WORK[UNITS[d % 2][n]] and d // 2 not in FINISH[UNITS[d % 2][n]]]
        for i in range(max(len(left) - 2, 0), len(left)):
            @pl.when(2 * chip + e == d)
            def _():
                drain(acc.at[0], g_send.at[depth + i % 2])


def finish_kernel(o, dq, dk, dv, o_out, dq_out, dk_out, dv_out, ring, g_in, g_out, ring_in, ring_out, g_load, g_store):
    n_rows, n_kv, blk, _ = dk.shape
    half = SUB // n_kv
    at = lax.broadcasted_iota(jnp.int32, (SUB, SUB), 0)
    take = lax.broadcasted_iota(jnp.int32, (SUB, SUB), 1)
    perm = jnp.where(take == (at % n_kv) * half + at // n_kv, 1.0, 0.0).astype(bf16)
    pairs = ((o, o_out), (dq, dq_out))
    grads = ((dk, dk_out), (dv, dv_out))

    def move(i, out):
        src, dst = pairs[i % 2]
        if out:
            return pltpu.make_async_copy(ring.at[i], dst.at[i // 2], ring_out.at[i])
        return pltpu.make_async_copy(src.at[i // 2], ring.at[i], ring_in.at[i])

    def grad_rows(r):
        return pl.ds(4 * (r // 4), 4)

    def load(a, r):
        return pltpu.make_async_copy(grads[a][0].at[grad_rows(r)], g_in.at[a, grad_rows(r)], g_load.at[a, r // 4])

    def store(a, r):
        return pltpu.make_async_copy(g_out.at[a, grad_rows(r)], grads[a][1].at[grad_rows(r)], g_store.at[a, r // 4])

    n = 2 * n_rows
    for i in range(4):
        move(i, False).start()
    for r in range(0, n_rows, 4):
        load(0, r).start()
        load(1, r).start()
    for i in range(4, n):
        move(i, False).start()
    for i in range(n):
        move(i, False).wait()
        move(i, True).start()
        a, r = i % 2, i // 2
        if r % 4 == 0:
            load(a, r).wait()
        for p in range(blk // half):
            x = jnp.concatenate([g_in[a, r, h, p * half:(p + 1) * half, :] for h in range(n_kv)], 0)
            g_out[a, r, p * SUB:(p + 1) * SUB, :] = dot(perm, x).astype(bf16)
        if r % 4 == 3:
            store(a, r).start()
    for i in range(n):
        move(i, True).wait()
    for r in range(0, n_rows, 4):
        store(0, r).wait()
        store(1, r).wait()


def solution(mesh):
    spec = P('data', CTX_AXES, None, None)

    def local_attn(q_in, k_in, v_in, do_in):
        n_rows, blk, n_heads, dim = q_in.shape
        n_kv = k_in.shape[2]
        grp = n_heads // n_kv
        n_units = n_rows // 2 * n_kv
        n_chunks = 4
        to_heads = lambda x: jnp.swapaxes(x, 1, 2)
        any_spec = pl.BlockSpec(memory_space=pl.ANY)
        shape = jax.ShapeDtypeStruct
        q_shape = shape((n_rows, n_heads, blk, dim), bf16)
        k_shape = shape((n_rows, n_kv, blk, dim), bf16)
        joined = shape((n_rows, blk * n_kv, dim), bf16)
        landing = (shape((n_units, 2, 2, grp, CHUNK, dim), bf16), shape((n_units, n_chunks, 2, CHUNK, dim), bf16),
                   shape((n_units, 3, 2, CHUNK, dim), f32))
        vmem, dma = pltpu.VMEM, pltpu.SemaphoreType.DMA
        res = pl.pallas_call(
            kernel,
            out_shape=(q_shape, q_shape, k_shape, k_shape, joined, joined, *landing),
            in_specs=[any_spec] * 4,
            out_specs=(any_spec,) * 9,
            scratch_shapes=[
                vmem((2, 2, grp, CHUNK, dim), bf16), vmem((2, n_chunks, 2, CHUNK, dim), bf16),
                vmem((OUT_SLOTS, 2, grp, CHUNK, dim), bf16),
                vmem(((LAG + 1) * n_chunks + 2, 2, CHUNK, dim), f32),
                vmem((3, 2, CHUNK, dim), f32), vmem((2, 2, 2, CHUNK, dim), bf16),
                vmem((n_chunks, dim, CHUNK), bf16), vmem((n_chunks, dim, CHUNK), bf16),
                vmem((2, dim, CHUNK), bf16), vmem((2, dim, CHUNK), bf16),
                vmem((2, n_chunks, CHUNK, CHUNK), f32), vmem((n_chunks, CHUNK, CHUNK), f32),
                vmem((dim, CHUNK), f32), vmem((dim, CHUNK), f32),
                vmem((2, SUB, CHUNK), bf16), vmem((2, SUB, CHUNK), bf16),
                dma((4,)), dma((4, 2)), dma((2, 2)), dma,
                dma((n_units, 2)), dma((n_units, n_chunks)),
                dma((LAG + 3,)), dma((n_units, 3)),
                dma((OUT_SLOTS,)), dma((4, 2)), dma((2, 2)), dma((2,)), dma((2, n_chunks)), dma((3,)),
            ],
            compiler_params=pltpu.CompilerParams(
                collective_id=0, has_side_effects=True, vmem_limit_bytes=63 * 2**20),
            name='pair_attention',
        )(to_heads(q_in), k_in.reshape(joined.shape), v_in.reshape(joined.shape), to_heads(do_in))
        o, dq, dk, dv = pl.pallas_call(
            finish_kernel,
            out_shape=(q_shape, q_shape, joined, joined),
            in_specs=[any_spec] * 4,
            out_specs=(any_spec,) * 4,
            scratch_shapes=[
                vmem((2 * n_rows, n_heads, blk, dim), bf16),
                vmem((2, n_rows, n_kv, blk, dim), bf16), vmem((2, n_rows, n_kv * blk, dim), bf16),
                dma((2 * n_rows,)), dma((2 * n_rows,)), dma((2, n_rows // 4)), dma((2, n_rows // 4)),
            ],
            compiler_params=pltpu.CompilerParams(vmem_limit_bytes=62 * 2**20),
            name='finish',
        )(*res[:4])
        return to_heads(o), to_heads(dq), dk.reshape(k_in.shape), dv.reshape(k_in.shape)

    return jax.shard_map(local_attn, mesh=mesh, in_specs=(spec,) * 4, out_specs=(spec,) * 4, check_vma=False)
```

```python
import functools
import math
import jax
import jax.numpy as jnp
from jax import lax
from jax.experimental import pallas as pl
from jax.experimental.pallas import tpu as pltpu
from jax.sharding import PartitionSpec as P

CTX_AXES = ('ctxo', 'ctx')
MESH = pl.DeviceIdType.MESH
f32 = jnp.float32
bf16 = jnp.bfloat16
CHUNK = 768
SUB = 256
def by_chip(rows, read):
    return {kind: {c: read(word) for c, word in enumerate(words.split()) if word != '-'} for kind, words in rows.items()}


def digits(word):
    return tuple(int(z) for z in word)


WORK = by_chip({'T': '02 13 - -', 'Y': '0 - 2 13', 'X': '01 - 23 -', 'V': '0 1 - 23'}, digits)
FEED = by_chip({'T': '- - 0 1', 'Y': '- 3 - -', 'X': '- 0 - 2', 'V': '- - 3 -'}, int)
SHARE = by_chip({'T': '1 0 - -', 'Y': '2 - 3 -', 'X': '2 - - -', 'V': '1 3 - -'}, digits)
RELAY = by_chip({'T': '21 - - -', 'Y': '- - 03 12', 'X': '12 - - -', 'V': '- 03 - -'}, digits)
SUMS = by_chip({'T': '110 201000 - -', 'Y': '022 - 130 221020', 'X': '- - 000101 -', 'V': '012 - - 010111'},
               lambda word: tuple(digits(word[i:i + 3]) for i in range(0, len(word), 3)))
FINISH = by_chip({'T': '02:0:1 13:0: - -', 'Y': '- - 02:02:1 13:0:', 'X': '01:0:1 - 23:: -', 'V': '- 01:02:1 - 23::'},
                 lambda word: tuple(digits(part) for part in word.split(':')))
KINDS = 'TYXV'
UNITS = ('TVXYTVXTYXTYXYVT', 'XTVXTVYXTYTYXVTX')
LEADS = (20, 25, 21, 10, 7)
LAG = 2
OUT_SLOTS = 4


def dot(a, b):
    return jnp.dot(a, b, preferred_element_type=f32)


def fold(x, op):
    return op(x.reshape(x.shape[0] // 8, 8, x.shape[1]), axis=0)


def tile(i):
    return slice(i * SUB, (i + 1) * SUB)


def attend_chunk(c, q, do, kv, o, dq, g, base, s, scale, hooks):
    kT, vT, qT, doT, sc_ref, dp_ref, oT, dqT, pb, sb = s
    score_scale = scale * math.log2(math.e)
    n_sub = CHUNK // SUB
    n_heads = q.shape[0]

    def cols(ki, diag):
        return range(ki, n_sub) if diag else range(n_sub)

    lowest = tuple(jnp.full((8, SUB), -jnp.inf, f32) for _ in range(n_sub))

    def load_heads(h, b):
        for i in range(n_sub):
            qT[b, :, tile(i)] = q[h, tile(i), :].T
            doT[b, :, tile(i)] = do[h, tile(i), :].T

    def scores(j, b, m, ki, diag):
        for qi in cols(ki, diag):
            x = dot(kv[j, 0, tile(ki), :], qT[b, :, tile(qi)]) * score_scale
            if diag and ki == qi:
                key = lax.broadcasted_iota(jnp.int32, (SUB, SUB), 0)
                query = lax.broadcasted_iota(jnp.int32, (SUB, SUB), 1)
                x = jnp.where(key <= query, x, -jnp.inf)
            sc_ref[b, j, tile(ki), tile(qi)] = x
            m[qi] = jnp.maximum(m[qi], fold(x, jnp.max))

    def score_pass(b):
        def body(j, m, diag=False):
            m = list(m)
            for ki in range(n_sub):
                scores(j, b, m, ki, diag)
            return tuple(m)
        return body(c, lax.fori_loop(0, c, body, lowest), True)

    def forward_pass(b, m):
        top = [jnp.max(x, axis=0, keepdims=True) for x in m]
        oT[...] = jnp.zeros_like(oT)

        def body(j, l, diag=False):
            l, acc = list(l), [None] * n_sub

            def probs(ki):
                for qi in cols(ki, diag):
                    e = jnp.exp2(sc_ref[b, j, tile(ki), tile(qi)] - top[qi])
                    sc_ref[b, j, tile(ki), tile(qi)] = e
                    l[qi] = l[qi] + fold(e, jnp.sum)
                    pb[ki % 2, :, tile(qi)] = e.astype(bf16)

            def prob_grads(ki):
                for qi in cols(ki, diag):
                    dp_ref[j, tile(ki), tile(qi)] = dot(kv[j, 1, tile(ki), :], doT[b, :, tile(qi)])

            def outputs(ki):
                for qi in cols(ki, diag):
                    d = dot(vT[j, :, tile(ki)], pb[ki % 2, :, tile(qi)])
                    acc[qi] = d if acc[qi] is None else acc[qi] + d

            for ki in range(n_sub + 1):
                if ki < n_sub:
                    prob_grads(ki)
                    probs(ki)
                if ki:
                    outputs(ki - 1)
            for qi in range(n_sub):
                oT[:, tile(qi)] += acc[qi]
            return tuple(l)

        l = tuple(jnp.zeros((8, SUB), f32) for _ in range(n_sub))
        l = body(c, lax.fori_loop(0, c, body, l), True)
        return [1.0 / jnp.sum(x, axis=0, keepdims=True) for x in l]

    def finish_outputs(h, b, inv):
        drow = []
        for qi in range(n_sub):
            out = oT[:, tile(qi)] * inv[qi]
            drow.append(jnp.sum(out * doT[b, :, tile(qi)].astype(f32), axis=0, keepdims=True))
            o[h, tile(qi), :] = out.astype(bf16).T
        return drow

    def backward_pass(h, b, inv, drow, more):
        dqT[...] = jnp.zeros_like(dqT)

        def body(j, m, diag=False):
            m, acc = list(m), [None] * n_sub

            def score_grads(ki):
                for qi in cols(ki, diag):
                    p = sc_ref[b, j, tile(ki), tile(qi)] * inv[qi]
                    ds = p * (dp_ref[j, tile(ki), tile(qi)] - drow[qi])
                    pb[ki % 2, :, tile(qi)] = p.astype(bf16)
                    sb[ki % 2, :, tile(qi)] = ds.astype(bf16)

            def grads(ki):
                first = ki * SUB if diag else 0
                for qi in cols(ki, diag):
                    d = dot(kT[j, :, tile(ki)], sb[ki % 2, :, tile(qi)])
                    acc[qi] = d if acc[qi] is None else acc[qi] + d
                g[base + j, 1, tile(ki), :] += dot(pb[ki % 2, :, first:], do[h, first:, :])
                g[base + j, 0, tile(ki), :] += dot(sb[ki % 2, :, first:], q[h, first:, :])

            if more:
                scores(j, 1 - b, m, 0, diag)
            score_grads(0)
            for ki in range(1, n_sub):
                score_grads(ki)
                grads(ki - 1)
                if more:
                    scores(j, 1 - b, m, ki, diag)
            grads(n_sub - 1)
            for qi in range(n_sub):
                dqT[:, tile(qi)] += acc[qi]
            return tuple(m)

        m = body(c, lax.fori_loop(0, c, body, lowest), True)
        for qi in range(n_sub):
            dq[h, tile(qi), :] = (dqT[:, tile(qi)] * scale).astype(bf16).T
        return m

    load_heads(0, 0)
    m = score_pass(0)
    for h in range(n_heads):
        b = h % 2
        inv = forward_pass(b, m)
        drow = finish_outputs(h, b, inv)
        if h + 1 < n_heads:
            load_heads(h + 1, 1 - b)
        m = backward_pass(h, b, inv, drow, h + 1 < n_heads)
        if h < len(hooks):
            hooks[h]()


def kernel(q, k_raw, v_raw, do, o, dq, dk, dv, k, v, qd_l, kv_l, g_l,
           qd_v, kv_v, od_v, acc, g_in, g_out, kT, vT, *rest):
    scratch, sems = rest[:8], rest[8:]
    own_send, fed_send, kv_send, relay_send, qd_recv, kv_recv, g_send, g_recv, out_send, out_recv, grad_send, qd_load, kv_load, g_load = sems
    y, b = lax.axis_index('ctxo'), lax.axis_index('ctx')
    x, e = b // 2, b % 2
    chip = 2 * y + x
    n_rows, n_heads, blk, dim = q.shape
    n_kv = k.shape[1] // blk
    grp = n_heads // n_kv
    lane_rows = n_rows // 2
    n_units = lane_rows * n_kv
    chips, lanes = range(4), range(2)
    scale = 1.0 / math.sqrt(dim)
    depth = LAG + 1

    def core(c, ce):
        return (0, c // 2, 2 * (c % 2) + ce)

    def row_of(n, lane):
        return lane * lane_rows + n // n_kv

    def half(h):
        return pl.ds(pl.multiple_of(h * blk, blk), blk)

    def remote(src, dst, send, recv, dev):
        pltpu.make_async_remote_copy(src, dst, send, recv, device_id=dev, device_id_type=MESH).start()

    def drain(ref, sem):
        pltpu.make_async_copy(ref, ref, sem).wait()

    def choose(values, index):
        return functools.reduce(lambda r, i: jnp.where(index == i, values[i], r), range(1, len(values)), values[0])

    def tasks_of(c, lane):
        return [(n, j) for n in range(n_units) for j in WORK[UNITS[lane][n]].get(c, ())]

    def finished_of(c, lane):
        return [n for n in range(n_units) if c in FINISH[UNITS[lane][n]]]

    def here(value):
        return choose([value(c, lane) for c in chips for lane in lanes], 2 * chip + e)

    def padded(items, i):
        return items[i] if i < len(items) else 0
    most = max(len(tasks_of(c, lane)) for c in chips for lane in lanes)
    n_tasks = here(lambda c, lane: len(tasks_of(c, lane)))
    task_tab = [here(lambda c, lane: padded([4 * n + j for n, j in tasks_of(c, lane)], i)) for i in range(most + 1)]
    start_tab = [here(lambda c, lane: sum(m < n for m, _ in tasks_of(c, lane))) for n in range(n_units)]
    n_finished = here(lambda c, lane: len(finished_of(c, lane)))
    fin_tab = [here(lambda c, lane: padded(finished_of(c, lane), i)) for i in range(n_units)]

    def units_before(c, lane, i, finished):
        tasks = tasks_of(c, lane)
        now = tasks[i][0] if i < len(tasks) else n_units
        return sum((n in finished_of(c, lane)) == finished for n in {m for m, _ in tasks if m < now})
    fin_before = [here(lambda c, lane: units_before(c, lane, i, True)) for i in range(most)]
    oth_before = [here(lambda c, lane: units_before(c, lane, i, False)) for i in range(most)]

    def kind_of(n, lane):
        return jnp.where(lane == 0, *(choose([KINDS.index(u) for u in UNITS[c]], n) for c in lanes))

    def role(table, kind, c=chip):
        return choose([table(u, i) for u in KINDS for i in chips], 4 * kind + c)

    def own(kind):
        return role(lambda u, c: int(c in WORK[u].get(c, ())), kind) == 1

    def relayed(kind):
        return role(lambda u, c: RELAY[u].get(c, (-1, 0))[0], kind)

    barrier = pltpu.get_barrier_semaphore()
    peers = [core(chip, 1 - e)] + [core(c, ce) for c in (2 * (1 - y) + x, 2 * y + 1 - x) for ce in lanes]
    for dev in peers:
        pl.semaphore_signal(barrier, inc=1, device_id=dev, device_id_type=MESH)
    pl.semaphore_wait(barrier, len(peers))

    def block(src, n, lane, a):
        if a < 2:
            return src.at[row_of(n, lane), pl.ds((n % n_kv) * grp, grp)]
        return src.at[row_of(n, lane), half(n % n_kv)]

    def split_heads():
        part = SUB // n_kv
        at = lax.broadcasted_iota(jnp.int32, (SUB, SUB), 0)
        take = lax.broadcasted_iota(jnp.int32, (SUB, SUB), 1)
        perm = jnp.where(take == (at % part) * n_kv + at // part, 1.0, 0.0).astype(bf16)

        def room(a, r):
            return od_v.at[r // 6, r // 3 % 2, r % 3] if a else kv_v.at[r // 8, r // 2 % 4, r % 2]

        for a, raw in enumerate((k_raw, v_raw)):
            for r in range(n_rows):
                pltpu.make_async_copy(raw.at[r], room(a, r), kv_load.at[a, r // 4]).start()
        for a, (raw, dst) in enumerate(((k_raw, k), (v_raw, v))):
            def sort(r, _):
                @pl.when(r % 4 == 0)
                def _():
                    drain(raw.at[0:4], kv_load.at[a, r // 4])
                x = room(a, r)
                y = [dot(perm, x[tile(p), :]).astype(bf16) for p in range(n_kv * blk // SUB)]
                for p, rows in enumerate(y):
                    for h in range(n_kv):
                        x[h * blk + p * part:h * blk + (p + 1) * part, :] = rows[h * part:(h + 1) * part]
                return 0
            lax.fori_loop(0, n_rows, sort, 0)
            for r in range(n_rows):
                pltpu.make_async_copy(room(a, r), dst.at[r], qd_load.at[a]).start()
        for a, dst in enumerate((k, v)):
            drain(dst, qd_load.at[a])

    def send_keys(n, lane, c, send):
        for a, src in enumerate((k, v)):
            remote(block(src, n, lane, 2), kv_l.at[n, chip, a, half(e), :], send(a), kv_recv.at[n, chip], core(c, lane))

    def send_queries(n, lane, c, place, send):
        for a, src in enumerate((q, do)):
            remote(block(src, n, lane, 0), qd_l.at[n, place, a, :, half(e), :], send(a), qd_recv.at[n, place], core(c, lane))

    def send_own(n):
        lane = 1 - e

        @pl.when(own(kind_of(n, lane)))
        def _():
            send_queries(n, lane, chip, 0, lambda a: own_send.at[a])
            send_keys(n, lane, chip, lambda a: own_send.at[2 + a])

    def feed_keys(n):
        for lane in lanes:
            c = role(lambda u, i: FEED[u].get(i, -1), kind_of(n, lane))

            @pl.when(c >= 0)
            def _():
                send_keys(n, lane, c, lambda a: fed_send.at[2 + a, lane])

    def feed_queries(n):
        for lane in lanes:
            c = role(lambda u, i: FEED[u].get(i, -1), kind_of(n, lane))

            @pl.when(c >= 0)
            def _():
                send_queries(n, lane, c, 1, lambda a: fed_send.at[a, lane])

    def share_keys(n):
        for lane in lanes:
            c = role(lambda u, i: SHARE[u].get(i, (-1,))[0], kind_of(n, lane))

            @pl.when(c >= 0)
            def _():
                send_keys(n, lane, c, lambda a: kv_send.at[a, lane])

    def pass_on(n):
        kind = kind_of(n, e)
        j = relayed(kind)

        @pl.when(j >= 0)
        def _():
            drain(kv_l.at[n, j], kv_recv.at[n, j])
            c = role(lambda u, i: RELAY[u].get(i, (0, 0))[1], kind)
            remote(kv_l.at[n, j], kv_l.at[n, j], relay_send, kv_recv.at[n, j], core(c, e))

    jobs = (send_own, share_keys, feed_keys, pass_on, feed_queries)
    early_units = n_kv

    def run_due(h):
        for job, lead in zip(jobs, LEADS):
            lo = sum(jnp.where(2 * t - lead < h, 1, 0) for t in start_tab)
            hi = sum(jnp.where(2 * t - lead < h + 1, 1, 0) for t in start_tab)
            if job is feed_queries:
                lo = jnp.where(lo < early_units, early_units, lo)

            def one(n, _):
                job(n)
                return 0
            lax.fori_loop(lo, hi, one, 0)

    def fetch(s, slot_kv, first, prev):
        code = choose(task_tab, s)
        n, c = code // 4, code % 4
        kind, slot = kind_of(n, e), s % 2

        def keys(j, _):
            dst, sem = kv_v.at[slot_kv, j], kv_load.at[slot_kv, j]

            @pl.when(j == chip)
            def _():
                other = kv_l.at[n, j, :, half(1 - e), :]
                drain(other, kv_recv.at[n, j])
                pltpu.make_async_copy(other, dst.at[:, half(1 - e), :], sem).start()
                for a, src in enumerate((k, v)):
                    pltpu.make_async_copy(block(src, n, e, 2), dst.at[a, half(e), :], sem).start()

            @pl.when(j != chip)
            def _():
                @pl.when(j != relayed(kind))
                def _():
                    drain(kv_l.at[n, j], kv_recv.at[n, j])
                pltpu.make_async_copy(kv_l.at[n, j], dst, sem).start()
            return 0
        lax.fori_loop(jnp.where(first, 0, prev + 1), c + 1, keys, 0)

        @pl.when(c == chip)
        def _():
            other = qd_l.at[n, 0, :, :, half(1 - e), :]
            drain(other, qd_recv.at[n, 0])
            pltpu.make_async_copy(other, qd_v.at[slot, :, :, half(1 - e), :], qd_load.at[slot]).start()
            for a, src in enumerate((q, do)):
                pltpu.make_async_copy(block(src, n, e, 0), qd_v.at[slot, a, :, half(e), :], qd_load.at[slot]).start()

        @pl.when(c != chip)
        def _():
            drain(qd_l.at[n, 1], qd_recv.at[n, 1])
            pltpu.make_async_copy(qd_l.at[n, 1], qd_v.at[slot], qd_load.at[slot]).start()

    def place(c, send, pieces):
        for h in range(2):
            local = (c == chip) & (e == h)
            for src, dst, recv in pieces(h):
                @pl.when(local)
                def _():
                    pltpu.make_async_copy(src, dst, send).start()

                @pl.when(jnp.logical_not(local))
                def _():
                    remote(src, dst, send, recv, core(c, h))

    def n_in(kind, f):
        return role(lambda u, c: len(FINISH[u][c][1 + f]) if c in FINISH[u] else 0, kind)

    def get_sums(n, a):
        drain(g_l.at[n, a], g_recv.at[n, a])
        pltpu.make_async_copy(g_l.at[n, a], g_in.at[a], g_load.at[a]).start()

    def fetch_sums(i):
        n = choose(fin_tab, i)
        kind = kind_of(n, e)
        for a, f, least in ((0, 0, 1), (2, 0, 2), (1, 1, 1)):
            @pl.when(n_in(kind, f) >= least)
            def _():
                get_sums(n, a)

    def merge(i):
        n = choose(fin_tab, i)
        kind, base, slot = kind_of(n, e), 4 * (i % depth), i % 2
        for f in range(2):
            c = role(lambda u, j: FINISH[u][j][0][f] if j in FINISH[u] else 0, kind)

            @pl.when(i >= 2)
            def _():
                drain(g_out.at[slot, f], grad_send.at[slot, f])
            for places in ((), (0,), (0, 2)) if f == 0 else ((), (1,)):
                @pl.when(n_in(kind, f) == len(places))
                def _():
                    for a in places:
                        drain(g_in.at[a], g_load.at[a])
                    for i_kv, factor in enumerate((scale, None)):
                        total = acc[base + c, i_kv]
                        for a in places:
                            total = total + g_in[a, i_kv]
                        g_out[slot, f, i_kv] = (total if factor is None else total * factor).astype(bf16)
            place(c, grad_send.at[slot, f], lambda h: [
                (g_out.at[slot, f, i_kv, h * blk:(h + 1) * blk, :], dst.at[row_of(n, e), n % n_kv], out_recv.at[2 + i_kv, e])
                for i_kv, dst in enumerate((dk, dv))])

    def n_sums(kind):
        return role(lambda u, c: len(SUMS[u].get(c, ())), kind)

    def send_sums(n, base, sem):
        kind = kind_of(n, e)
        for m in range(2):
            @pl.when(n_sums(kind) > m)
            def _():
                j, c, a = (role(lambda u, i: SUMS[u][i][m][part] if len(SUMS[u].get(i, ())) > m else 0, kind) for part in range(3))
                remote(acc.at[base + j], g_l.at[n, a], sem, g_recv.at[n, a], core(c, e))

    def sums_left(i):
        n = choose(fin_tab, i)
        for m in (1, 2):
            @pl.when(n_sums(kind_of(n, e)) == m)
            def _():
                drain(acc.at[0:m], g_send.at[i % depth])

    lax.fori_loop(0, early_units, lambda n, _: (feed_queries(n), 0)[1], 0)
    split_heads()

    def before(h, _):
        run_due(h - max(LEADS))
        return 0
    lax.fori_loop(0, max(LEADS), before, 0)
    fetch(0, 0, True, 0)

    def task(s, _):
        n_fin, n_oth = choose(fin_before, s), choose(oth_before, s)
        code, after = choose(task_tab, s), choose(task_tab, s + 1)
        n, c = code // 4, code % 4
        prev = choose([task_tab[0]] + task_tab[:-1], s)
        first = (s == 0) | (prev // 4 != n)
        last = (s + 1 == n_tasks) | (after // 4 != n)
        kind = kind_of(n, e)
        fin = role(lambda u, i: int(i in FINISH[u]), kind) == 1
        base = jnp.where(fin, 4 * (n_fin % depth), 4 * depth + n_oth % 2)
        slot, slot_kv, o_slot = s % 2, (n_fin + n_oth) % 2, s % OUT_SLOTS
        lo = jnp.where(first, 0, prev % 4 + 1)

        @pl.when(first & fin & (n_fin >= depth))
        def _():
            sums_left(n_fin - depth)

        @pl.when(first & jnp.logical_not(fin) & (n_oth >= 2))
        def _():
            drain(acc.at[0], g_send.at[depth + n_oth % 2])

        def turn(j, _):
            drain(kv_v.at[slot_kv, j], kv_load.at[slot_kv, j])
            kT[j] = kv_v[slot_kv, j, 0].T
            vT[j] = kv_v[slot_kv, j, 1].T
            acc[base + j] = jnp.zeros(acc.shape[1:], f32)
            return 0
        lax.fori_loop(lo, c + 1, turn, 0)
        drain(qd_v.at[slot], qd_load.at[slot])

        @pl.when(s >= OUT_SLOTS)
        def _():
            drain(od_v.at[o_slot], out_send.at[o_slot])

        def early():
            run_due(2 * s)

        def late():
            run_due(2 * s + 1)

            @pl.when(s + 1 < n_tasks)
            def _():
                fetch(s + 1, (n_fin + n_oth + jnp.where(last, 1, 0)) % 2, last, c)
        attend_chunk(c, qd_v.at[slot, 0], qd_v.at[slot, 1], kv_v.at[slot_kv], od_v.at[o_slot, 0], od_v.at[o_slot, 1],
                     acc, base, (kT, vT, *scratch), scale, (early, late))
        place(c, out_send.at[o_slot], lambda h: [
            (od_v.at[o_slot, i, :, h * blk:(h + 1) * blk, :], block(dst, n, e, 0), out_recv.at[i, e]) for i, dst in enumerate((o, dq))])

        @pl.when(last)
        def _():
            send_sums(n, base, g_send.at[jnp.where(fin, n_fin % depth, depth + n_oth % 2)])

            @pl.when(fin & (n_fin >= LAG))
            def _():
                fetch_sums(n_fin - LAG)
                merge(n_fin - LAG)
        return 0

    def task_or_rest(s, _):
        @pl.when(s < n_tasks)
        def _():
            task(s, 0)
        return 0
    lax.fori_loop(0, most, task_or_rest, 0)

    def rest_of(i, _):
        fetch_sums(i)
        merge(i)
        return 0
    lax.fori_loop(n_finished - LAG, n_finished, rest_of, 0)

    for slot in range(OUT_SLOTS):
        drain(od_v.at[slot], out_send.at[slot])
    for slot in range(2):
        for f in range(2):
            drain(g_out.at[slot, f], grad_send.at[slot, f])
    lax.fori_loop(n_finished - depth, n_finished, lambda i, _: (sums_left(i), 0)[1], 0)

    def count(table, c, lane):
        return sum(int(table(UNITS[lane][n], c)) for n in range(n_units))

    def wait_blocks(m, sem, ref):
        if m:
            drain(ref(m), sem)

    for d in range(8):
        c, lane = d // 2, d % 2

        @pl.when(2 * chip + e == d)
        def _():
            queries = [lambda m, src=src: src.at[0:m, pl.ds(0, grp)] for src in (q, do, o, dq)]
            keys = [lambda m, src=src: src.at[0:m, pl.ds(0, blk)] for src in (k, v)]
            grads = [lambda m, src=src: src.at[0:m, 0] for src in (dk, dv)]
            for a, ref in enumerate(queries[:2] + keys):
                wait_blocks(count(lambda u, i: i in WORK[u].get(i, ()), c, 1 - lane), own_send.at[a], ref)
                for ln in lanes:
                    wait_blocks(count(lambda u, i: i in FEED[u], c, ln), fed_send.at[a, ln], ref)
            for a, ref in enumerate(keys):
                for ln in lanes:
                    wait_blocks(count(lambda u, i: i in SHARE[u], c, ln), kv_send.at[a, ln], ref)
            wait_blocks(count(lambda u, i: i in RELAY[u], c, lane), relay_send, lambda m: kv_l.at[0:m, 0])
            for a, ref in enumerate(queries[2:] + grads):
                for ln in lanes:
                    at_home = (lambda u, i: i in WORK[u].get(i, ())) if a < 2 else (lambda u, i: i in FINISH[u] and i in FINISH[u][i][0])
                    wait_blocks(n_units - (count(at_home, c, ln) if ln == lane else 0), out_recv.at[a, ln], ref)
    for d in range(8):
        left = [n for n in range(n_units) if d // 2 in WORK[UNITS[d % 2][n]] and d // 2 not in FINISH[UNITS[d % 2][n]]]
        for i in range(max(len(left) - 2, 0), len(left)):
            @pl.when(2 * chip + e == d)
            def _():
                drain(acc.at[0], g_send.at[depth + i % 2])


def finish_kernel(o, dq, dk, dv, o_out, dq_out, dk_out, dv_out, ring, g_in, g_out, ring_in, ring_out, g_load, g_store):
    n_rows, n_kv, blk, _ = dk.shape
    half = SUB // n_kv
    at = lax.broadcasted_iota(jnp.int32, (SUB, SUB), 0)
    take = lax.broadcasted_iota(jnp.int32, (SUB, SUB), 1)
    perm = jnp.where(take == (at % n_kv) * half + at // n_kv, 1.0, 0.0).astype(bf16)
    pairs = ((o, o_out), (dq, dq_out))
    grads = ((dk, dk_out), (dv, dv_out))

    def move(i, out):
        src, dst = pairs[i % 2]
        if out:
            return pltpu.make_async_copy(ring.at[i], dst.at[i // 2], ring_out.at[i])
        return pltpu.make_async_copy(src.at[i // 2], ring.at[i], ring_in.at[i])

    def grad_rows(r):
        return pl.ds(4 * (r // 4), 4)

    def load(a, r):
        return pltpu.make_async_copy(grads[a][0].at[grad_rows(r)], g_in.at[a, grad_rows(r)], g_load.at[a, r // 4])

    def store(a, r):
        return pltpu.make_async_copy(g_out.at[a, grad_rows(r)], grads[a][1].at[grad_rows(r)], g_store.at[a, r // 4])

    n = 2 * n_rows
    for i in range(4):
        move(i, False).start()
    for r in range(0, n_rows, 4):
        load(0, r).start()
        load(1, r).start()
    for i in range(4, n):
        move(i, False).start()
    for i in range(n):
        move(i, False).wait()
        move(i, True).start()
        a, r = i % 2, i // 2
        if r % 4 == 0:
            load(a, r).wait()
        for p in range(blk // half):
            x = jnp.concatenate([g_in[a, r, h, p * half:(p + 1) * half, :] for h in range(n_kv)], 0)
            g_out[a, r, p * SUB:(p + 1) * SUB, :] = dot(perm, x).astype(bf16)
        if r % 4 == 3:
            store(a, r).start()
    for i in range(n):
        move(i, True).wait()
    for r in range(0, n_rows, 4):
        store(0, r).wait()
        store(1, r).wait()


def solution(mesh):
    spec = P('data', CTX_AXES, None, None)

    def local_attn(q_in, k_in, v_in, do_in):
        n_rows, blk, n_heads, dim = q_in.shape
        n_kv = k_in.shape[2]
        grp = n_heads // n_kv
        n_units = n_rows // 2 * n_kv
        n_chunks = 4
        to_heads = lambda x: jnp.swapaxes(x, 1, 2)
        any_spec = pl.BlockSpec(memory_space=pl.ANY)
        shape = jax.ShapeDtypeStruct
        q_shape = shape((n_rows, n_heads, blk, dim), bf16)
        k_shape = shape((n_rows, n_kv, blk, dim), bf16)
        joined = shape((n_rows, blk * n_kv, dim), bf16)
        landing = (shape((n_units, 2, 2, grp, CHUNK, dim), bf16), shape((n_units, n_chunks, 2, CHUNK, dim), bf16),
                   shape((n_units, 3, 2, CHUNK, dim), f32))
        vmem, dma = pltpu.VMEM, pltpu.SemaphoreType.DMA
        res = pl.pallas_call(
            kernel,
            out_shape=(q_shape, q_shape, k_shape, k_shape, joined, joined, *landing),
            in_specs=[any_spec] * 4,
            out_specs=(any_spec,) * 9,
            scratch_shapes=[
                vmem((2, 2, grp, CHUNK, dim), bf16), vmem((2, n_chunks, 2, CHUNK, dim), bf16),
                vmem((OUT_SLOTS, 2, grp, CHUNK, dim), bf16),
                vmem(((LAG + 1) * n_chunks + 2, 2, CHUNK, dim), f32),
                vmem((3, 2, CHUNK, dim), f32), vmem((2, 2, 2, CHUNK, dim), bf16),
                vmem((n_chunks, dim, CHUNK), bf16), vmem((n_chunks, dim, CHUNK), bf16),
                vmem((2, dim, CHUNK), bf16), vmem((2, dim, CHUNK), bf16),
                vmem((2, n_chunks, CHUNK, CHUNK), f32), vmem((n_chunks, CHUNK, CHUNK), f32),
                vmem((dim, CHUNK), f32), vmem((dim, CHUNK), f32),
                vmem((2, SUB, CHUNK), bf16), vmem((2, SUB, CHUNK), bf16),
                dma((4,)), dma((4, 2)), dma((2, 2)), dma,
                dma((n_units, 2)), dma((n_units, n_chunks)),
                dma((LAG + 3,)), dma((n_units, 3)),
                dma((OUT_SLOTS,)), dma((4, 2)), dma((2, 2)), dma((2,)), dma((2, n_chunks)), dma((3,)),
            ],
            compiler_params=pltpu.CompilerParams(
                collective_id=0, has_side_effects=True, vmem_limit_bytes=63 * 2**20),
            name='pair_attention',
        )(to_heads(q_in), k_in.reshape(joined.shape), v_in.reshape(joined.shape), to_heads(do_in))
        o, dq, dk, dv = pl.pallas_call(
            finish_kernel,
            out_shape=(q_shape, q_shape, joined, joined),
            in_specs=[any_spec] * 4,
            out_specs=(any_spec,) * 4,
            scratch_shapes=[
                vmem((2 * n_rows, n_heads, blk, dim), bf16),
                vmem((2, n_rows, n_kv, blk, dim), bf16), vmem((2, n_rows, n_kv * blk, dim), bf16),
                dma((2 * n_rows,)), dma((2 * n_rows,)), dma((2, n_rows // 4)), dma((2, n_rows // 4)),
            ],
            compiler_params=pltpu.CompilerParams(vmem_limit_bytes=62 * 2**20),
            name='finish',
        )(*res[:4])
        return to_heads(o), to_heads(dq), dk.reshape(k_in.shape), dv.reshape(k_in.shape)

    return jax.shard_map(local_attn, mesh=mesh, in_specs=(spec,) * 4, out_specs=(spec,) * 4, check_vma=False)
```
